32 devices in a mesh: dp: 1 (over z), tp: 4 (over y), cp: 8 (over x, core).
Axes of the slice: x: 4, y: 4, z: 1, core: 2. Of those that a mesh axis runs over, the one named last changes fastest.
The devices are a block of a 4x4x8 slice.
Arguments:
- hidden: bfloat16 [4096, 3072], P(('dp', 'cp'))
- positions: int32 [4096], P(('dp', 'cp'))
- norm_gain: bfloat16 [3072], replicated
- w_query: bfloat16 [3072, 3072], P(None, 'tp')
- w_key: bfloat16 [3072, 1024], P(None, 'tp')
- w_value: bfloat16 [3072, 1024], P(None, 'tp')
- w_out: bfloat16 [3072, 3072], P('tp')
Outputs:
- output 1: bfloat16 [4096, 3072], P(('dp', 'cp'))
- output 2: bfloat16 [4096, 8, 128], P(('dp', 'cp'), 'tp')
- output 3: bfloat16 [4096, 8, 128], P(('dp', 'cp'), 'tp')
All inputs are finite; a program needn't handle non-finite values.
Results may differ from the reference program's by a relative error of at most 0.00840561.
Values are sent between devices in bfloat16 or wider.
A program may use at most 768 MiB of HBM per device.

```python
import math
import jax
import jax.numpy as jnp
from jax import lax

D = 3072
HEADS = 24
KV_HEADS = 8
HEAD = 128
SEQ = 4096
Q_ROWS = 128

EPS = 1e-5
LOG_THETA = math.log(1000000.0)


def setup_inputs(seed: int = 0, part: int = 0) -> dict:
    base_key = jax.random.key(seed)
    shared = jax.random.split(base_key, 5)
    part_keys = jax.random.split(jax.random.fold_in(base_key, part), 3)
    sharpness = math.sqrt(math.log(SEQ / 16.0))
    hidden = 0.5 * jax.random.normal(part_keys[0], (SEQ, D), jnp.float32)
    first_pos = jax.random.randint(part_keys[1], (), 0, SEQ, dtype=jnp.int32)
    pos_steps = jax.random.randint(part_keys[2], (SEQ,), 1, 3, dtype=jnp.int32)
    positions = (first_pos + jnp.cumsum(pos_steps) - 1).astype(jnp.int32)
    norm_gain = 1.0 + 0.3 * jax.random.normal(shared[0], (D,), jnp.float32)
    w_query = (sharpness / math.sqrt(D)) * jax.random.normal(shared[1], (D, HEADS * HEAD), jnp.float32)
    w_key = jax.random.normal(shared[2], (D, KV_HEADS * HEAD), jnp.float32) / math.sqrt(D)
    w_value = jax.random.normal(shared[3], (D, KV_HEADS * HEAD), jnp.float32) / math.sqrt(D)
    w_out = jax.random.normal(shared[4], (HEADS * HEAD, D), jnp.float32) / math.sqrt(HEADS * HEAD)
    return {
        'hidden': hidden.astype(jnp.bfloat16),
        'positions': positions,
        'norm_gain': norm_gain.astype(jnp.bfloat16),
        'w_query': w_query.astype(jnp.bfloat16),
        'w_key': w_key.astype(jnp.bfloat16),
        'w_value': w_value.astype(jnp.bfloat16),
        'w_out': w_out.astype(jnp.bfloat16),
    }


def rope_tables(positions):
    half_dim = HEAD // 2
    inv_freq = jnp.exp(jnp.arange(half_dim, dtype=jnp.float32) * (-2.0 * LOG_THETA / HEAD))
    angles = positions.astype(jnp.float32)[..., None] * inv_freq
    return jnp.cos(angles), jnp.sin(angles)


def apply_rope(head_vals, cos_t, sin_t):
    half_dim = HEAD // 2
    first_half = head_vals[..., :half_dim]
    second_half = head_vals[..., half_dim:]
    return jnp.concatenate([first_half * cos_t - second_half * sin_t, second_half * cos_t + first_half * sin_t], axis=-1)


def reference(hidden, positions, norm_gain, w_query, w_key, w_value, w_out):
    group_size = HEADS // KV_HEADS
    tile_count = SEQ // Q_ROWS
    hidden_f = hidden.astype(jnp.float32)
    inv_rms = lax.rsqrt(jnp.mean(hidden_f * hidden_f, axis=-1, keepdims=True) + EPS)
    normed = (hidden_f * inv_rms * norm_gain.astype(jnp.float32)).astype(jnp.bfloat16)
    cos_t, sin_t = rope_tables(positions)
    cos_b = cos_t[:, None, :]
    sin_b = sin_t[:, None, :]
    q_proj = jnp.dot(normed, w_query, preferred_element_type=jnp.float32).reshape(SEQ, HEADS, HEAD)
    k_proj = jnp.dot(normed, w_key, preferred_element_type=jnp.float32).reshape(SEQ, KV_HEADS, HEAD)
    queries = apply_rope(q_proj, cos_b, sin_b).astype(jnp.bfloat16)
    k_rope = apply_rope(k_proj, cos_b, sin_b).astype(jnp.bfloat16)
    values = jnp.dot(normed, w_value, preferred_element_type=jnp.float32).astype(jnp.bfloat16).reshape(SEQ, KV_HEADS, HEAD)
    q_tiles = queries.astype(jnp.float32).reshape(tile_count, Q_ROWS, KV_HEADS, group_size, HEAD)
    pos_tiles = positions.reshape(tile_count, Q_ROWS)
    k_full = k_rope.astype(jnp.float32)
    v_full = values.astype(jnp.float32)
    score_scale = 1.0 / math.sqrt(HEAD)

    def one_tile(tile_in):
        q_tile, q_pos = tile_in
        scores = jnp.einsum('qngd,knd->ngqk', q_tile, k_full) * score_scale
        visible = positions[None, :] <= q_pos[:, None]
        scores = jnp.where(visible, scores, -jnp.inf)
        weights = jax.nn.softmax(scores, axis=-1)
        return jnp.einsum('ngqk,knd->qngd', weights, v_full)

    attn_tiles = lax.map(one_tile, (q_tiles, pos_tiles))
    attn_o = attn_tiles.reshape(SEQ, HEADS * HEAD).astype(jnp.bfloat16)
    attn_sum = jnp.dot(attn_o, w_out, preferred_element_type=jnp.float32)
    hidden_out = (hidden_f + attn_sum).astype(jnp.bfloat16)
    return hidden_out, k_rope, values
```

```python
import math
import jax
import jax.numpy as jnp
from jax import lax
from jax.experimental import pallas as pl
from jax.experimental.pallas import tpu as pltpu
from jax.sharding import PartitionSpec as P

HEAD = 128
EPS = 1e-5
LOG_THETA = math.log(1000000.0)
SCORE_EXP2 = math.log2(math.e) / math.sqrt(HEAD)
BF = jnp.bfloat16
F32 = jnp.float32
GROUPS = 4
Q_TILE = 256
NORM_ROWS = 32


def rope_tables(positions):
    half_dim = HEAD // 2
    inv_freq = jnp.exp(jnp.arange(half_dim, dtype=F32) * (-2.0 * LOG_THETA / HEAD))
    angles = positions.astype(F32)[:, None] * inv_freq
    cos_t, sin_t = jnp.cos(angles), jnp.sin(angles)
    return jnp.concatenate([cos_t, cos_t], axis=-1), jnp.concatenate([-sin_t, sin_t], axis=-1)


def block_kernel(ring, kv_heads, group_size,
                 x_hbm, gain_ref, cos_ref, sin_ref, wq_hbm, wk_hbm, wv_hbm, wo_hbm,
                 out_hbm, k_hbm, v_hbm,
                 x_v, h_v, wq_v, wk_v, wv_v, wo_v, q_v, kv_v, m_v, l_v, acc_v, o_v,
                 part_v, r1_v, r2_v, out_v,
                 load_sem, cache_sem, kv_send, kv_recv, kv_fwd_send,
                 s1_send, s1_recv, s2_send, s2_recv, f1_send, f1_recv, f2_send, f2_recv, out_sem):
    rows, width = x_v.shape
    cp = lax.axis_index('cp')
    tp = lax.axis_index('tp')
    chip = cp // 2
    core = cp % 2
    seg_rows = rows // ring
    half_cols = width // (2 * GROUPS)

    x_right = {'cp': ((chip + 1) % ring) * 2 + core}
    x_left = {'cp': ((chip + ring - 1) % ring) * 2 + core}
    sibling = {'cp': chip * 2 + 1 - core}
    y_right = {'tp': (tp + 1) % ring}
    y_left = {'tp': (tp + ring - 1) % ring}

    loads = [
        pltpu.make_async_copy(x_hbm, x_v, load_sem.at[0]),
        pltpu.make_async_copy(wk_hbm, wk_v, load_sem.at[1]),
        pltpu.make_async_copy(wv_hbm, wv_v, load_sem.at[2]),
        pltpu.make_async_copy(wq_hbm, wq_v, load_sem.at[3]),
        pltpu.make_async_copy(wo_hbm, wo_v, load_sem.at[4]),
    ]
    for copy in loads:
        copy.start()

    barrier = pltpu.get_barrier_semaphore()
    for peer in (x_right, x_left, sibling, y_right, y_left):
        pl.semaphore_signal(barrier, inc=1, device_id=peer, device_id_type=pl.DeviceIdType.MESH)

    loads[0].wait()

    def norm_step(i, carry):
        r0 = pl.multiple_of(i * NORM_ROWS, NORM_ROWS)
        xf = x_v[pl.ds(r0, NORM_ROWS), :].astype(F32)
        inv = lax.rsqrt(jnp.mean(xf * xf, axis=-1, keepdims=True) + EPS)
        h_v[pl.ds(r0, NORM_ROWS), :] = (xf * inv * gain_ref[...].astype(F32)).astype(BF)
        return carry

    lax.fori_loop(0, rows // NORM_ROWS, norm_step, 0)

    def rope(vals):
        return (vals * cos_ref[...] + pltpu.roll(vals, HEAD // 2, 1) * sin_ref[...]).astype(BF)

    loads[1].wait()
    k_proj = jnp.dot(h_v[...], wk_v[...], preferred_element_type=F32)
    for h in range(kv_heads):
        kv_v[0, 0, h, 0] = rope(k_proj[:, h * HEAD:(h + 1) * HEAD])
    loads[2].wait()
    v_proj = jnp.dot(h_v[...], wv_v[...], preferred_element_type=F32)
    for h in range(kv_heads):
        kv_v[0, 0, h, 1] = v_proj[:, h * HEAD:(h + 1) * HEAD].astype(BF)

    pl.semaphore_wait(barrier, 5)

    def remote(src, dst, send, recv, peer):
        return pltpu.make_async_remote_copy(src_ref=src, dst_ref=dst, send_sem=send, recv_sem=recv,
                                            device_id=peer, device_id_type=pl.DeviceIdType.MESH)

    def own_to(rel, cc, head, peer):
        return remote(kv_v.at[0, 0, head], kv_v.at[rel, cc, head],
                      kv_send.at[rel, head], kv_recv.at[rel, cc, head], peer)

    def fwd_far(head):
        rel, peer = (1, x_right) if head == 1 else (2, x_left)
        return remote(kv_v.at[rel, 0, head], kv_v.at[3, 0, head],
                      kv_send.at[3, head], kv_recv.at[3, 0, head], peer)

    def fwd_sib(rel, head):
        return remote(kv_v.at[rel, 0, head], kv_v.at[rel, 1, head],
                      kv_fwd_send.at[rel, head], kv_recv.at[rel, 1, head], sibling)

    right_sends = chip < ring - 1
    left_h0_sends = chip < 2
    left_h1_sends = chip < 1

    @pl.when(core == 0)
    def _():
        own_to(0, 1, 0, sibling).start()
        own_to(0, 1, 1, sibling).start()

    @pl.when(right_sends)
    def _():
        own_to(1, 0, 1, x_right).start()

    @pl.when(left_h0_sends)
    def _():
        own_to(2, 0, 0, x_left).start()

    @pl.when(right_sends)
    def _():
        own_to(1, 0, 0, x_right).start()

    @pl.when(left_h1_sends)
    def _():
        own_to(2, 0, 1, x_left).start()

    cache_copies = []
    for h in range(kv_heads):
        for kv, dst in ((0, k_hbm), (1, v_hbm)):
            cache_copies.append(pltpu.make_async_copy(
                kv_v.at[0, 0, h, kv], dst.at[:, h * HEAD:(h + 1) * HEAD], cache_sem.at[h, kv]))
    for copy in cache_copies:
        copy.start()

    loads[3].wait()

    def q_step(j, carry):
        c0 = pl.multiple_of(j * 2 * HEAD, 2 * HEAD)
        q_proj = jnp.dot(h_v[...], wq_v[:, pl.ds(c0, 2 * HEAD)], preferred_element_type=F32)
        q_v[2 * j] = rope(q_proj[:, :HEAD])
        q_v[2 * j + 1] = rope(q_proj[:, HEAD:])
        return carry

    lax.fori_loop(0, kv_heads * group_size // 2, q_step, 0)

    def scores(q_tile, k_tile):
        return lax.dot_general(q_tile, k_tile, (((1,), (1,)), ((), ())), preferred_element_type=F32)

    def lane_chunks(s):
        return [s[:, i * HEAD:(i + 1) * HEAD] for i in range(s.shape[1] // HEAD)]

    def tree(op, parts):
        parts = list(parts)
        while len(parts) > 1:
            parts = [op(parts[i], parts[i + 1]) if i + 1 < len(parts) else parts[i] for i in range(0, len(parts), 2)]
        return parts[0]

    def row_max(chunks):
        return jnp.max(tree(jnp.maximum, chunks), axis=1, keepdims=True)

    def weights(chunks, m_new):
        probs = [jnp.exp2((s - m_new) * SCORE_EXP2) for s in chunks]
        return probs, tree(jnp.add, probs)

    def pv(probs, v_tile):
        return jnp.dot(jnp.concatenate([p.astype(BF) for p in probs], axis=1), v_tile, preferred_element_type=F32)

    def own_unit(qi, carry):
        head = qi // group_size
        for rt in range(rows // Q_TILE):
            r0, keys = rt * Q_TILE, (rt + 1) * Q_TILE
            s = scores(q_v[qi, r0:r0 + Q_TILE, :], kv_v[0, 0, head, 0, :keys, :])
            row_id = lax.broadcasted_iota(jnp.int32, s.shape, 0) + r0
            col_id = lax.broadcasted_iota(jnp.int32, s.shape, 1)
            chunks = lane_chunks(jnp.where(col_id <= row_id, s, -jnp.inf))
            m_new = jnp.broadcast_to(row_max(chunks), (Q_TILE, HEAD))
            probs, l_new = weights(chunks, m_new)
            acc_v[qi, r0:r0 + Q_TILE, :] = pv(probs, kv_v[0, 0, head, 1, :keys, :])
            m_v[qi, r0:r0 + Q_TILE, :] = m_new
            l_v[qi, r0:r0 + Q_TILE, :] = l_new
        return carry

    lax.fori_loop(0, kv_heads * group_size, own_unit, 0)

    def far_unit(rel, cc, head):
        def q_head(g, carry):
            qi = head * group_size + g
            for rt in range(rows // Q_TILE):
                rs = slice(rt * Q_TILE, (rt + 1) * Q_TILE)
                chunks = lane_chunks(scores(q_v[qi, rs, :], kv_v[rel, cc, head, 0]))
                m_old = m_v[qi, rs, :]
                m_new = jnp.maximum(m_old, row_max(chunks))
                alpha = jnp.exp2((m_old - m_new) * SCORE_EXP2)
                probs, l_new = weights(chunks, m_new)
                acc_v[qi, rs, :] = acc_v[qi, rs, :] * alpha + pv(probs, kv_v[rel, cc, head, 1])
                l_v[qi, rs, :] = l_v[qi, rs, :] * alpha + l_new
                m_v[qi, rs, :] = m_new
            return carry

        lax.fori_loop(0, group_size, q_head, 0)

    has_left = chip >= 1
    has_right = chip >= 3
    has_far = chip >= 2
    fwd_right = jnp.logical_and(chip >= 1, chip <= 2)
    fwd_left = jnp.logical_or(chip == 0, chip == 3)

    def phase(p, carry):
        @pl.when(jnp.logical_and(p == 0, core == 1))
        def _():
            own_to(0, 1, 0, sibling).wait_recv()
            own_to(0, 1, 1, sibling).wait_recv()

        @pl.when(jnp.logical_and(p == 1, has_left))
        def _():
            own_to(1, 0, 1, x_right).wait_recv()

            @pl.when(fwd_right)
            def _():
                fwd_far(1).start()

            fwd_sib(1, 1).start()

        @pl.when(jnp.logical_and(p == 1, fwd_left))
        def _():
            own_to(2, 0, 0, x_left).wait_recv()
            fwd_far(0).start()

            @pl.when(has_right)
            def _():
                fwd_sib(2, 0).start()

        @pl.when(jnp.logical_and(p == 2, has_left))
        def _():
            own_to(1, 0, 0, x_right).wait_recv()
            fwd_sib(1, 0).start()

        @pl.when(jnp.logical_and(p == 2, has_right))
        def _():
            own_to(2, 0, 1, x_left).wait_recv()
            fwd_sib(2, 1).start()

        @pl.when(jnp.logical_and(p == 3, has_far))
        def _():
            fwd_far(1).wait_recv()
            fwd_sib(3, 1).start()
            fwd_far(0).wait_recv()
            fwd_sib(3, 0).start()

        def unit(i, inner):
            cc, which = i // 2, i % 2
            head = (p + which) % 2
            rel = ((p + 2) // 3) * (1 + which) + (p // 3) * (2 - which)
            need = ((p == 0) & (cc == 1) & (core == 1)) | ((rel == 1) & has_left) | ((rel == 2) & has_right) | ((rel == 3) & has_far)

            @pl.when(need & (p > 0) & (cc == 1))
            def _():
                remote(kv_v.at[rel, 0, head], kv_v.at[rel, 1, head], kv_fwd_send.at[rel, head],
                       kv_recv.at[rel, 1, head], sibling).wait_recv()

            @pl.when(need)
            def _():
                far_unit(rel, cc, head)

            return inner

        lax.fori_loop(0, 4, unit, 0)
        return carry

    lax.fori_loop(0, 4, phase, 0)

    def norm_out(qi, carry):
        l_row = jnp.sum(l_v[qi], axis=1, keepdims=True)
        c0 = pl.multiple_of(qi * HEAD, HEAD)
        o_v[:, pl.ds(c0, HEAD)] = (acc_v[qi] / l_row).astype(BF)
        return carry

    lax.fori_loop(0, kv_heads * group_size, norm_out, 0)
    loads[4].wait()

    def seg(offset):
        return pl.ds(pl.multiple_of(((tp + offset + ring) % ring) * seg_rows, seg_rows), seg_rows)

    def s1(g, d):
        return remote(part_v.at[g, d, seg(2), :], r1_v.at[g, d], s1_send.at[g, d], s1_recv.at[g, d],
                      y_left if d else y_right)

    def s2(g, d, half):
        return remote(part_v.at[g, half, seg(-1 if d else 1), :], r2_v.at[g, d, half],
                      s2_send.at[g, d, half], s2_recv.at[g, d, half], y_left if d else y_right)

    def f1(g, d):
        return remote(out_v.at[g, :, seg(0), :], out_v.at[g, :, seg(0), :], f1_send.at[g, d], f1_recv.at[g, d],
                      y_left if d else y_right)

    def f1_arrival(g, d):
        own = seg(1 if d else -1)
        return remote(out_v.at[g, :, own, :], out_v.at[g, :, own, :], f1_send.at[g, d], f1_recv.at[g, d],
                      y_left if d else y_right)

    def f2(g, d):
        own = seg(1 if d else -1)
        return remote(out_v.at[g, d, own, :], out_v.at[g, d, own, :], f2_send.at[g, d], f2_recv.at[g, d],
                      y_left if d else y_right)

    def f2_arrival(g, d):
        return remote(out_v.at[g, d, seg(2), :], out_v.at[g, d, seg(2), :], f2_send.at[g, d], f2_recv.at[g, d],
                      y_left if d else y_right)

    def write(g, offset, half, slot):
        c0 = pl.multiple_of((2 * g + half) * half_cols, half_cols)
        return pltpu.make_async_copy(out_v.at[g, half, seg(offset), :], out_hbm.at[seg(offset), pl.ds(c0, half_cols)],
                                     out_sem.at[g, slot, half])

    def project(g, carry):
        for half in range(2):
            c0 = pl.multiple_of((2 * g + half) * half_cols, half_cols)
            part_v[g, half] = jnp.dot(o_v[...], wo_v[:, pl.ds(c0, half_cols)], preferred_element_type=F32).astype(BF)
        for d in range(2):
            s1(g, d).start()
        for d in range(2):
            s2(g, d, 1 - d).start()
        return carry

    lax.fori_loop(0, GROUPS, project, 0)

    def add_first(g, carry):
        for d in range(2):
            s1(g, d).wait_recv()
            rs = seg(-1 if d else 1)
            part_v[g, d, rs, :] = (part_v[g, d, rs, :].astype(F32) + r1_v[g, d].astype(F32)).astype(BF)
            s2(g, d, d).start()
        return carry

    lax.fori_loop(0, GROUPS, add_first, 0)

    def add_last(g, carry):
        for d in range(2):
            for half in range(2):
                s2(g, d, half).wait_recv()
        for half in range(2):
            c0 = pl.multiple_of((2 * g + half) * half_cols, half_cols)
            attn = part_v[g, half, seg(0), :].astype(F32) + r2_v[g, 0, half].astype(F32) + r2_v[g, 1, half].astype(F32)
            out_v[g, half, seg(0), :] = (x_v[seg(0), pl.ds(c0, half_cols)].astype(F32) + attn).astype(BF)
        for d in range(2):
            f1(g, d).start()
        for half in range(2):
            write(g, 0, half, 0).start()
        return carry

    lax.fori_loop(0, GROUPS, add_last, 0)

    def pass_on(g, carry):
        for d in range(2):
            f1_arrival(g, d).wait_recv()
            f2(g, d).start()
            for half in range(2):
                write(g, 1 if d else -1, half, 1 + d).start()
        return carry

    lax.fori_loop(0, GROUPS, pass_on, 0)

    def finish(g, carry):
        for d in range(2):
            f2_arrival(g, d).wait_recv()
            write(g, 2, d, 3).start()
        return carry

    lax.fori_loop(0, GROUPS, finish, 0)

    def drain(g, carry):
        for d in range(2):
            s1(g, d).wait_send()
            for half in range(2):
                s2(g, d, half).wait_send()
            f1(g, d).wait_send()
            f2(g, d).wait_send()
        for half in range(2):
            for slot, offset in enumerate((0, -1, 1, 2)):
                write(g, offset, half, slot).wait()
        return carry

    lax.fori_loop(0, GROUPS, drain, 0)

    for copy in cache_copies:
        copy.wait()

    @pl.when(core == 0)
    def _():
        own_to(0, 1, 0, sibling).wait_send()
        own_to(0, 1, 1, sibling).wait_send()

    @pl.when(right_sends)
    def _():
        own_to(1, 0, 1, x_right).wait_send()
        own_to(1, 0, 0, x_right).wait_send()

    @pl.when(left_h0_sends)
    def _():
        own_to(2, 0, 0, x_left).wait_send()

    @pl.when(left_h1_sends)
    def _():
        own_to(2, 0, 1, x_left).wait_send()

    @pl.when(has_left)
    def _():
        fwd_sib(1, 0).wait_send()
        fwd_sib(1, 1).wait_send()

    @pl.when(has_right)
    def _():
        fwd_sib(2, 0).wait_send()
        fwd_sib(2, 1).wait_send()

    @pl.when(has_far)
    def _():
        fwd_sib(3, 0).wait_send()
        fwd_sib(3, 1).wait_send()

    @pl.when(fwd_right)
    def _():
        fwd_far(1).wait_send()

    @pl.when(fwd_left)
    def _():
        fwd_far(0).wait_send()


def solution(mesh):
    ring = mesh.shape['tp']
    if mesh.shape['cp'] != 2 * ring or ring != 4:
        raise ValueError('mesh')
    row_spec = P(('dp', 'cp'), None)
    cache_spec = P(('dp', 'cp'), 'tp', None)
    head_cols = P(None, 'tp')

    def local_block(hidden, positions, norm_gain, w_query, w_key, w_value, w_out):
        rows, width = hidden.shape
        kv_heads = w_key.shape[1] // HEAD
        q_heads = w_query.shape[1] // HEAD
        seg_rows, half_cols = rows // ring, width // (2 * GROUPS)
        cos_t, sin_t = rope_tables(positions)
        dma = pltpu.SemaphoreType.DMA
        out, k_new, v_new = pl.pallas_call(
            lambda *refs: block_kernel(ring, kv_heads, q_heads // kv_heads, *refs),
            out_shape=(
                jax.ShapeDtypeStruct((rows, width), BF),
                jax.ShapeDtypeStruct((rows, kv_heads * HEAD), BF),
                jax.ShapeDtypeStruct((rows, kv_heads * HEAD), BF),
            ),
            in_specs=[pl.BlockSpec(memory_space=pl.ANY)] + [pl.BlockSpec(memory_space=pltpu.VMEM)] * 3
            + [pl.BlockSpec(memory_space=pl.ANY)] * 4,
            out_specs=[pl.BlockSpec(memory_space=pl.ANY)] * 3,
            scratch_shapes=[
                pltpu.VMEM((rows, width), BF),
                pltpu.VMEM((rows, width), BF),
                pltpu.VMEM(w_query.shape, BF),
                pltpu.VMEM(w_key.shape, BF),
                pltpu.VMEM(w_value.shape, BF),
                pltpu.VMEM(w_out.shape, BF),
                pltpu.VMEM((q_heads, rows, HEAD), BF),
                pltpu.VMEM((4, 2, kv_heads, 2, rows, HEAD), BF),
                pltpu.VMEM((q_heads, rows, HEAD), F32),
                pltpu.VMEM((q_heads, rows, HEAD), F32),
                pltpu.VMEM((q_heads, rows, HEAD), F32),
                pltpu.VMEM((rows, q_heads * HEAD), BF),
                pltpu.VMEM((GROUPS, 2, rows, half_cols), BF),
                pltpu.VMEM((GROUPS, 2, seg_rows, half_cols), BF),
                pltpu.VMEM((GROUPS, 2, 2, seg_rows, half_cols), BF),
                pltpu.VMEM((GROUPS, 2, rows, half_cols), BF),
                dma((5,)),
                dma((kv_heads, 2)),
                dma((4, kv_heads)),
                dma((4, 2, kv_heads)),
                dma((4, kv_heads)),
                dma((GROUPS, 2)), dma((GROUPS, 2)),
                dma((GROUPS, 2, 2)), dma((GROUPS, 2, 2)),
                dma((GROUPS, 2)), dma((GROUPS, 2)),
                dma((GROUPS, 2)), dma((GROUPS, 2)),
                dma((GROUPS, 4, 2)),
            ],
            compiler_params=pltpu.CompilerParams(collective_id=0, has_side_effects=True, vmem_limit_bytes=60 * 1024 * 1024),
            name='attn_block',
        )(hidden, norm_gain.reshape(1, width), cos_t, sin_t, w_query, w_key, w_value, w_out)
        cache_shape = (rows, kv_heads, HEAD)
        return out, k_new.reshape(cache_shape), v_new.reshape(cache_shape)

    return jax.shard_map(local_block, mesh=mesh,
                         in_specs=(row_spec, P(('dp', 'cp')), P(None), head_cols, head_cols, head_cols, P('tp', None)),
                         out_specs=(row_spec, cache_spec, cache_spec), check_vma=False)
```

```python
import math
import jax
import jax.numpy as jnp
import numpy as np
from jax import lax
from jax.experimental import pallas as pl
from jax.experimental.pallas import tpu as pltpu
from jax.sharding import PartitionSpec as P

HEAD = 128
EPS = 1e-5
LOG_THETA = math.log(1000000.0)
SCORE_EXP2 = math.log2(math.e) / math.sqrt(HEAD)
BF = jnp.bfloat16
F32 = jnp.float32
GROUPS = 6
Q_TILE = 256
NORM_ROWS = 32
LOAD_CHUNKS = 4


def inverse_freq():
    half = np.exp(np.arange(HEAD // 2, dtype=np.float64) * (-2.0 * LOG_THETA / HEAD)).astype(np.float32)
    return np.concatenate([half, half])[None, :]


def block_kernel(ring, kv_heads, group_size,
                 x_hbm, pos_ref, gain_ref, freq_ref, wq_hbm, wk_hbm, wv_hbm, wo_hbm,
                 out_v, k_out, v_out,
                 x_v, h_v, wq_v, wkv_v, wo_v, cos_v, sin_v, kc_v, vc_v, q_v, kv_v, m_v, l_v, acc_v, o_v,
                 part_v, r1_v, r2_v,
                 load_sem, kv_send, kv_recv, kv_fwd_send,
                 s1_send, s1_recv, s2_send, s2_recv, f1_send, f1_recv, f2_send, f2_recv):
    rows, width = x_v.shape
    cp = lax.axis_index('cp')
    tp = lax.axis_index('tp')
    chip = cp // 2
    core = cp % 2
    seg_rows = rows // ring
    half_cols = width // (2 * GROUPS)

    x_right = {'cp': ((chip + 1) % ring) * 2 + core}
    x_left = {'cp': ((chip + ring - 1) % ring) * 2 + core}
    sibling = {'cp': chip * 2 + 1 - core}
    y_right = {'tp': (tp + 1) % ring}
    y_left = {'tp': (tp + ring - 1) % ring}

    kv_cols = kv_heads * HEAD
    chunk = rows // LOAD_CHUNKS
    x_loads = [pltpu.make_async_copy(x_hbm.at[i * chunk:(i + 1) * chunk, :], x_v.at[i * chunk:(i + 1) * chunk, :],
                                     load_sem.at[4 + i]) for i in range(LOAD_CHUNKS)]
    loads = [
        pltpu.make_async_copy(wk_hbm, wkv_v.at[:, :kv_cols], load_sem.at[0]),
        pltpu.make_async_copy(wv_hbm, wkv_v.at[:, kv_cols:], load_sem.at[1]),
        pltpu.make_async_copy(wq_hbm, wq_v, load_sem.at[2]),
        pltpu.make_async_copy(wo_hbm, wo_v, load_sem.at[3]),
    ]
    for copy in x_loads + loads[:2]:
        copy.start()

    barrier = pltpu.get_barrier_semaphore()
    for peer in (x_right, x_left, sibling, y_right, y_left):
        pl.semaphore_signal(barrier, inc=1, device_id=peer, device_id_type=pl.DeviceIdType.MESH)

    with jax.named_scope('load_wait'):
        pos = pos_ref[...].astype(F32).reshape(rows // HEAD, HEAD)
        pos = jnp.concatenate([pos, jnp.zeros((8 - rows // HEAD, HEAD), F32)], axis=0).T
        sign = jnp.where(lax.broadcasted_iota(jnp.int32, (1, HEAD), 1) < HEAD // 2, -1.0, 1.0)
        for i in range(rows // HEAD):
            angles = pos[:, i:i + 1] * freq_ref[...]
            cos_v[i * HEAD:(i + 1) * HEAD, :] = jnp.cos(angles)
            sin_v[i * HEAD:(i + 1) * HEAD, :] = jnp.sin(angles) * sign

    def norm_step(i, carry):
        r0 = pl.multiple_of(i * NORM_ROWS, NORM_ROWS)
        xf = x_v[pl.ds(r0, NORM_ROWS), :].astype(F32)
        inv = lax.rsqrt(jnp.mean(xf * xf, axis=-1, keepdims=True) + EPS)
        h_v[pl.ds(r0, NORM_ROWS), :] = (xf * inv * gain_ref[...].astype(F32).reshape(1, width)).astype(BF)
        return carry

    with jax.named_scope('norm'):
        for i in range(LOAD_CHUNKS):
            x_loads[i].wait()
            lax.fori_loop(i * chunk // NORM_ROWS, (i + 1) * chunk // NORM_ROWS, norm_step, 0)
    for copy in loads[2:]:
        copy.start()

    def rope(vals):
        return (vals * cos_v[...] + pltpu.roll(vals, HEAD // 2, 1) * sin_v[...]).astype(BF)

    for copy in loads[:2]:
        copy.wait()
    kv_scope = jax.named_scope('kv_proj')
    kv_scope.__enter__()
    kv_proj = jnp.dot(h_v[...], wkv_v[...], preferred_element_type=F32)
    for h in range(kv_heads):
        cols = slice(h * HEAD, (h + 1) * HEAD)
        k_head = rope(kv_proj[:, cols])
        kv_v[0, 0, h, 0] = k_head
        kc_v[:, cols] = k_head
        v_head = kv_proj[:, kv_cols + h * HEAD:kv_cols + (h + 1) * HEAD].astype(BF)
        vc_v[:, cols] = v_head
        for j in range(rows // HEAD):
            kv_v[0, 0, h, 1, j * HEAD:(j + 1) * HEAD, :] = v_head[j * HEAD:(j + 1) * HEAD, :].T
    kv_scope.__exit__(None, None, None)
    with jax.named_scope('barrier'):
        pl.semaphore_wait(barrier, 5)

    def remote(src, dst, send, recv, peer):
        return pltpu.make_async_remote_copy(src_ref=src, dst_ref=dst, send_sem=send, recv_sem=recv,
                                            device_id=peer, device_id_type=pl.DeviceIdType.MESH)

    def own_to(rel, cc, head, peer):
        return remote(kv_v.at[0, 0, head], kv_v.at[rel, cc, head],
                      kv_send.at[rel, head], kv_recv.at[rel, cc, head], peer)

    def fwd_far(head):
        rel, peer = (1, x_right) if head == 1 else (2, x_left)
        return remote(kv_v.at[rel, 0, head], kv_v.at[3, 0, head],
                      kv_send.at[3, head], kv_recv.at[3, 0, head], peer)

    def fwd_sib(rel, head):
        return remote(kv_v.at[rel, 0, head], kv_v.at[rel, 1, head],
                      kv_fwd_send.at[rel, head], kv_recv.at[rel, 1, head], sibling)

    right_sends = chip < ring - 1
    left_h0_sends = chip < 2
    left_h1_sends = chip < 1

    @pl.when(core == 0)
    def _():
        own_to(0, 1, 0, sibling).start()
        own_to(0, 1, 1, sibling).start()

    @pl.when(right_sends)
    def _():
        own_to(1, 0, 1, x_right).start()

    @pl.when(left_h0_sends)
    def _():
        own_to(2, 0, 0, x_left).start()

    @pl.when(right_sends)
    def _():
        own_to(1, 0, 0, x_right).start()

    @pl.when(left_h1_sends)
    def _():
        own_to(2, 0, 1, x_left).start()

    loads[2].wait()

    def q_step(j, carry):
        c0 = pl.multiple_of(j * 2 * HEAD, 2 * HEAD)
        q_proj = jnp.dot(h_v[...], wq_v[:, pl.ds(c0, 2 * HEAD)], preferred_element_type=F32)
        q_v[2 * j] = rope(q_proj[:, :HEAD]).T
        q_v[2 * j + 1] = rope(q_proj[:, HEAD:]).T
        return carry

    with jax.named_scope('q_proj'):
        lax.fori_loop(0, kv_heads * group_size // 2, q_step, 0)

    def scores(rel, cc, head, qi, r0, keys):
        return jnp.dot(kv_v[rel, cc, head, 0, :keys, :], q_v[qi, :, r0:r0 + Q_TILE], preferred_element_type=F32)

    def attend(tiles, first):
        def start(tile):
            rel, cc, head, qi, r0 = tile
            s = scores(rel, cc, head, qi, r0, r0 + Q_TILE if first else rows)
            if first:
                key_id = lax.broadcasted_iota(jnp.int32, s.shape, 0)
                row_id = lax.broadcasted_iota(jnp.int32, s.shape, 1) + r0
                s = jnp.where(key_id <= row_id, s, -jnp.inf)
            return s

        def soften(tile, s):
            rel, cc, head, qi, r0 = tile
            rs = slice(r0, r0 + Q_TILE)
            m_new = jnp.max(s, axis=0, keepdims=True)
            alpha = None
            if not first:
                m_old = m_v[qi, :, rs]
                m_new = jnp.maximum(m_old, m_new)
                alpha = jnp.exp2((m_old - m_new) * SCORE_EXP2)
            p = jnp.exp2((s - m_new) * SCORE_EXP2)
            l_new = jnp.sum(p, axis=0, keepdims=True)
            l_v[qi, :, rs] = l_new if first else l_v[qi, :, rs] * alpha + l_new
            m_v[qi, :, rs] = m_new
            return p.astype(BF), alpha

        def gather(tile, p, alpha):
            rel, cc, head, qi, r0 = tile
            rs = slice(r0, r0 + Q_TILE)
            v_t = jnp.concatenate([kv_v[rel, cc, head, 1, j * HEAD:(j + 1) * HEAD, :] for j in range(p.shape[0] // HEAD)], axis=1)
            o_new = jnp.dot(v_t, p, preferred_element_type=F32)
            acc_v[qi, :, rs] = o_new if first else acc_v[qi, :, rs] * alpha + o_new

        s = start(tiles[0])
        held = None
        for i in range(len(tiles) + 1):
            s_next = start(tiles[i + 1]) if i + 1 < len(tiles) else None
            if held is not None:
                gather(tiles[i - 1], *held)
            if i < len(tiles):
                held = soften(tiles[i], s)
            s = s_next

    def head_tiles(rel, cc, head):
        return [(rel, cc, head, head * group_size + g, rt * Q_TILE) for g in range(group_size) for rt in range(rows // Q_TILE)]

    def own_unit(head, carry):
        attend(head_tiles(0, 0, head), True)
        return carry

    with jax.named_scope('own'):
        lax.fori_loop(0, kv_heads, own_unit, 0)

    def far_unit(rel, cc, head):
        with jax.named_scope('far'):
            attend(head_tiles(rel, cc, head), False)

    has_left = chip >= 1
    has_right = chip >= 3
    has_far = chip >= 2
    fwd_right = jnp.logical_and(chip >= 1, chip <= 2)
    fwd_left = jnp.logical_or(chip == 0, chip == 3)

    def phase(p, carry):
        @pl.when(jnp.logical_and(p == 0, core == 1))
        def _():
            own_to(0, 1, 0, sibling).wait_recv()
            own_to(0, 1, 1, sibling).wait_recv()

        @pl.when(jnp.logical_and(p == 1, has_left))
        def _():
            own_to(1, 0, 1, x_right).wait_recv()

            @pl.when(fwd_right)
            def _():
                fwd_far(1).start()

            fwd_sib(1, 1).start()

        @pl.when(jnp.logical_and(p == 1, fwd_left))
        def _():
            own_to(2, 0, 0, x_left).wait_recv()
            fwd_far(0).start()

            @pl.when(has_right)
            def _():
                fwd_sib(2, 0).start()

        @pl.when(jnp.logical_and(p == 2, has_left))
        def _():
            own_to(1, 0, 0, x_right).wait_recv()
            fwd_sib(1, 0).start()

        @pl.when(jnp.logical_and(p == 2, has_right))
        def _():
            own_to(2, 0, 1, x_left).wait_recv()
            fwd_sib(2, 1).start()

        @pl.when(jnp.logical_and(p == 3, has_far))
        def _():
            fwd_far(1).wait_recv()
            fwd_sib(3, 1).start()
            fwd_far(0).wait_recv()
            fwd_sib(3, 0).start()

        def unit(i, inner):
            cc, which = i // 2, i % 2
            head = (p + which) % 2
            rel = ((p + 2) // 3) * (1 + which) + (p // 3) * (2 - which)
            need = ((p == 0) & (cc == 1) & (core == 1)) | ((rel == 1) & has_left) | ((rel == 2) & has_right) | ((rel == 3) & has_far)

            @pl.when(need & (p > 0) & (cc == 1))
            def _():
                remote(kv_v.at[rel, 0, head], kv_v.at[rel, 1, head], kv_fwd_send.at[rel, head],
                       kv_recv.at[rel, 1, head], sibling).wait_recv()

            @pl.when(need)
            def _():
                far_unit(rel, cc, head)

            return inner

        lax.fori_loop(0, 4, unit, 0)
        return carry

    with jax.named_scope('phase'):
        lax.fori_loop(0, 4, phase, 0)

    def norm_out(qi, carry):
        c0 = pl.multiple_of(qi * HEAD, HEAD)
        o_v[:, pl.ds(c0, HEAD)] = (acc_v[qi] * (1.0 / l_v[qi])).astype(BF).T
        return carry

    with jax.named_scope('norm_out'):
        lax.fori_loop(0, kv_heads * group_size, norm_out, 0)
    loads[3].wait()

    def seg(offset):
        return pl.ds(pl.multiple_of(((tp + offset + ring) % ring) * seg_rows, seg_rows), seg_rows)

    def s1(g, d):
        return remote(part_v.at[g, d, seg(2), :], r1_v.at[g, d], s1_send.at[g, d], s1_recv.at[g, d],
                      y_left if d else y_right)

    def s2(g, d, half):
        return remote(part_v.at[g, half, seg(-1 if d else 1), :], r2_v.at[g, d, half],
                      s2_send.at[g, d, half], s2_recv.at[g, d, half], y_left if d else y_right)

    def out_at(g, offset, half=None):
        c0, cols = (2 * g * half_cols, 2 * half_cols) if half is None else ((2 * g + half) * half_cols, half_cols)
        return out_v.at[seg(offset), pl.ds(pl.multiple_of(c0, half_cols), cols)]

    def f1(g, d, offset=0):
        return remote(out_at(g, offset), out_at(g, offset), f1_send.at[g, d], f1_recv.at[g, d],
                      y_left if d else y_right)

    def f2(g, d, offset):
        return remote(out_at(g, offset, d), out_at(g, offset, d), f2_send.at[g, d], f2_recv.at[g, d],
                      y_left if d else y_right)

    def project(g, carry):
        for half in range(2):
            c0 = pl.multiple_of((2 * g + half) * half_cols, half_cols)
            part_v[g, half] = jnp.dot(o_v[...], wo_v[:, pl.ds(c0, half_cols)], preferred_element_type=F32).astype(BF)
        for d in range(2):
            s1(g, d).start()
        for d in range(2):
            s2(g, d, 1 - d).start()
        return carry

    with jax.named_scope('project'):
        lax.fori_loop(0, GROUPS, project, 0)

    def add_first(g, carry):
        for d in range(2):
            s1(g, d).wait_recv()
            rs = seg(-1 if d else 1)
            part_v[g, d, rs, :] = (part_v[g, d, rs, :].astype(F32) + r1_v[g, d].astype(F32)).astype(BF)
            s2(g, d, d).start()
        return carry

    with jax.named_scope('add_first'):
        lax.fori_loop(0, GROUPS, add_first, 0)

    def add_last(g, carry):
        for d in range(2):
            for half in range(2):
                s2(g, d, half).wait_recv()
        for half in range(2):
            c0 = pl.multiple_of((2 * g + half) * half_cols, half_cols)
            attn = part_v[g, half, seg(0), :].astype(F32) + r2_v[g, 0, half].astype(F32) + r2_v[g, 1, half].astype(F32)
            out_v[seg(0), pl.ds(c0, half_cols)] = (x_v[seg(0), pl.ds(c0, half_cols)].astype(F32) + attn).astype(BF)
        for d in range(2):
            f1(g, d).start()
        return carry

    with jax.named_scope('add_last'):
        lax.fori_loop(0, GROUPS, add_last, 0)

    def pass_on(g, carry):
        for d in range(2):
            f1(g, d, 1 if d else -1).wait_recv()
            f2(g, d, 1 if d else -1).start()
        return carry

    with jax.named_scope('caches'):
        k_out[...] = kc_v[...].reshape(k_out.shape)
        v_out[...] = vc_v[...].reshape(v_out.shape)

    with jax.named_scope('pass_on'):
        lax.fori_loop(0, GROUPS, pass_on, 0)

    def finish(g, carry):
        for d in range(2):
            f2(g, d, 2).wait_recv()
        return carry

    with jax.named_scope('finish'):
        lax.fori_loop(0, GROUPS, finish, 0)

    def drain(g, carry):
        for d in range(2):
            s1(g, d).wait_send()
            for half in range(2):
                s2(g, d, half).wait_send()
            f1(g, d).wait_send()
            f2(g, d, 1 if d else -1).wait_send()
        return carry

    with jax.named_scope('drain'):
        lax.fori_loop(0, GROUPS, drain, 0)

    @pl.when(core == 0)
    def _():
        own_to(0, 1, 0, sibling).wait_send()
        own_to(0, 1, 1, sibling).wait_send()

    @pl.when(right_sends)
    def _():
        own_to(1, 0, 1, x_right).wait_send()
        own_to(1, 0, 0, x_right).wait_send()

    @pl.when(left_h0_sends)
    def _():
        own_to(2, 0, 0, x_left).wait_send()

    @pl.when(left_h1_sends)
    def _():
        own_to(2, 0, 1, x_left).wait_send()

    @pl.when(has_left)
    def _():
        fwd_sib(1, 0).wait_send()
        fwd_sib(1, 1).wait_send()

    @pl.when(has_right)
    def _():
        fwd_sib(2, 0).wait_send()
        fwd_sib(2, 1).wait_send()

    @pl.when(has_far)
    def _():
        fwd_sib(3, 0).wait_send()
        fwd_sib(3, 1).wait_send()

    @pl.when(fwd_right)
    def _():
        fwd_far(1).wait_send()

    @pl.when(fwd_left)
    def _():
        fwd_far(0).wait_send()


def solution(mesh):
    ring = mesh.shape['tp']
    if mesh.shape['cp'] != 2 * ring or ring != 4:
        raise ValueError('mesh')
    row_spec = P(('dp', 'cp'), None)
    cache_spec = P(('dp', 'cp'), 'tp', None)
    head_cols = P(None, 'tp')

    def local_block(hidden, positions, norm_gain, w_query, w_key, w_value, w_out):
        rows, width = hidden.shape
        kv_heads = w_key.shape[1] // HEAD
        q_heads = w_query.shape[1] // HEAD
        seg_rows, half_cols = rows // ring, width // (2 * GROUPS)
        dma = pltpu.SemaphoreType.DMA
        out, k_new, v_new = pl.pallas_call(
            lambda *refs: block_kernel(ring, kv_heads, q_heads // kv_heads, *refs),
            out_shape=(
                pltpu.VMEM((rows, width), BF),
                pltpu.VMEM((rows, kv_heads, HEAD), BF),
                pltpu.VMEM((rows, kv_heads, HEAD), BF),
            ),
            in_specs=[pl.BlockSpec(memory_space=pl.ANY)] + [pl.BlockSpec(memory_space=pltpu.VMEM)] * 3
            + [pl.BlockSpec(memory_space=pl.ANY)] * 4,
            out_specs=[pl.BlockSpec(memory_space=pltpu.VMEM)] * 3,
            scratch_shapes=[
                pltpu.VMEM((rows, width), BF),
                pltpu.VMEM((rows, width), BF),
                pltpu.VMEM(w_query.shape, BF),
                pltpu.VMEM((width, 2 * kv_heads * HEAD), BF),
                pltpu.VMEM(w_out.shape, BF),
                pltpu.VMEM((rows, HEAD), F32),
                pltpu.VMEM((rows, HEAD), F32),
                pltpu.VMEM((rows, kv_heads * HEAD), BF),
                pltpu.VMEM((rows, kv_heads * HEAD), BF),
                pltpu.VMEM((q_heads, HEAD, rows), BF),
                pltpu.VMEM((4, 2, kv_heads, 2, rows, HEAD), BF),
                pltpu.VMEM((q_heads, 1, rows), F32),
                pltpu.VMEM((q_heads, 1, rows), F32),
                pltpu.VMEM((q_heads, HEAD, rows), F32),
                pltpu.VMEM((rows, q_heads * HEAD), BF),
                pltpu.VMEM((GROUPS, 2, rows, half_cols), BF),
                pltpu.VMEM((GROUPS, 2, seg_rows, half_cols), BF),
                pltpu.VMEM((GROUPS, 2, 2, seg_rows, half_cols), BF),
                dma((4 + LOAD_CHUNKS,)),
                dma((4, kv_heads)),
                dma((4, 2, kv_heads)),
                dma((4, kv_heads)),
                dma((GROUPS, 2)), dma((GROUPS, 2)),
                dma((GROUPS, 2, 2)), dma((GROUPS, 2, 2)),
                dma((GROUPS, 2)), dma((GROUPS, 2)),
                dma((GROUPS, 2)), dma((GROUPS, 2)),
            ],
            compiler_params=pltpu.CompilerParams(collective_id=0, has_side_effects=True, vmem_limit_bytes=60 * 1024 * 1024),
            name='attn_block',
        )(hidden, positions, norm_gain, jnp.asarray(inverse_freq()), w_query, w_key, w_value, w_out)
        return out, k_new, v_new

    return jax.shard_map(local_block, mesh=mesh,
                         in_specs=(row_spec, P(('dp', 'cp')), P(None), head_cols, head_cols, head_cols, P('tp', None)),
                         out_specs=(row_spec, cache_spec, cache_spec), check_vma=False)
```

```python
import math
import jax
import jax.numpy as jnp
import numpy as np
from jax import lax
from jax.experimental import pallas as pl
from jax.experimental.pallas import tpu as pltpu
from jax.sharding import PartitionSpec as P

HEAD = 128
EPS = 1e-5
LOG_THETA = math.log(1000000.0)
SCORE_EXP2 = math.log2(math.e) / math.sqrt(HEAD)
BF = jnp.bfloat16
F32 = jnp.float32
CHUNKS = 3
Q_TILE = 256
NORM_ROWS = 32
LOAD_CHUNKS = 4


def inverse_freq():
    half = np.exp(np.arange(HEAD // 2, dtype=np.float64) * (-2.0 * LOG_THETA / HEAD)).astype(np.float32)
    return np.concatenate([half, half])[None, :]


def block_kernel(ring, kv_heads, group_size,
                 x_hbm, pos_ref, gain_ref, freq_ref, wq_hbm, wk_hbm, wv_hbm, wo_hbm,
                 out_v, k_out, v_out,
                 x_v, h_v, wq_v, wkv_v, wo_v, cos_v, sin_v, kc_v, vc_v, q_v, kv_v, m_v, l_v, acc_v, o_v,
                 wox_v, ox_v, part_v, recv_v,
                 load_sem, kv_send, kv_recv, kv_fwd_send,
                 wo_send, wo_recv, wo_fwd_send, wo_fwd_recv, o_send, o_recv, part_send, part_recv,
                 f1_send, f1_recv, f2_send, f2_recv):
    rows, width = x_v.shape
    cp = lax.axis_index('cp')
    tp = lax.axis_index('tp')
    chip = cp // 2
    core = cp % 2
    seg_rows = rows // ring
    half = width // 2
    cols = half // CHUNKS
    k_half = wo_v.shape[0] // 2

    x_right = {'cp': ((chip + 1) % ring) * 2 + core}
    x_left = {'cp': ((chip + ring - 1) % ring) * 2 + core}
    sibling = {'cp': chip * 2 + 1 - core}
    y_right = {'tp': (tp + 1) % ring}
    y_left = {'tp': (tp + ring - 1) % ring}
    turn = 1 - 2 * (tp % 2)
    y_mate = ({'tp': (tp + ring + turn) % ring}, {'tp': (tp + ring - turn) % ring})

    kv_cols = kv_heads * HEAD
    chunk = rows // LOAD_CHUNKS
    x_loads = [pltpu.make_async_copy(x_hbm.at[i * chunk:(i + 1) * chunk, :], x_v.at[i * chunk:(i + 1) * chunk, :],
                                     load_sem.at[4 + i]) for i in range(LOAD_CHUNKS)]
    loads = [
        pltpu.make_async_copy(wk_hbm, wkv_v.at[:, :kv_cols], load_sem.at[0]),
        pltpu.make_async_copy(wv_hbm, wkv_v.at[:, kv_cols:], load_sem.at[1]),
        pltpu.make_async_copy(wq_hbm, wq_v, load_sem.at[2]),
        pltpu.make_async_copy(wo_hbm, wo_v, load_sem.at[3]),
    ]
    for copy in x_loads + loads[:2]:
        copy.start()

    barrier = pltpu.get_barrier_semaphore()
    for peer in (x_right, x_left, sibling, y_right, y_left):
        pl.semaphore_signal(barrier, inc=1, device_id=peer, device_id_type=pl.DeviceIdType.MESH)

    with jax.named_scope('load_wait'):
        pos = pos_ref[...].astype(F32).reshape(rows // HEAD, HEAD)
        pos = jnp.concatenate([pos, jnp.zeros((8 - rows // HEAD, HEAD), F32)], axis=0).T
        sign = jnp.where(lax.broadcasted_iota(jnp.int32, (1, HEAD), 1) < HEAD // 2, -1.0, 1.0)
        for i in range(rows // HEAD):
            angles = pos[:, i:i + 1] * freq_ref[...]
            cos_v[i * HEAD:(i + 1) * HEAD, :] = jnp.cos(angles)
            sin_v[i * HEAD:(i + 1) * HEAD, :] = jnp.sin(angles) * sign

    def remote(src, dst, send, recv, peer):
        return pltpu.make_async_remote_copy(src_ref=src, dst_ref=dst, send_sem=send, recv_sem=recv,
                                            device_id=peer, device_id_type=pl.DeviceIdType.MESH)

    with jax.named_scope('barrier'):
        pl.semaphore_wait(barrier, 5)

    def wo_part(c):
        return remote(wo_hbm.at[pl.ds(pl.multiple_of(core * k_half, k_half), k_half), c * half:(c + 1) * half],
                      wox_v.at[c, pl.ds(pl.multiple_of(core * k_half, k_half), k_half), :],
                      wo_send.at[c], wo_recv.at[c], y_mate[c])

    def wo_share(c, from_core):
        part = wox_v.at[c, pl.ds(pl.multiple_of(from_core * k_half, k_half), k_half), :]
        return remote(part, part, wo_fwd_send.at[c], wo_fwd_recv.at[c], sibling)

    for c in range(2):
        wo_part(c).start()

    def norm_step(i, carry):
        r0 = pl.multiple_of(i * NORM_ROWS, NORM_ROWS)
        xf = x_v[pl.ds(r0, NORM_ROWS), :].astype(F32)
        inv = lax.rsqrt(jnp.mean(xf * xf, axis=-1, keepdims=True) + EPS)
        h_v[pl.ds(r0, NORM_ROWS), :] = (xf * inv * gain_ref[...].astype(F32).reshape(1, width)).astype(BF)
        return carry

    with jax.named_scope('norm'):
        for i in range(LOAD_CHUNKS):
            x_loads[i].wait()
            lax.fori_loop(i * chunk // NORM_ROWS, (i + 1) * chunk // NORM_ROWS, norm_step, 0)
    for copy in loads[2:]:
        copy.start()

    def rope(vals):
        return (vals * cos_v[...] + pltpu.roll(vals, HEAD // 2, 1) * sin_v[...]).astype(BF)

    for copy in loads[:2]:
        copy.wait()
    kv_scope = jax.named_scope('kv_proj')
    kv_scope.__enter__()
    kv_proj = jnp.dot(h_v[...], wkv_v[...], preferred_element_type=F32)
    for h in range(kv_heads):
        hc = slice(h * HEAD, (h + 1) * HEAD)
        k_head = rope(kv_proj[:, hc])
        kv_v[0, 0, h, 0] = k_head
        kc_v[:, hc] = k_head
        v_head = kv_proj[:, kv_cols + h * HEAD:kv_cols + (h + 1) * HEAD].astype(BF)
        vc_v[:, hc] = v_head
        for j in range(rows // HEAD):
            kv_v[0, 0, h, 1, j * HEAD:(j + 1) * HEAD, :] = v_head[j * HEAD:(j + 1) * HEAD, :].T
    kv_scope.__exit__(None, None, None)

    def own_to(rel, cc, head, peer):
        return remote(kv_v.at[0, 0, head], kv_v.at[rel, cc, head],
                      kv_send.at[rel, head], kv_recv.at[rel, cc, head], peer)

    def fwd_far(head):
        rel, peer = (1, x_right) if head == 1 else (2, x_left)
        return remote(kv_v.at[rel, 0, head], kv_v.at[3, 0, head],
                      kv_send.at[3, head], kv_recv.at[3, 0, head], peer)

    def fwd_sib(rel, head):
        return remote(kv_v.at[rel, 0, head], kv_v.at[rel, 1, head],
                      kv_fwd_send.at[rel, head], kv_recv.at[rel, 1, head], sibling)

    right_sends = chip < ring - 1
    left_h0_sends = chip < 2
    left_h1_sends = chip < 1

    @pl.when(core == 0)
    def _():
        own_to(0, 1, 0, sibling).start()
        own_to(0, 1, 1, sibling).start()

    @pl.when(right_sends)
    def _():
        own_to(1, 0, 1, x_right).start()

    @pl.when(left_h0_sends)
    def _():
        own_to(2, 0, 0, x_left).start()

    @pl.when(right_sends)
    def _():
        own_to(1, 0, 0, x_right).start()

    @pl.when(left_h1_sends)
    def _():
        own_to(2, 0, 1, x_left).start()

    loads[2].wait()

    def q_step(j, carry):
        c0 = pl.multiple_of(j * 2 * HEAD, 2 * HEAD)
        q_proj = jnp.dot(h_v[...], wq_v[:, pl.ds(c0, 2 * HEAD)], preferred_element_type=F32)
        q_v[2 * j] = rope(q_proj[:, :HEAD]).T
        q_v[2 * j + 1] = rope(q_proj[:, HEAD:]).T
        return carry

    with jax.named_scope('q_proj'):
        lax.fori_loop(0, kv_heads * group_size // 2, q_step, 0)

    def attend(tiles, first):
        def start(tile):
            rel, ccs, head, qi, rs, r0 = tile
            keys = r0 + Q_TILE if first else rows
            q_t = q_v[qi, :, rs]
            s = jnp.concatenate([jnp.dot(kv_v[rel, cc, head, 0, :keys, :], q_t, preferred_element_type=F32) for cc in ccs], axis=0)
            if first:
                key_id = lax.broadcasted_iota(jnp.int32, s.shape, 0)
                row_id = lax.broadcasted_iota(jnp.int32, s.shape, 1) + r0
                s = jnp.where(key_id <= row_id, s, -jnp.inf)
            return s

        def soften(tile, s):
            rel, ccs, head, qi, rs, r0 = tile
            m_new = jnp.max(s, axis=0, keepdims=True)
            alpha = None
            if not first:
                m_old = m_v[qi, :, rs]
                m_new = jnp.maximum(m_old, m_new)
                alpha = jnp.exp2((m_old - m_new) * SCORE_EXP2)
            p = jnp.exp2((s - m_new) * SCORE_EXP2)
            l_new = jnp.sum(p, axis=0, keepdims=True)
            l_v[qi, :, rs] = l_new if first else l_v[qi, :, rs] * alpha + l_new
            m_v[qi, :, rs] = m_new
            return p.astype(BF), alpha

        def gather(tile, p, alpha):
            rel, ccs, head, qi, rs, r0 = tile
            keys = r0 + Q_TILE if first else rows
            v_t = jnp.concatenate([kv_v[rel, cc, head, 1, j * HEAD:(j + 1) * HEAD, :] for cc in ccs for j in range(keys // HEAD)], axis=1)
            o_new = jnp.dot(v_t, p, preferred_element_type=F32)
            acc_v[qi, :, rs] = o_new if first else acc_v[qi, :, rs] * alpha + o_new

        s = start(tiles[0])
        held = None
        for i in range(len(tiles) + 1):
            s_next = start(tiles[i + 1]) if i + 1 < len(tiles) else None
            if held is not None:
                gather(tiles[i - 1], *held)
            if i < len(tiles):
                held = soften(tiles[i], s)
            s = s_next

    def head_tiles(rel, cc, head):
        return [(rel, (cc,), head, head * group_size + g, slice(rt * Q_TILE, (rt + 1) * Q_TILE), rt * Q_TILE)
                for g in range(group_size) for rt in range(rows // Q_TILE)]

    def own_unit(head, carry):
        attend(head_tiles(0, 0, head), True)
        return carry

    with jax.named_scope('own'):
        lax.fori_loop(0, kv_heads, own_unit, 0)

    def far_unit(rel, cc, head):
        with jax.named_scope('far'):
            attend(head_tiles(rel, cc, head), False)

    has_left = chip >= 1
    has_right = chip >= 3
    has_far = chip >= 2
    fwd_right = jnp.logical_and(chip >= 1, chip <= 2)
    fwd_left = jnp.logical_or(chip == 0, chip == 3)

    def phase(p, carry):
        @pl.when(jnp.logical_and(p == 0, core == 1))
        def _():
            own_to(0, 1, 0, sibling).wait_recv()
            own_to(0, 1, 1, sibling).wait_recv()

        @pl.when(jnp.logical_and(p == 1, has_left))
        def _():
            own_to(1, 0, 1, x_right).wait_recv()

            @pl.when(fwd_right)
            def _():
                fwd_far(1).start()

            fwd_sib(1, 1).start()

        @pl.when(jnp.logical_and(p == 1, fwd_left))
        def _():
            own_to(2, 0, 0, x_left).wait_recv()
            fwd_far(0).start()

            @pl.when(has_right)
            def _():
                fwd_sib(2, 0).start()

        @pl.when(jnp.logical_and(p == 2, has_left))
        def _():
            own_to(1, 0, 0, x_right).wait_recv()
            fwd_sib(1, 0).start()

        @pl.when(jnp.logical_and(p == 2, has_right))
        def _():
            own_to(2, 0, 1, x_left).wait_recv()
            fwd_sib(2, 1).start()

        def unit(i, inner):
            cc, which = i // 2, i % 2

            @pl.when(jnp.logical_and(jnp.logical_and(p == 2, i == 3), has_far))
            def _():
                fwd_far(1).wait_recv()
                fwd_sib(3, 1).start()
                fwd_far(0).wait_recv()
                fwd_sib(3, 0).start()

            head = (p + which) % 2
            rel = ((p + 1) // 2) * (1 + which)
            need = ((p == 0) & (cc == 1) & (core == 1)) | ((rel == 1) & has_left) | ((rel == 2) & has_right)

            @pl.when(need & (p > 0) & (cc == 1))
            def _():
                remote(kv_v.at[rel, 0, head], kv_v.at[rel, 1, head], kv_fwd_send.at[rel, head],
                       kv_recv.at[rel, 1, head], sibling).wait_recv()

            @pl.when(need)
            def _():
                far_unit(rel, cc, head)

            return inner

        lax.fori_loop(0, 4, unit, 0)
        return carry

    with jax.named_scope('phase'):
        lax.fori_loop(0, 3, phase, 0)

    def seg(index):
        return pl.ds(pl.multiple_of(index * seg_rows, seg_rows), seg_rows)

    own_seg, far_seg = tp, (tp + 2) % ring
    mate_seg = ((tp + ring + turn) % ring, (tp + ring - turn) % ring)

    def o_part(c, which):
        return remote(o_v.at[seg(mate_seg[c] if which else far_seg), :], ox_v.at[c, which],
                      o_send.at[c, which], o_recv.at[c, which], y_mate[c])

    @pl.when(has_far)
    def _():
        for head in range(kv_heads):
            remote(kv_v.at[3, 0, head], kv_v.at[3, 1, head], kv_fwd_send.at[3, head], kv_recv.at[3, 1, head], sibling).wait_recv()

    loads[3].wait()

    def seg_step(j, carry):
        index = (tp + ring + 2 * ((3 - j) // 3) + turn * ((j % 3) % 2) - turn * (j // 2 - j // 3)) % ring
        rs = seg(index)

        @pl.when(has_far)
        def _():
            with jax.named_scope('far_seg'):
                attend([(3, (0, 1), head, head * group_size + g, rs, 0) for head in range(kv_heads) for g in range(group_size)], False)

        for qi in range(kv_heads * group_size):
            o_v[rs, qi * HEAD:(qi + 1) * HEAD] = (acc_v[qi, :, rs] * (1.0 / l_v[qi, :, rs])).astype(BF).T

        @pl.when(j == 0)
        def _():
            for c in range(2):
                o_part(c, 0).start()

        @pl.when(j == 1)
        def _():
            o_part(0, 1).start()
            with jax.named_scope('wo_wait'):
                for c in range(2):
                    wo_part(c).wait_recv()
                    wo_share(c, core).start()

        @pl.when(j == 2)
        def _():
            o_part(1, 1).start()

        return carry

    with jax.named_scope('segs'):
        lax.fori_loop(0, ring, seg_step, 0)

    def col(c, g):
        return pl.ds(pl.multiple_of(c * half + g * cols, cols), cols)

    def two_mates(c, g, own_rows, which):
        g0 = pl.multiple_of(g * cols, cols)
        return (jnp.dot(o_v[seg(own_rows), :], wo_v[:, col(c, g)], preferred_element_type=F32)
                + jnp.dot(ox_v[c, which], wox_v[c, :, pl.ds(g0, cols)], preferred_element_type=F32))

    def cross(c, g):
        return remote(part_v.at[c, g], recv_v.at[c, g], part_send.at[c, g], part_recv.at[c, g], y_mate[1 - c])

    def f1(c, g, d, owner):
        block = out_v.at[seg(owner), col(c, g)]
        return remote(block, block, f1_send.at[c, g, d], f1_recv.at[c, g, d], y_left if d else y_right)

    def f2(g, d, owner):
        block = out_v.at[seg(owner), col(d, g)]
        return remote(block, block, f2_send.at[g, d], f2_recv.at[g, d], y_left if d else y_right)

    with jax.named_scope('mates'):
        for c in range(2):
            wo_share(c, 1 - core).wait_recv()
            o_part(c, 0).wait_recv()

    def project_cross(g, carry):
        for c in range(2):
            part_v[c, g] = two_mates(c, g, mate_seg[1 - c], 0).astype(BF)
            cross(c, g).start()
        return carry

    with jax.named_scope('cross'):
        lax.fori_loop(0, CHUNKS, project_cross, 0)

    with jax.named_scope('caches'):
        k_out[...] = kc_v[...].reshape(k_out.shape)
        v_out[...] = vc_v[...].reshape(v_out.shape)

    for c in range(2):
        o_part(c, 1).wait_recv()

    def project_own(g, carry):
        for c in range(2):
            attn = two_mates(c, g, own_seg, 1)
            cross(c, g).wait_recv()
            attn = attn + recv_v[c, g].astype(F32)
            out_v[seg(own_seg), col(c, g)] = (x_v[seg(own_seg), col(c, g)].astype(F32) + attn).astype(BF)
            for d in range(2):
                f1(c, g, d, own_seg).start()
        return carry

    with jax.named_scope('own_out'):
        lax.fori_loop(0, CHUNKS, project_own, 0)

    side_seg = ((tp + ring - 1) % ring, (tp + 1) % ring)

    def pass_on(g, carry):
        for d in range(2):
            f1(d, g, d, side_seg[d]).wait_recv()
            f2(g, d, side_seg[d]).start()
        return carry

    with jax.named_scope('pass_on'):
        lax.fori_loop(0, CHUNKS, pass_on, 0)

    def finish(g, carry):
        for d in range(2):
            f1(1 - d, g, d, side_seg[d]).wait_recv()
            f2(g, d, far_seg).wait_recv()
        return carry

    with jax.named_scope('finish'):
        lax.fori_loop(0, CHUNKS, finish, 0)

    def drain(g, carry):
        for d in range(2):
            cross(d, g).wait_send()
            f2(g, d, side_seg[d]).wait_send()
            for c in range(2):
                f1(c, g, d, own_seg).wait_send()
        return carry

    with jax.named_scope('drain'):
        lax.fori_loop(0, CHUNKS, drain, 0)
    for c in range(2):
        wo_part(c).wait_send()
        wo_share(c, core).wait_send()
        for which in range(2):
            o_part(c, which).wait_send()

    @pl.when(core == 0)
    def _():
        own_to(0, 1, 0, sibling).wait_send()
        own_to(0, 1, 1, sibling).wait_send()

    @pl.when(right_sends)
    def _():
        own_to(1, 0, 1, x_right).wait_send()
        own_to(1, 0, 0, x_right).wait_send()

    @pl.when(left_h0_sends)
    def _():
        own_to(2, 0, 0, x_left).wait_send()

    @pl.when(left_h1_sends)
    def _():
        own_to(2, 0, 1, x_left).wait_send()

    @pl.when(has_left)
    def _():
        fwd_sib(1, 0).wait_send()
        fwd_sib(1, 1).wait_send()

    @pl.when(has_right)
    def _():
        fwd_sib(2, 0).wait_send()
        fwd_sib(2, 1).wait_send()

    @pl.when(has_far)
    def _():
        fwd_sib(3, 0).wait_send()
        fwd_sib(3, 1).wait_send()

    @pl.when(fwd_right)
    def _():
        fwd_far(1).wait_send()

    @pl.when(fwd_left)
    def _():
        fwd_far(0).wait_send()


def solution(mesh):
    ring = mesh.shape['tp']
    if mesh.shape['cp'] != 2 * ring or ring != 4:
        raise ValueError('mesh')
    row_spec = P(('dp', 'cp'), None)
    cache_spec = P(('dp', 'cp'), 'tp', None)
    head_cols = P(None, 'tp')

    def local_block(hidden, positions, norm_gain, w_query, w_key, w_value, w_out):
        rows, width = hidden.shape
        kv_heads = w_key.shape[1] // HEAD
        q_heads = w_query.shape[1] // HEAD
        seg_rows, half = rows // ring, width // 2
        cols = half // CHUNKS
        dma = pltpu.SemaphoreType.DMA
        out, k_new, v_new = pl.pallas_call(
            lambda *refs: block_kernel(ring, kv_heads, q_heads // kv_heads, *refs),
            out_shape=(
                pltpu.VMEM((rows, width), BF),
                pltpu.VMEM((rows, kv_heads, HEAD), BF),
                pltpu.VMEM((rows, kv_heads, HEAD), BF),
            ),
            in_specs=[pl.BlockSpec(memory_space=pl.ANY)] + [pl.BlockSpec(memory_space=pltpu.VMEM)] * 3
            + [pl.BlockSpec(memory_space=pl.ANY)] * 4,
            out_specs=[pl.BlockSpec(memory_space=pltpu.VMEM)] * 3,
            scratch_shapes=[
                pltpu.VMEM((rows, width), BF),
                pltpu.VMEM((rows, width), BF),
                pltpu.VMEM(w_query.shape, BF),
                pltpu.VMEM((width, 2 * kv_heads * HEAD), BF),
                pltpu.VMEM(w_out.shape, BF),
                pltpu.VMEM((rows, HEAD), F32),
                pltpu.VMEM((rows, HEAD), F32),
                pltpu.VMEM((rows, kv_heads * HEAD), BF),
                pltpu.VMEM((rows, kv_heads * HEAD), BF),
                pltpu.VMEM((q_heads, HEAD, rows), BF),
                pltpu.VMEM((4, 2, kv_heads, 2, rows, HEAD), BF),
                pltpu.VMEM((q_heads, 1, rows), F32),
                pltpu.VMEM((q_heads, 1, rows), F32),
                pltpu.VMEM((q_heads, HEAD, rows), F32),
                pltpu.VMEM((rows, q_heads * HEAD), BF),
                pltpu.VMEM((2, q_heads * HEAD, half), BF),
                pltpu.VMEM((2, 2, seg_rows, q_heads * HEAD), BF),
                pltpu.VMEM((2, CHUNKS, seg_rows, cols), BF),
                pltpu.VMEM((2, CHUNKS, seg_rows, cols), BF),
                dma((4 + LOAD_CHUNKS,)),
                dma((4, kv_heads)),
                dma((4, 2, kv_heads)),
                dma((4, kv_heads)),
                dma((2,)), dma((2,)), dma((2,)), dma((2,)),
                dma((2, 2)), dma((2, 2)),
                dma((2, CHUNKS)), dma((2, CHUNKS)),
                dma((2, CHUNKS, 2)), dma((2, CHUNKS, 2)),
                dma((CHUNKS, 2)), dma((CHUNKS, 2)),
            ],
            compiler_params=pltpu.CompilerParams(collective_id=0, has_side_effects=True, vmem_limit_bytes=60 * 1024 * 1024),
            name='attn_block',
        )(hidden, positions, norm_gain, jnp.asarray(inverse_freq()), w_query, w_key, w_value, w_out)
        return out, k_new, v_new

    return jax.shard_map(local_block, mesh=mesh,
                         in_specs=(row_spec, P(('dp', 'cp')), P(None), head_cols, head_cols, head_cols, P('tp', None)),
                         out_specs=(row_spec, cache_spec, cache_spec), check_vma=False)
```

```python
import math
import jax
import jax.numpy as jnp
import numpy as np
from jax import lax
from jax.experimental import pallas as pl
from jax.experimental.pallas import tpu as pltpu
from jax.sharding import PartitionSpec as P

HEAD = 128
EPS = 1e-5
LOG_THETA = math.log(1000000.0)
SCORE_EXP2 = math.log2(math.e) / math.sqrt(HEAD)
BF = jnp.bfloat16
F32 = jnp.float32
CHUNKS = 3
Q_TILE = 256
NORM_ROWS = 32
LOAD_CHUNKS = 4
SHARED_ROWS = 128


def inverse_freq():
    half = np.exp(np.arange(HEAD // 2, dtype=np.float64) * (-2.0 * LOG_THETA / HEAD)).astype(np.float32)
    return np.concatenate([half, half])[None, :]


def block_kernel(ring, kv_heads, group_size,
                 x_hbm, pos_ref, gain_ref, freq_ref, wq_hbm, wk_hbm, wv_hbm, wo_hbm,
                 out_v, k_out, v_out,
                 x_v, h_v, wq_v, wkv_v, wo_v, cos_v, sin_v, kc_v, vc_v, q_v, kv_v, m_v, l_v, acc_v, o_v,
                 wox_v, ox_v, part_v, recv_v,
                 load_sem, kv_send, kv_recv, kv_fwd_send,
                 wo_send, wo_recv, wx_send, wx_recv, wf_send, wf_recv, wo_fwd_send, wo_fwd_recv, o_send, o_recv, part_send, part_recv,
                 f1_send, f1_recv, f2_send, f2_recv):
    rows, width = x_v.shape
    cp = lax.axis_index('cp')
    tp = lax.axis_index('tp')
    chip = cp // 2
    core = cp % 2
    seg_rows = rows // ring
    half = width // 2
    cols = half // CHUNKS
    k_half = wo_v.shape[0] // 2

    x_right = {'cp': ((chip + 1) % ring) * 2 + core}
    x_left = {'cp': ((chip + ring - 1) % ring) * 2 + core}
    sibling = {'cp': chip * 2 + 1 - core}
    y_right = {'tp': (tp + 1) % ring}
    y_left = {'tp': (tp + ring - 1) % ring}
    turn = 1 - 2 * (tp % 2)
    y_mate = ({'tp': (tp + ring + turn) % ring}, {'tp': (tp + ring - turn) % ring})

    kv_cols = kv_heads * HEAD
    chunk = rows // LOAD_CHUNKS
    x_loads = [pltpu.make_async_copy(x_hbm.at[i * chunk:(i + 1) * chunk, :], x_v.at[i * chunk:(i + 1) * chunk, :],
                                     load_sem.at[4 + i]) for i in range(LOAD_CHUNKS)]
    loads = [
        pltpu.make_async_copy(wk_hbm, wkv_v.at[:, :kv_cols], load_sem.at[0]),
        pltpu.make_async_copy(wv_hbm, wkv_v.at[:, kv_cols:], load_sem.at[1]),
        pltpu.make_async_copy(wq_hbm, wq_v, load_sem.at[2]),
        pltpu.make_async_copy(wo_hbm, wo_v, load_sem.at[3]),
    ]
    for copy in x_loads[:1] + loads[:2] + x_loads[1:] + loads[2:3]:
        copy.start()

    barrier = pltpu.get_barrier_semaphore()
    for peer in (x_right, x_left, sibling, y_right, y_left):
        pl.semaphore_signal(barrier, inc=1, device_id=peer, device_id_type=pl.DeviceIdType.MESH)

    with jax.named_scope('load_wait'):
        pos = pos_ref[...].astype(F32).reshape(rows // HEAD, HEAD)
        pos = jnp.concatenate([pos, jnp.zeros((8 - rows // HEAD, HEAD), F32)], axis=0).T
        sign = jnp.where(lax.broadcasted_iota(jnp.int32, (1, HEAD), 1) < HEAD // 2, -1.0, 1.0)
        for i in range(rows // HEAD):
            angles = pos[:, i:i + 1] * freq_ref[...]
            cos_v[i * HEAD:(i + 1) * HEAD, :] = jnp.cos(angles)
            sin_v[i * HEAD:(i + 1) * HEAD, :] = jnp.sin(angles) * sign

    def remote(src, dst, send, recv, peer):
        return pltpu.make_async_remote_copy(src_ref=src, dst_ref=dst, send_sem=send, recv_sem=recv,
                                            device_id=peer, device_id_type=pl.DeviceIdType.MESH)

    with jax.named_scope('barrier'):
        pl.semaphore_wait(barrier, 5)

    base = core * k_half
    direct_rows = k_half - SHARED_ROWS
    sub_rows = SHARED_ROWS // ring

    def sub_at(c, index):
        return wox_v.at[c, pl.ds(pl.multiple_of(base + direct_rows + index * sub_rows, sub_rows), sub_rows), :]

    def wo_part(c, kind):
        start, count = (base, direct_rows) if kind == 0 else (base + direct_rows + chip * sub_rows, sub_rows)
        ks = pl.ds(pl.multiple_of(start, sub_rows), count)
        return remote(wo_hbm.at[ks, c * half:(c + 1) * half], wox_v.at[c, ks, :],
                      wo_send.at[c, kind], wo_recv.at[c, kind], y_mate[c])

    def wx_own(d, c, index):
        return remote(sub_at(c, index), sub_at(c, index), wx_send.at[d, c], wx_recv.at[d, c], x_left if d else x_right)

    def wx_pass(c, index):
        return remote(sub_at(c, index), sub_at(c, index), wf_send.at[c], wf_recv.at[c], x_left if c else x_right)

    def wo_share(c, kind, from_core):
        start = from_core * k_half + kind * direct_rows
        part = wox_v.at[c, pl.ds(pl.multiple_of(start, sub_rows), SHARED_ROWS if kind else direct_rows), :]
        return remote(part, part, wo_fwd_send.at[c, kind], wo_fwd_recv.at[c, kind], sibling)

    chip_left, chip_right, chip_far = (chip + ring - 1) % ring, (chip + 1) % ring, (chip + 2) % ring

    for c in range(2):
        wo_part(c, 1).start()
    for c in range(2):
        wo_part(c, 0).start()

    def norm_step(i, carry):
        r0 = pl.multiple_of(i * NORM_ROWS, NORM_ROWS)
        xf = x_v[pl.ds(r0, NORM_ROWS), :].astype(F32)
        inv = lax.rsqrt(jnp.mean(xf * xf, axis=-1, keepdims=True) + EPS)
        h_v[pl.ds(r0, NORM_ROWS), :] = (xf * inv * gain_ref[...].astype(F32).reshape(1, width)).astype(BF)
        return carry

    def rope(vals, rs=slice(None)):
        return (vals * cos_v[rs, :] + pltpu.roll(vals, HEAD // 2, 1) * sin_v[rs, :]).astype(BF)

    def own_to(rel, cc, head, peer):
        return remote(kv_v.at[0, 0, head], kv_v.at[rel, cc, head],
                      kv_send.at[rel, head], kv_recv.at[rel, cc, head], peer)

    def own_chunk(rel, cc, head, peer, i):
        ks = slice(i * chunk, (i + 1) * chunk)
        return remote(kv_v.at[0, 0, head, :, ks, :], kv_v.at[rel, cc, head, :, ks, :],
                      kv_send.at[rel, head], kv_recv.at[rel, cc, head], peer)

    def fwd_far(head):
        rel, peer = (1, x_right) if head == 1 else (2, x_left)
        return remote(kv_v.at[rel, 0, head], kv_v.at[3, 0, head],
                      kv_send.at[3, head], kv_recv.at[3, 0, head], peer)

    def fwd_sib(rel, head):
        return remote(kv_v.at[rel, 0, head], kv_v.at[rel, 1, head],
                      kv_fwd_send.at[rel, head], kv_recv.at[rel, 1, head], sibling)

    right_sends = chip < ring - 1
    left_h0_sends = chip < 2
    left_h1_sends = chip < 1


    for i in range(LOAD_CHUNKS):
        x_loads[i].wait()
        with jax.named_scope('norm'):
            lax.fori_loop(i * chunk // NORM_ROWS, (i + 1) * chunk // NORM_ROWS, norm_step, 0)
        if i == 0:
            for copy in loads[:2]:
                copy.wait()
        ks = slice(i * chunk, (i + 1) * chunk)
        with jax.named_scope('kv_proj'):
            kv_proj = jnp.dot(h_v[ks, :], wkv_v[...], preferred_element_type=F32)
            for h in range(kv_heads):
                hc = slice(h * HEAD, (h + 1) * HEAD)
                k_head = rope(kv_proj[:, hc], ks)
                kv_v[0, 0, h, 0, ks, :] = k_head
                kc_v[ks, hc] = k_head
                v_head = kv_proj[:, kv_cols + h * HEAD:kv_cols + (h + 1) * HEAD].astype(BF)
                vc_v[ks, hc] = v_head
                kv_v[0, 0, h, 1, ks, :] = v_head.T

        @pl.when(right_sends)
        def _(i=i):
            own_chunk(1, 0, 1, x_right, i).start()

        @pl.when(left_h0_sends)
        def _(i=i):
            own_chunk(2, 0, 0, x_left, i).start()

    loads[3].start()

    @pl.when(core == 0)
    def _():
        own_to(0, 1, 0, sibling).start()
        own_to(0, 1, 1, sibling).start()

    @pl.when(right_sends)
    def _():
        own_to(1, 0, 0, x_right).start()

    @pl.when(left_h1_sends)
    def _():
        own_to(2, 0, 1, x_left).start()

    loads[2].wait()

    with jax.named_scope('q_proj'):
        q_pair = None
        for j in range(kv_heads * group_size // 2 + 1):
            last = q_pair
            if j < kv_heads * group_size // 2:
                q_pair = jnp.dot(h_v[...], wq_v[:, j * 2 * HEAD:(j + 1) * 2 * HEAD], preferred_element_type=F32)
            if j > 0:
                q_v[2 * j - 2] = rope(last[:, :HEAD]).T
                q_v[2 * j - 1] = rope(last[:, HEAD:]).T

    def attend(tiles, first):
        def start(tile):
            rel, ccs, head, qi, rs, r0 = tile
            keys = r0 + Q_TILE if first else rows
            q_t = q_v[qi, :, rs]
            s = jnp.concatenate([jnp.dot(kv_v[rel, cc, head, 0, :keys, :], q_t, preferred_element_type=F32) for cc in ccs], axis=0)
            if first:
                key_id = lax.broadcasted_iota(jnp.int32, s.shape, 0)
                row_id = lax.broadcasted_iota(jnp.int32, s.shape, 1) + r0
                s = jnp.where(key_id <= row_id, s, -jnp.inf)
            return s

        def soften(tile, s):
            rel, ccs, head, qi, rs, r0 = tile
            m_new = jnp.max(s, axis=0, keepdims=True)
            alpha = None
            if not first:
                m_old = m_v[qi, :, rs]
                m_new = jnp.maximum(m_old, m_new)
                alpha = jnp.exp2((m_old - m_new) * SCORE_EXP2)
            p = jnp.exp2((s - m_new) * SCORE_EXP2)
            l_new = jnp.sum(p, axis=0, keepdims=True)
            l_v[qi, :, rs] = l_new if first else l_v[qi, :, rs] * alpha + l_new
            m_v[qi, :, rs] = m_new
            return p.astype(BF), alpha

        def gather(tile, p, alpha):
            rel, ccs, head, qi, rs, r0 = tile
            keys = r0 + Q_TILE if first else rows
            v_t = jnp.concatenate([kv_v[rel, cc, head, 1, j * HEAD:(j + 1) * HEAD, :] for cc in ccs for j in range(keys // HEAD)], axis=1)
            o_new = jnp.dot(v_t, p, preferred_element_type=F32)
            acc_v[qi, :, rs] = o_new if first else acc_v[qi, :, rs] * alpha + o_new

        s = start(tiles[0])
        held = None
        for i in range(len(tiles) + 1):
            s_next = start(tiles[i + 1]) if i + 1 < len(tiles) else None
            if held is not None:
                gather(tiles[i - 1], *held)
            if i < len(tiles):
                held = soften(tiles[i], s)
            s = s_next

    def head_tiles(rel, ccs, head):
        return [(rel, ccs, head, head * group_size + g, slice(rt * Q_TILE, (rt + 1) * Q_TILE), rt * Q_TILE)
                for g in range(group_size) for rt in range(rows // Q_TILE)]

    def own_unit(head, carry):
        attend(head_tiles(0, (0,), head), True)
        return carry

    with jax.named_scope('own'):
        lax.fori_loop(0, kv_heads, own_unit, 0)

    def far_unit(rel, ccs, head):
        with jax.named_scope('far'):
            attend(head_tiles(rel, ccs, head), False)

    has_left = chip >= 1
    has_right = chip >= 3
    has_far = chip >= 2
    fwd_right = jnp.logical_and(chip >= 1, chip <= 2)
    fwd_left = jnp.logical_or(chip == 0, chip == 3)

    @pl.when(core == 1)
    def _():
        own_to(0, 1, 0, sibling).wait_recv()
        own_to(0, 1, 1, sibling).wait_recv()

    @pl.when(has_left)
    def _():
        own_to(1, 0, 1, x_right).wait_recv()

        @pl.when(fwd_right)
        def _():
            fwd_far(1).start()

        fwd_sib(1, 1).start()

    @pl.when(fwd_left)
    def _():
        own_to(2, 0, 0, x_left).wait_recv()
        fwd_far(0).start()

        @pl.when(has_right)
        def _():
            fwd_sib(2, 0).start()

    for c in range(2):
        wo_part(c, 1).wait_recv()
        for d in range(2):
            wx_own(d, c, chip).start()

    def sibling_unit(head, carry):
        far_unit(0, (1,), head)
        return carry

    @pl.when(core == 1)
    def _():
        lax.fori_loop(0, kv_heads, sibling_unit, 0)

    def seg(index):
        return pl.ds(pl.multiple_of(index * seg_rows, seg_rows), seg_rows)

    own_seg, far_seg = tp, (tp + 2) % ring
    mate_seg = ((tp + ring + turn) % ring, (tp + ring - turn) % ring)

    def o_part(c, which):
        return remote(o_v.at[seg(mate_seg[c] if which else far_seg), :], ox_v.at[c, which],
                      o_send.at[c, which], o_recv.at[c, which], y_mate[c])

    loads[3].wait()

    def sib_wait(rel, head):
        remote(kv_v.at[rel, 0, head], kv_v.at[rel, 1, head], kv_fwd_send.at[rel, head], kv_recv.at[rel, 1, head], sibling).wait_recv()

    def side_unit(i, carry):
        @pl.when((i == 0) & has_left)
        def _():
            sib_wait(1, 1)

        @pl.when((i == 1) & has_left)
        def _():
            own_to(1, 0, 0, x_right).wait_recv()
            fwd_sib(1, 0).start()

        @pl.when((i == 1) & has_right)
        def _():
            sib_wait(2, 0)
            own_to(2, 0, 1, x_left).wait_recv()
            fwd_sib(2, 1).start()

        @pl.when(((i == 0) & has_left) | ((i == 1) & has_right))
        def _():
            far_unit(1 + i, (0, 1), 1 - i)

        return carry

    lax.fori_loop(0, 2, side_unit, 0)

    def seg_tiles(rs, *pieces):
        return [(rel, (0, 1), head, head * group_size + g, rs, 0) for rel, head in pieces for g in range(group_size)]

    def seg_step(k, carry):
        j = (k % 2) * (1 - k // 4) + (k // 2) * (k // 4)
        index = (tp + ring + 2 * ((3 - j) // 3) + turn * ((j % 3) % 2) - turn * (j // 2 - j // 3)) % ring
        rs = seg(index)
        near = (k < 2) | (k == 4) | (k == 6)

        @pl.when((k == 0) & has_left)
        def _():
            sib_wait(1, 0)

        @pl.when((k == 0) & has_right)
        def _():
            sib_wait(2, 1)

        @pl.when((k == 1) & has_far)
        def _():
            fwd_far(1).wait_recv()
            fwd_sib(3, 1).start()
            fwd_far(0).wait_recv()
            fwd_sib(3, 0).start()

        @pl.when((k == 2) & has_far)
        def _():
            sib_wait(3, 1)
            sib_wait(3, 0)

        @pl.when(k == 3)
        def _():
            with jax.named_scope('wx_wait'):
                wx_own(0, 0, chip_left).wait_recv()
                wx_pass(0, chip_left).start()
                wx_own(1, 1, chip_right).wait_recv()
                wx_pass(1, chip_right).start()

        @pl.when(near & has_right)
        def _():
            with jax.named_scope('near_seg'):
                attend(seg_tiles(rs, (1, 0), (2, 1)), False)

        @pl.when(near & (has_left & (chip < 3)))
        def _():
            with jax.named_scope('left_seg'):
                attend(seg_tiles(rs, (1, 0)), False)

        @pl.when(jnp.logical_not(near) & has_far)
        def _():
            with jax.named_scope('far_seg'):
                attend(seg_tiles(rs, (3, 1), (3, 0)), False)

        @pl.when(jnp.logical_not(near))
        def _():
            seg_done(j, rs)

        return carry

    def seg_done(j, rs):
        for qi in range(kv_heads * group_size):
            o_v[rs, qi * HEAD:(qi + 1) * HEAD] = (acc_v[qi, :, rs] * (1.0 / l_v[qi, :, rs])).astype(BF).T

        @pl.when(j == 0)
        def _():
            for c in range(2):
                o_part(c, 0).start()

        @pl.when(j == 1)
        def _():
            o_part(0, 1).start()
            with jax.named_scope('wo_wait'):
                for c in range(2):
                    wo_part(c, 0).wait_recv()
                    wo_share(c, 0, core).start()

        @pl.when(j == 2)
        def _():
            o_part(1, 1).start()
            with jax.named_scope('sub_wait'):
                wx_own(0, 1, chip_left).wait_recv()
                wx_own(1, 0, chip_right).wait_recv()
                for c in range(2):
                    wx_pass(c, chip_far).wait_recv()
                    wo_share(c, 1, core).start()

    with jax.named_scope('segs'):
        lax.fori_loop(0, 2 * ring, seg_step, 0)

    def col(c, g):
        return pl.ds(pl.multiple_of(c * half + g * cols, cols), cols)

    def two_mates(c, g, own_rows, which):
        g0 = pl.multiple_of(g * cols, cols)
        return (jnp.dot(o_v[seg(own_rows), :], wo_v[:, col(c, g)], preferred_element_type=F32)
                + jnp.dot(ox_v[c, which], wox_v[c, :, pl.ds(g0, cols)], preferred_element_type=F32))

    def cross(c, g):
        return remote(part_v.at[c, g], recv_v.at[c, g], part_send.at[c, g], part_recv.at[c, g], y_mate[1 - c])

    def f1(c, g, d, owner):
        block = out_v.at[seg(owner), col(c, g)]
        return remote(block, block, f1_send.at[c, g, d], f1_recv.at[c, g, d], y_left if d else y_right)

    def f2(g, d, owner):
        block = out_v.at[seg(owner), col(d, g)]
        return remote(block, block, f2_send.at[g, d], f2_recv.at[g, d], y_left if d else y_right)

    with jax.named_scope('mates'):
        for c in range(2):
            for kind in range(2):
                wo_share(c, kind, 1 - core).wait_recv()
            o_part(c, 0).wait_recv()

    def project_cross(g, carry):
        for c in range(2):
            part_v[c, g] = two_mates(c, g, mate_seg[1 - c], 0).astype(BF)
            cross(c, g).start()
        return carry

    with jax.named_scope('cross'):
        lax.fori_loop(0, CHUNKS, project_cross, 0)

    with jax.named_scope('caches'):
        k_out[...] = kc_v[...].reshape(k_out.shape)
        v_out[...] = vc_v[...].reshape(v_out.shape)

    for c in range(2):
        o_part(c, 1).wait_recv()

    def project_own(g, carry):
        for c in range(2):
            attn = two_mates(c, g, own_seg, 1)
            cross(c, g).wait_recv()
            attn = attn + recv_v[c, g].astype(F32)
            out_v[seg(own_seg), col(c, g)] = (x_v[seg(own_seg), col(c, g)].astype(F32) + attn).astype(BF)
            for d in range(2):
                f1(c, g, d, own_seg).start()
        return carry

    with jax.named_scope('own_out'):
        lax.fori_loop(0, CHUNKS, project_own, 0)

    side_seg = ((tp + ring - 1) % ring, (tp + 1) % ring)

    def pass_on(g, carry):
        for d in range(2):
            f1(d, g, d, side_seg[d]).wait_recv()
            f2(g, d, side_seg[d]).start()
        return carry

    with jax.named_scope('pass_on'):
        lax.fori_loop(0, CHUNKS, pass_on, 0)

    def finish(g, carry):
        for d in range(2):
            f1(1 - d, g, d, side_seg[d]).wait_recv()
            f2(g, d, far_seg).wait_recv()
        return carry

    with jax.named_scope('finish'):
        lax.fori_loop(0, CHUNKS, finish, 0)

    def drain(g, carry):
        for d in range(2):
            cross(d, g).wait_send()
            f2(g, d, side_seg[d]).wait_send()
            for c in range(2):
                f1(c, g, d, own_seg).wait_send()
        return carry

    with jax.named_scope('drain'):
        lax.fori_loop(0, CHUNKS, drain, 0)
    for c in range(2):
        wx_pass(c, chip_right if c else chip_left).wait_send()
        for i in range(2):
            wo_part(c, i).wait_send()
            wx_own(i, c, chip).wait_send()
            wo_share(c, i, core).wait_send()
            o_part(c, i).wait_send()

    @pl.when(core == 0)
    def _():
        own_to(0, 1, 0, sibling).wait_send()
        own_to(0, 1, 1, sibling).wait_send()

    @pl.when(right_sends)
    def _():
        own_to(1, 0, 1, x_right).wait_send()
        own_to(1, 0, 0, x_right).wait_send()

    @pl.when(left_h0_sends)
    def _():
        own_to(2, 0, 0, x_left).wait_send()

    @pl.when(left_h1_sends)
    def _():
        own_to(2, 0, 1, x_left).wait_send()

    @pl.when(has_left)
    def _():
        fwd_sib(1, 0).wait_send()
        fwd_sib(1, 1).wait_send()

    @pl.when(has_right)
    def _():
        fwd_sib(2, 0).wait_send()
        fwd_sib(2, 1).wait_send()

    @pl.when(has_far)
    def _():
        fwd_sib(3, 0).wait_send()
        fwd_sib(3, 1).wait_send()

    @pl.when(fwd_right)
    def _():
        fwd_far(1).wait_send()

    @pl.when(fwd_left)
    def _():
        fwd_far(0).wait_send()


def solution(mesh):
    ring = mesh.shape['tp']
    if mesh.shape['cp'] != 2 * ring or ring != 4:
        raise ValueError('mesh')
    row_spec = P(('dp', 'cp'), None)
    cache_spec = P(('dp', 'cp'), 'tp', None)
    head_cols = P(None, 'tp')

    def local_block(hidden, positions, norm_gain, w_query, w_key, w_value, w_out):
        rows, width = hidden.shape
        kv_heads = w_key.shape[1] // HEAD
        q_heads = w_query.shape[1] // HEAD
        seg_rows, half = rows // ring, width // 2
        cols = half // CHUNKS
        dma = pltpu.SemaphoreType.DMA
        out, k_new, v_new = pl.pallas_call(
            lambda *refs: block_kernel(ring, kv_heads, q_heads // kv_heads, *refs),
            out_shape=(
                pltpu.VMEM((rows, width), BF),
                pltpu.VMEM((rows, kv_heads, HEAD), BF),
                pltpu.VMEM((rows, kv_heads, HEAD), BF),
            ),
            in_specs=[pl.BlockSpec(memory_space=pl.ANY)] + [pl.BlockSpec(memory_space=pltpu.VMEM)] * 3
            + [pl.BlockSpec(memory_space=pl.ANY)] * 4,
            out_specs=[pl.BlockSpec(memory_space=pltpu.VMEM)] * 3,
            scratch_shapes=[
                pltpu.VMEM((rows, width), BF),
                pltpu.VMEM((rows, width), BF),
                pltpu.VMEM(w_query.shape, BF),
                pltpu.VMEM((width, 2 * kv_heads * HEAD), BF),
                pltpu.VMEM(w_out.shape, BF),
                pltpu.VMEM((rows, HEAD), F32),
                pltpu.VMEM((rows, HEAD), F32),
                pltpu.VMEM((rows, kv_heads * HEAD), BF),
                pltpu.VMEM((rows, kv_heads * HEAD), BF),
                pltpu.VMEM((q_heads, HEAD, rows), BF),
                pltpu.VMEM((4, 2, kv_heads, 2, rows, HEAD), BF),
                pltpu.VMEM((q_heads, 1, rows), F32),
                pltpu.VMEM((q_heads, 1, rows), F32),
                pltpu.VMEM((q_heads, HEAD, rows), F32),
                pltpu.VMEM((rows, q_heads * HEAD), BF),
                pltpu.VMEM((2, q_heads * HEAD, half), BF),
                pltpu.VMEM((2, 2, seg_rows, q_heads * HEAD), BF),
                pltpu.VMEM((2, CHUNKS, seg_rows, cols), BF),
                pltpu.VMEM((2, CHUNKS, seg_rows, cols), BF),
                dma((4 + LOAD_CHUNKS,)),
                dma((4, kv_heads)),
                dma((4, 2, kv_heads)),
                dma((4, kv_heads)),
                dma((2, 2)), dma((2, 2)), dma((2, 2)), dma((2, 2)), dma((2,)), dma((2,)), dma((2, 2)), dma((2, 2)),
                dma((2, 2)), dma((2, 2)),
                dma((2, CHUNKS)), dma((2, CHUNKS)),
                dma((2, CHUNKS, 2)), dma((2, CHUNKS, 2)),
                dma((CHUNKS, 2)), dma((CHUNKS, 2)),
            ],
            compiler_params=pltpu.CompilerParams(collective_id=0, has_side_effects=True, vmem_limit_bytes=60 * 1024 * 1024),
            name='attn_block',
        )(hidden, positions, norm_gain, jnp.asarray(inverse_freq()), w_query, w_key, w_value, w_out)
        return out, k_new, v_new

    return jax.shard_map(local_block, mesh=mesh,
                         in_specs=(row_spec, P(('dp', 'cp')), P(None), head_cols, head_cols, head_cols, P('tp', None)),
                         out_specs=(row_spec, cache_spec, cache_spec), check_vma=False)
```

```python
import math
import jax
import jax.numpy as jnp
import numpy as np
from jax import lax
from jax.experimental import pallas as pl
from jax.experimental.pallas import tpu as pltpu
from jax.sharding import PartitionSpec as P

HEAD = 128
EPS = 1e-5
LOG_THETA = math.log(1000000.0)
SCORE_EXP2 = math.log2(math.e) / math.sqrt(HEAD)
BF = jnp.bfloat16
F32 = jnp.float32
CHUNKS = 3
Q_TILE = 256
NORM_ROWS = 32
LOAD_CHUNKS = 4
SHARED_ROWS = 64


def inverse_freq():
    half = np.exp(np.arange(HEAD // 2, dtype=np.float64) * (-2.0 * LOG_THETA / HEAD)).astype(np.float32)
    return np.concatenate([half, half])[None, :]


def block_kernel(ring, kv_heads, group_size,
                 x_hbm, pos_ref, gain_ref, freq_ref, wq_hbm, wk_hbm, wv_hbm, wo_hbm,
                 out_v, k_out, v_out,
                 x_v, h_v, wq_v, wkv_v, wo_v, cos_v, sin_v, kc_v, vc_v, q_v, kv_v, m_v, l_v, acc_v, o_v,
                 wox_v, ox_v, part_v, recv_v,
                 load_sem, kv_send, kv_recv, kv_fwd_send, far_send, far_recv,
                 wo_send, wo_recv, wx_send, wx_recv, wf_send, wf_recv, wo_fwd_send, wo_fwd_recv, o_send, o_recv, part_send, part_recv,
                 f1_send, f1_recv, f2_send, f2_recv):
    rows, width = x_v.shape
    cp = lax.axis_index('cp')
    tp = lax.axis_index('tp')
    chip = cp // 2
    core = cp % 2
    seg_rows = rows // ring
    half = width // 2
    cols = half // CHUNKS
    k_half = wo_v.shape[0] // 2

    x_right = {'cp': ((chip + 1) % ring) * 2 + core}
    x_left = {'cp': ((chip + ring - 1) % ring) * 2 + core}
    sibling = {'cp': chip * 2 + 1 - core}
    y_right = {'tp': (tp + 1) % ring}
    y_left = {'tp': (tp + ring - 1) % ring}
    turn = 1 - 2 * (tp % 2)
    y_mate = ({'tp': (tp + ring + turn) % ring}, {'tp': (tp + ring - turn) % ring})

    kv_cols = kv_heads * HEAD
    chunk = rows // LOAD_CHUNKS
    x_loads = [pltpu.make_async_copy(x_hbm.at[i * chunk:(i + 1) * chunk, :], x_v.at[i * chunk:(i + 1) * chunk, :],
                                     load_sem.at[4 + i]) for i in range(LOAD_CHUNKS)]
    loads = [
        pltpu.make_async_copy(wk_hbm, wkv_v.at[:, :kv_cols], load_sem.at[0]),
        pltpu.make_async_copy(wv_hbm, wkv_v.at[:, kv_cols:], load_sem.at[1]),
        pltpu.make_async_copy(wq_hbm, wq_v, load_sem.at[2]),
        pltpu.make_async_copy(wo_hbm, wo_v, load_sem.at[3]),
    ]
    for copy in x_loads[:1] + loads[:2] + x_loads[1:] + loads[2:3]:
        copy.start()

    barrier = pltpu.get_barrier_semaphore()
    for peer in (x_right, x_left, sibling, y_right, y_left):
        pl.semaphore_signal(barrier, inc=1, device_id=peer, device_id_type=pl.DeviceIdType.MESH)

    with jax.named_scope('load_wait'):
        pos = pos_ref[...].astype(F32).reshape(rows // HEAD, HEAD)
        pos = jnp.concatenate([pos, jnp.zeros((8 - rows // HEAD, HEAD), F32)], axis=0).T
        sign = jnp.where(lax.broadcasted_iota(jnp.int32, (1, HEAD), 1) < HEAD // 2, -1.0, 1.0)
        for i in range(rows // HEAD):
            angles = pos[:, i:i + 1] * freq_ref[...]
            cos_v[i * HEAD:(i + 1) * HEAD, :] = jnp.cos(angles)
            sin_v[i * HEAD:(i + 1) * HEAD, :] = jnp.sin(angles) * sign

    def remote(src, dst, send, recv, peer):
        return pltpu.make_async_remote_copy(src_ref=src, dst_ref=dst, send_sem=send, recv_sem=recv,
                                            device_id=peer, device_id_type=pl.DeviceIdType.MESH)

    with jax.named_scope('barrier'):
        pl.semaphore_wait(barrier, 5)

    base = core * k_half
    direct_rows = k_half - SHARED_ROWS
    sub_rows = SHARED_ROWS // ring

    def sub_at(c, index):
        return wox_v.at[c, pl.ds(pl.multiple_of(base + direct_rows + index * sub_rows, sub_rows), sub_rows), :]

    def wo_part(c, kind):
        start, count = (base, direct_rows) if kind == 0 else (base + direct_rows + chip * sub_rows, sub_rows)
        ks = pl.ds(pl.multiple_of(start, sub_rows), count)
        return remote(wo_hbm.at[ks, c * half:(c + 1) * half], wox_v.at[c, ks, :],
                      wo_send.at[c, kind], wo_recv.at[c, kind], y_mate[c])

    def wx_own(d, c, index):
        return remote(sub_at(c, index), sub_at(c, index), wx_send.at[d, c], wx_recv.at[d, c], x_left if d else x_right)

    def wx_pass(d, c, index):
        return remote(sub_at(c, index), sub_at(c, index), wf_send.at[d, c], wf_recv.at[d, c], x_left if d else x_right)

    def wo_share(c, kind, from_core):
        start = from_core * k_half + kind * direct_rows
        part = wox_v.at[c, pl.ds(pl.multiple_of(start, sub_rows), SHARED_ROWS if kind else direct_rows), :]
        return remote(part, part, wo_fwd_send.at[c, kind], wo_fwd_recv.at[c, kind], sibling)

    chip_left, chip_right, chip_far = (chip + ring - 1) % ring, (chip + 1) % ring, (chip + 2) % ring

    for c in range(2):
        wo_part(c, 1).start()
    for c in range(2):
        wo_part(c, 0).start()

    def norm_rows(r0, count):
        xf = x_v[pl.ds(r0, count), :].astype(F32)
        inv = lax.rsqrt(jnp.mean(xf * xf, axis=-1, keepdims=True) + EPS)
        h_v[pl.ds(r0, count), :] = (xf * inv * gain_ref[...].astype(F32).reshape(1, width)).astype(BF)

    def norm_step(i, carry):
        norm_rows(pl.multiple_of(i * NORM_ROWS, NORM_ROWS), NORM_ROWS)
        return carry

    def rope(vals, rs=slice(None)):
        return (vals * cos_v[rs, :] + pltpu.roll(vals, HEAD // 2, 1) * sin_v[rs, :]).astype(BF)

    def own_to(rel, cc, head, peer):
        return remote(kv_v.at[0, 0, head], kv_v.at[rel, cc, head],
                      kv_send.at[rel, head], kv_recv.at[rel, cc, head], peer)

    def own_chunk(rel, head, peer, i):
        ks = slice(i * chunk, (i + 1) * chunk)
        return remote(kv_v.at[0, 0, head, :, ks, :], kv_v.at[rel, 0, head, :, ks, :],
                      kv_send.at[rel, head], kv_recv.at[rel, 0, head], peer)

    def left_v(head, ks=slice(None)):
        return remote(kv_v.at[0, 0, head, 1, ks, :], kv_v.at[2, 0, head, 1, ks, :],
                      kv_send.at[2, head], kv_recv.at[2, 0, head], x_left)

    def far_k(head):
        return remote(kv_v.at[1, 0, head, 0], kv_v.at[3, 0, head, 0], far_send.at[head, 0], far_recv.at[head, 0], x_right)

    def far_v(head):
        return remote(kv_v.at[2, 0, head, 1], kv_v.at[3, 0, head, 1], far_send.at[head, 1], far_recv.at[head, 1], x_left)

    def fwd_sib(rel, head):
        return remote(kv_v.at[rel, 0, head], kv_v.at[rel, 1, head],
                      kv_fwd_send.at[rel, head], kv_recv.at[rel, 1, head], sibling)

    right_sends = chip < ring - 1

    x_loads[0].wait()
    with jax.named_scope('norm'):
        lax.fori_loop(0, chunk // NORM_ROWS, norm_step, 0)
    for copy in loads[:2]:
        copy.wait()
    for i in range(LOAD_CHUNKS):
        if i + 1 < LOAD_CHUNKS:
            x_loads[i + 1].wait()
        ks = slice(i * chunk, (i + 1) * chunk)
        with jax.named_scope('kv_proj'):
            kv_proj = jnp.dot(h_v[ks, :], wkv_v[...], preferred_element_type=F32)
            if i + 1 < LOAD_CHUNKS:
                for r in range(0, chunk, 16):
                    norm_rows((i + 1) * chunk + r, 16)
            for h in range(kv_heads):
                hc = slice(h * HEAD, (h + 1) * HEAD)
                k_head = rope(kv_proj[:, hc], ks)
                kv_v[0, 0, h, 0, ks, :] = k_head
                kc_v[ks, hc] = k_head
                v_head = kv_proj[:, kv_cols + h * HEAD:kv_cols + (h + 1) * HEAD].astype(BF)
                vc_v[ks, hc] = v_head
                kv_v[0, 0, h, 1, ks, :] = v_head.T

        @pl.when(right_sends)
        def _(i=i):
            own_chunk(1, 0, x_right, i).start()

        @pl.when(chip == 0)
        def _(i=i):
            own_chunk(2, 0, x_left, i).start()

        @pl.when(chip == 1)
        def _(i=i):
            left_v(0, slice(i * chunk, (i + 1) * chunk)).start()

    loads[3].start()

    @pl.when(core == 0)
    def _():
        own_to(0, 1, 0, sibling).start()
        own_to(0, 1, 1, sibling).start()

    @pl.when(right_sends)
    def _():
        own_to(1, 0, 1, x_right).start()

    @pl.when(chip == 0)
    def _():
        own_to(2, 0, 1, x_left).start()

    @pl.when(chip == 1)
    def _():
        left_v(1).start()

    loads[2].wait()

    with jax.named_scope('q_proj'):
        q_pair = None
        for j in range(kv_heads * group_size // 2 + 1):
            last = q_pair
            if j < kv_heads * group_size // 2:
                q_pair = jnp.dot(h_v[...], wq_v[:, j * 2 * HEAD:(j + 1) * 2 * HEAD], preferred_element_type=F32)
            if j > 0:
                q_v[2 * j - 2] = rope(last[:, :HEAD]).T
                q_v[2 * j - 1] = rope(last[:, HEAD:]).T

    def attend(tiles, first):
        def start(tile):
            rel, ccs, head, qi, rs, r0 = tile
            keys = r0 + Q_TILE if first else rows
            q_t = q_v[qi, :, rs]
            s = jnp.concatenate([jnp.dot(kv_v[rel, cc, head, 0, :keys, :], q_t, preferred_element_type=F32) for cc in ccs], axis=0)
            if first:
                key_id = lax.broadcasted_iota(jnp.int32, s.shape, 0)
                row_id = lax.broadcasted_iota(jnp.int32, s.shape, 1) + r0
                s = jnp.where(key_id <= row_id, s, -jnp.inf)
            return s

        def soften(tile, s):
            rel, ccs, head, qi, rs, r0 = tile
            m_new = jnp.max(s, axis=0, keepdims=True)
            alpha = None
            if not first:
                m_old = m_v[qi, :, rs]
                m_new = jnp.maximum(m_old, m_new)
                alpha = jnp.exp2((m_old - m_new) * SCORE_EXP2)
            p = jnp.exp2((s - m_new) * SCORE_EXP2)
            l_new = jnp.sum(p, axis=0, keepdims=True)
            l_v[qi, :, rs] = l_new if first else l_v[qi, :, rs] * alpha + l_new
            m_v[qi, :, rs] = m_new
            return p.astype(BF), alpha

        def gather(tile, p, alpha):
            rel, ccs, head, qi, rs, r0 = tile
            keys = r0 + Q_TILE if first else rows
            v_t = jnp.concatenate([kv_v[rel, cc, head, 1, j * HEAD:(j + 1) * HEAD, :] for cc in ccs for j in range(keys // HEAD)], axis=1)
            o_new = jnp.dot(v_t, p, preferred_element_type=F32)
            acc_v[qi, :, rs] = o_new if first else acc_v[qi, :, rs] * alpha + o_new

        s = start(tiles[0])
        held = None
        for i in range(len(tiles) + 1):
            s_next = start(tiles[i + 1]) if i + 1 < len(tiles) else None
            if held is not None:
                gather(tiles[i - 1], *held)
            if i < len(tiles):
                held = soften(tiles[i], s)
            s = s_next

    def head_tiles(rel, ccs, head):
        return [(rel, ccs, head, head * group_size + g, slice(rt * Q_TILE, (rt + 1) * Q_TILE), rt * Q_TILE)
                for g in range(group_size) for rt in range(rows // Q_TILE)]

    def own_unit(head, carry):
        attend(head_tiles(0, (0,), head), True)
        return carry

    with jax.named_scope('own'):
        lax.fori_loop(0, kv_heads, own_unit, 0)

    def far_unit(rel, ccs, head):
        with jax.named_scope('far'):
            attend(head_tiles(rel, ccs, head), False)

    has_left = chip >= 1
    has_right = chip >= 3
    has_far = chip >= 2
    fwd_right = jnp.logical_and(chip >= 1, chip <= 2)

    def take_left(head):
        own_to(1, 0, head, x_right).wait_recv()

        @pl.when(fwd_right)
        def _():
            far_k(head).start()

        fwd_sib(1, head).start()

    def take_right(head):
        own_to(2, 0, head, x_left).wait_recv()
        far_v(head).start()
        fwd_sib(2, head).start()

    def relay_right(head):
        left_v(head).wait_recv()
        far_v(head).start()

    @pl.when(core == 1)
    def _():
        own_to(0, 1, 0, sibling).wait_recv()
        own_to(0, 1, 1, sibling).wait_recv()

    @pl.when(has_left)
    def _():
        take_left(0)

    @pl.when(has_right)
    def _():
        take_right(0)

    @pl.when(chip == 0)
    def _():
        relay_right(0)

    ends = jnp.logical_or(chip == 0, chip == 3)

    def wx_start(d):
        for c in range(2):
            wx_own(d, c, chip).start()

    for c in range(2):
        wo_part(c, 1).wait_recv()

    @pl.when(ends)
    def _():
        wx_start(0)

    @pl.when(fwd_right)
    def _():
        wx_start(1)

    def sibling_unit(head, carry):
        far_unit(0, (1,), head)
        return carry

    @pl.when(core == 1)
    def _():
        lax.fori_loop(0, kv_heads, sibling_unit, 0)

    @pl.when(fwd_right)
    def _():
        take_left(1)

    @pl.when(chip == 0)
    def _():
        relay_right(1)

    def seg(index):
        return pl.ds(pl.multiple_of(index * seg_rows, seg_rows), seg_rows)

    own_seg, far_seg = tp, (tp + 2) % ring
    mate_seg = ((tp + ring + turn) % ring, (tp + ring - turn) % ring)

    head_cols = group_size * HEAD

    def o_part(c, which, head):
        hc = slice(head * head_cols, (head + 1) * head_cols)
        return remote(o_v.at[seg(mate_seg[c] if which else far_seg), hc], ox_v.at[c, which, :, hc],
                      o_send.at[c, which, head], o_recv.at[c, which, head], y_mate[c])

    def finish_rows(head, rs):
        for qi in range(head * group_size, (head + 1) * group_size):
            o_v[rs, qi * HEAD:(qi + 1) * HEAD] = (acc_v[qi, :, rs] * (1.0 / l_v[qi, :, rs])).astype(BF).T

    loads[3].wait()

    def sib_wait(rel, head):
        remote(kv_v.at[rel, 0, head], kv_v.at[rel, 1, head], kv_fwd_send.at[rel, head], kv_recv.at[rel, 1, head], sibling).wait_recv()

    def side_unit(u, carry):
        head = (1 - u % 2) * ((u + 2) // 4)
        rel = (1 - u % 2) * (1 + u // 4) + (u % 2) * (2 + u // 3)
        need = ((rel == 1) & has_left) | ((rel == 2) & has_right) | ((rel == 3) & has_far)

        @pl.when((u == 0) & has_left)
        def _():
            sib_wait(1, 0)

        @pl.when((u == 1) & has_right)
        def _():
            take_left(1)
            take_right(1)

        @pl.when((u == 1) & fwd_right)
        def _():
            wx_start(0)

        @pl.when((u == 1) & ends)
        def _():
            wx_start(1)

        @pl.when((u == 1) & has_right)
        def _():
            sib_wait(2, 0)

        @pl.when((u == 2) & (chip < 2))
        def _():
            with jax.named_scope('wx_wait'):
                for d in range(2):
                    for c in range(2):
                        wx_own(d, c, chip_right if d else chip_left).wait_recv()
                        wx_pass(d, c, chip_right if d else chip_left).start()

        @pl.when((u == 2) & has_far)
        def _():
            with jax.named_scope('far_h0'):
                far_k(0).wait_recv()
                far_v(0).wait_recv()
                fwd_sib(3, 0).start()

        @pl.when((u == 2) & has_left)
        def _():
            sib_wait(1, 1)

        @pl.when((u == 3) & has_far)
        def _():
            sib_wait(3, 0)

        @pl.when(u == 4)
        def _():
            finish_rows(0, slice(0, rows))
            for c in range(2):
                o_part(c, 0, 0).start()
            for c in range(2):
                o_part(c, 1, 0).start()

        @pl.when((u == 4) & has_far)
        def _():
            with jax.named_scope('far_h1'):
                far_k(1).wait_recv()
                far_v(1).wait_recv()
                fwd_sib(3, 1).start()

        @pl.when((u == 4) & has_right)
        def _():
            sib_wait(2, 1)

        @pl.when(need)
        def _():
            far_unit(rel, (0, 1), head)

        return carry

    lax.fori_loop(0, 5, side_unit, 0)

    with jax.named_scope('wo_wait'):
        for c in range(2):
            wo_part(c, 0).wait_recv()
            wo_share(c, 0, core).start()

    @pl.when(has_far)
    def _():
        sib_wait(3, 1)

    def seg_step(j, carry):
        index = (tp + ring + 2 * ((3 - j) // 3) + turn * ((j % 3) % 2) - turn * (j // 2 - j // 3)) % ring
        rs = seg(index)

        @pl.when(has_far)
        def _():
            with jax.named_scope('far_seg'):
                attend([(3, (0, 1), 1, group_size + g, rs, 0) for g in range(group_size)], False)

        finish_rows(1, rs)

        @pl.when(j == 0)
        def _():
            for c in range(2):
                o_part(c, 0, 1).start()

        @pl.when(j == 1)
        def _():
            o_part(0, 1, 1).start()

        @pl.when(j == 2)
        def _():
            o_part(1, 1, 1).start()
            with jax.named_scope('sub_wait'):
                @pl.when(has_far)
                def _():
                    for d in range(2):
                        for c in range(2):
                            wx_own(d, c, chip_right if d else chip_left).wait_recv()

                for d, gets in ((0, fwd_right), (1, ends)):
                    @pl.when(gets)
                    def _(d=d):
                        for c in range(2):
                            wx_pass(d, c, chip_far).wait_recv()

                for c in range(2):
                    wo_share(c, 1, core).start()

        return carry

    with jax.named_scope('segs'):
        lax.fori_loop(0, ring, seg_step, 0)

    def col(c, g):
        return pl.ds(pl.multiple_of(c * half + g * cols, cols), cols)

    def two_mates(c, g, own_rows, which):
        g0 = pl.multiple_of(g * cols, cols)
        return (jnp.dot(o_v[seg(own_rows), :], wo_v[:, col(c, g)], preferred_element_type=F32)
                + jnp.dot(ox_v[c, which], wox_v[c, :, pl.ds(g0, cols)], preferred_element_type=F32))

    def cross(c, g):
        return remote(part_v.at[c, g], recv_v.at[c, g], part_send.at[c, g], part_recv.at[c, g], y_mate[1 - c])

    def f1(c, g, d, owner):
        block = out_v.at[seg(owner), col(c, g)]
        return remote(block, block, f1_send.at[c, g, d], f1_recv.at[c, g, d], y_left if d else y_right)

    def f2(g, d, owner):
        block = out_v.at[seg(owner), col(d, g)]
        return remote(block, block, f2_send.at[g, d], f2_recv.at[g, d], y_left if d else y_right)

    with jax.named_scope('mates'):
        for c in range(2):
            for kind in range(2):
                wo_share(c, kind, 1 - core).wait_recv()
            for head in range(kv_heads):
                o_part(c, 0, head).wait_recv()

    def project_cross(g, carry):
        for c in range(2):
            part_v[c, g] = two_mates(c, g, mate_seg[1 - c], 0).astype(BF)
            cross(c, g).start()
        return carry

    with jax.named_scope('cross'):
        lax.fori_loop(0, CHUNKS, project_cross, 0)

    with jax.named_scope('caches'):
        k_out[...] = kc_v[...].reshape(k_out.shape)
        v_out[...] = vc_v[...].reshape(v_out.shape)

    for c in range(2):
        for head in range(kv_heads):
            o_part(c, 1, head).wait_recv()

    def project_own(g, carry):
        for c in range(2):
            attn = two_mates(c, g, own_seg, 1)
            cross(c, g).wait_recv()
            attn = attn + recv_v[c, g].astype(F32)
            out_v[seg(own_seg), col(c, g)] = (x_v[seg(own_seg), col(c, g)].astype(F32) + attn).astype(BF)
            for d in range(2):
                f1(c, g, d, own_seg).start()
        return carry

    with jax.named_scope('own_out'):
        lax.fori_loop(0, CHUNKS, project_own, 0)

    side_seg = ((tp + ring - 1) % ring, (tp + 1) % ring)

    def pass_on(g, carry):
        for d in range(2):
            f1(d, g, d, side_seg[d]).wait_recv()
            f2(g, d, side_seg[d]).start()
        return carry

    with jax.named_scope('pass_on'):
        lax.fori_loop(0, CHUNKS, pass_on, 0)

    def finish(g, carry):
        for d in range(2):
            f1(1 - d, g, d, side_seg[d]).wait_recv()
            f2(g, d, far_seg).wait_recv()
        return carry

    with jax.named_scope('finish'):
        lax.fori_loop(0, CHUNKS, finish, 0)

    def drain(g, carry):
        for d in range(2):
            cross(d, g).wait_send()
            f2(g, d, side_seg[d]).wait_send()
            for c in range(2):
                f1(c, g, d, own_seg).wait_send()
        return carry

    with jax.named_scope('drain'):
        lax.fori_loop(0, CHUNKS, drain, 0)
    for c in range(2):
        @pl.when(chip < 2)
        def _(c=c):
            for d in range(2):
                wx_pass(d, c, chip_right if d else chip_left).wait_send()

        for i in range(2):
            wo_part(c, i).wait_send()
            wx_own(i, c, chip).wait_send()
            wo_share(c, i, core).wait_send()
            for head in range(kv_heads):
                o_part(c, i, head).wait_send()

    @pl.when(core == 0)
    def _():
        own_to(0, 1, 0, sibling).wait_send()
        own_to(0, 1, 1, sibling).wait_send()

    for head in range(kv_heads):
        @pl.when(right_sends)
        def _(head=head):
            own_to(1, 0, head, x_right).wait_send()

        @pl.when(chip == 0)
        def _(head=head):
            own_to(2, 0, head, x_left).wait_send()

        @pl.when(chip == 1)
        def _(head=head):
            left_v(head).wait_send()

        @pl.when(fwd_right)
        def _(head=head):
            far_k(head).wait_send()

        @pl.when(jnp.logical_or(chip == 0, has_right))
        def _(head=head):
            far_v(head).wait_send()

        for rel, sent in ((1, has_left), (2, has_right), (3, has_far)):
            @pl.when(sent)
            def _(rel=rel, head=head):
                fwd_sib(rel, head).wait_send()


def solution(mesh):
    ring = mesh.shape['tp']
    if mesh.shape['cp'] != 2 * ring or ring != 4:
        raise ValueError('mesh')
    row_spec = P(('dp', 'cp'), None)
    cache_spec = P(('dp', 'cp'), 'tp', None)
    head_cols = P(None, 'tp')

    def local_block(hidden, positions, norm_gain, w_query, w_key, w_value, w_out):
        rows, width = hidden.shape
        kv_heads = w_key.shape[1] // HEAD
        q_heads = w_query.shape[1] // HEAD
        seg_rows, half = rows // ring, width // 2
        cols = half // CHUNKS
        dma = pltpu.SemaphoreType.DMA
        out, k_new, v_new = pl.pallas_call(
            lambda *refs: block_kernel(ring, kv_heads, q_heads // kv_heads, *refs),
            out_shape=(
                pltpu.VMEM((rows, width), BF),
                pltpu.VMEM((rows, kv_heads, HEAD), BF),
                pltpu.VMEM((rows, kv_heads, HEAD), BF),
            ),
            in_specs=[pl.BlockSpec(memory_space=pl.ANY)] + [pl.BlockSpec(memory_space=pltpu.VMEM)] * 3
            + [pl.BlockSpec(memory_space=pl.ANY)] * 4,
            out_specs=[pl.BlockSpec(memory_space=pltpu.VMEM)] * 3,
            scratch_shapes=[
                pltpu.VMEM((rows, width), BF),
                pltpu.VMEM((rows, width), BF),
                pltpu.VMEM(w_query.shape, BF),
                pltpu.VMEM((width, 2 * kv_heads * HEAD), BF),
                pltpu.VMEM(w_out.shape, BF),
                pltpu.VMEM((rows, HEAD), F32),
                pltpu.VMEM((rows, HEAD), F32),
                pltpu.VMEM((rows, kv_heads * HEAD), BF),
                pltpu.VMEM((rows, kv_heads * HEAD), BF),
                pltpu.VMEM((q_heads, HEAD, rows), BF),
                pltpu.VMEM((4, 2, kv_heads, 2, rows, HEAD), BF),
                pltpu.VMEM((q_heads, 1, rows), F32),
                pltpu.VMEM((q_heads, 1, rows), F32),
                pltpu.VMEM((q_heads, HEAD, rows), F32),
                pltpu.VMEM((rows, q_heads * HEAD), BF),
                pltpu.VMEM((2, q_heads * HEAD, half), BF),
                pltpu.VMEM((2, 2, seg_rows, q_heads * HEAD), BF),
                pltpu.VMEM((2, CHUNKS, seg_rows, cols), BF),
                pltpu.VMEM((2, CHUNKS, seg_rows, cols), BF),
                dma((4 + LOAD_CHUNKS,)),
                dma((3, kv_heads)),
                dma((4, 2, kv_heads)),
                dma((4, kv_heads)),
                dma((kv_heads, 2)), dma((kv_heads, 2)),
                dma((2, 2)), dma((2, 2)), dma((2, 2)), dma((2, 2)), dma((2, 2)), dma((2, 2)), dma((2, 2)), dma((2, 2)),
                dma((2, 2, kv_heads)), dma((2, 2, kv_heads)),
                dma((2, CHUNKS)), dma((2, CHUNKS)),
                dma((2, CHUNKS, 2)), dma((2, CHUNKS, 2)),
                dma((CHUNKS, 2)), dma((CHUNKS, 2)),
            ],
            compiler_params=pltpu.CompilerParams(collective_id=0, has_side_effects=True, vmem_limit_bytes=60 * 1024 * 1024),
            name='attn_block',
        )(hidden, positions, norm_gain, jnp.asarray(inverse_freq()), w_query, w_key, w_value, w_out)
        return out, k_new, v_new

    return jax.shard_map(local_block, mesh=mesh,
                         in_specs=(row_spec, P(('dp', 'cp')), P(None), head_cols, head_cols, head_cols, P('tp', None)),
                         out_specs=(row_spec, cache_spec, cache_spec), check_vma=False)
```

```python
import math
import jax
import jax.numpy as jnp
import numpy as np
from jax import lax
from jax.experimental import pallas as pl
from jax.experimental.pallas import tpu as pltpu
from jax.sharding import PartitionSpec as P

HEAD = 128
EPS = 1e-5
LOG_THETA = math.log(1000000.0)
SCORE_EXP2 = math.log2(math.e) / math.sqrt(HEAD)
BF = jnp.bfloat16
F32 = jnp.float32
CHUNKS = 3
Q_TILE = 256
NORM_ROWS = 32
LOAD_CHUNKS = 4
SHARED_ROWS = 96


def inverse_freq():
    half = np.exp(np.arange(HEAD // 2, dtype=np.float64) * (-2.0 * LOG_THETA / HEAD)).astype(np.float32)
    return np.concatenate([half, half])[None, :]


def block_kernel(ring, kv_heads, group_size,
                 x_hbm, pos_ref, gain_ref, freq_ref, wq_hbm, wk_hbm, wv_hbm, wo_hbm,
                 out_v, k_out, v_out,
                 x_v, h_v, wq_v, wkv_v, wo_v, cos_v, sin_v, kc_v, vc_v, q_v, kv_v, m_v, l_v, acc_v, o_v,
                 wox_v, ox_v, part_v, recv_v,
                 load_sem, kv_send, kv_recv, kv_fwd_send, far_send, far_recv, late_recv,
                 wo_send, wo_recv, wx_send, wx_recv, wf_send, wf_recv, wo_fwd_send, wo_fwd_recv, o_send, o_recv, part_send, part_recv,
                 f1_send, f1_recv, f2_send, f2_recv):
    rows, width = x_v.shape
    cp = lax.axis_index('cp')
    tp = lax.axis_index('tp')
    chip = cp // 2
    core = cp % 2
    seg_rows = rows // ring
    half = width // 2
    cols = half // CHUNKS
    k_half = wo_v.shape[0] // 2

    x_right = {'cp': ((chip + 1) % ring) * 2 + core}
    x_left = {'cp': ((chip + ring - 1) % ring) * 2 + core}
    sibling = {'cp': chip * 2 + 1 - core}
    y_right = {'tp': (tp + 1) % ring}
    y_left = {'tp': (tp + ring - 1) % ring}
    turn = 1 - 2 * (tp % 2)
    y_mate = ({'tp': (tp + ring + turn) % ring}, {'tp': (tp + ring - turn) % ring})

    kv_cols = kv_heads * HEAD
    chunk = rows // LOAD_CHUNKS
    x_loads = [pltpu.make_async_copy(x_hbm.at[i * chunk:(i + 1) * chunk, :], x_v.at[i * chunk:(i + 1) * chunk, :],
                                     load_sem.at[4 + i]) for i in range(LOAD_CHUNKS)]
    loads = [
        pltpu.make_async_copy(wk_hbm, wkv_v.at[:, :kv_cols], load_sem.at[0]),
        pltpu.make_async_copy(wv_hbm, wkv_v.at[:, kv_cols:], load_sem.at[1]),
        pltpu.make_async_copy(wq_hbm, wq_v, load_sem.at[2]),
        pltpu.make_async_copy(wo_hbm, wo_v, load_sem.at[3]),
    ]
    for copy in x_loads[:1] + loads[:2] + x_loads[1:] + loads[2:3]:
        copy.start()

    barrier = pltpu.get_barrier_semaphore()
    for peer in (x_right, x_left, sibling, y_right, y_left):
        pl.semaphore_signal(barrier, inc=1, device_id=peer, device_id_type=pl.DeviceIdType.MESH)

    with jax.named_scope('load_wait'):
        pos = pos_ref[...].astype(F32).reshape(rows // HEAD, HEAD)
        pos = jnp.concatenate([pos, jnp.zeros((8 - rows // HEAD, HEAD), F32)], axis=0).T
        sign = jnp.where(lax.broadcasted_iota(jnp.int32, (1, HEAD), 1) < HEAD // 2, -1.0, 1.0)
        for i in range(rows // HEAD):
            angles = pos[:, i:i + 1] * freq_ref[...]
            cos_v[i * HEAD:(i + 1) * HEAD, :] = jnp.cos(angles)
            sin_v[i * HEAD:(i + 1) * HEAD, :] = jnp.sin(angles) * sign

    def remote(src, dst, send, recv, peer):
        return pltpu.make_async_remote_copy(src_ref=src, dst_ref=dst, send_sem=send, recv_sem=recv,
                                            device_id=peer, device_id_type=pl.DeviceIdType.MESH)

    with jax.named_scope('barrier'):
        pl.semaphore_wait(barrier, 5)

    base = core * k_half
    direct_rows = k_half - SHARED_ROWS
    sub_cols = half // ring

    def shared_rows(from_core):
        return pl.ds(pl.multiple_of(from_core * k_half + direct_rows, 32), SHARED_ROWS)

    def sub_at(c, index):
        return wox_v.at[c, shared_rows(core), pl.ds(pl.multiple_of(index * sub_cols, sub_cols), sub_cols)]

    def wo_part(c, kind):
        if kind:
            src = wo_hbm.at[shared_rows(core), pl.ds(pl.multiple_of(c * half + chip * sub_cols, sub_cols), sub_cols)]
            dst = sub_at(c, chip)
        else:
            ks = pl.ds(pl.multiple_of(base, 32), direct_rows)
            src, dst = wo_hbm.at[ks, c * half:(c + 1) * half], wox_v.at[c, ks, :]
        return remote(src, dst, wo_send.at[c, kind], wo_recv.at[c, kind], y_mate[c])

    def wx_own(d, c, index):
        return remote(sub_at(c, index), sub_at(c, index), wx_send.at[d, c], wx_recv.at[d, c], x_left if d else x_right)

    def wx_pass(d, c, index):
        return remote(sub_at(c, index), sub_at(c, index), wf_send.at[d, c], wf_recv.at[d, c], x_left if d else x_right)

    def wo_share(c, kind, from_core):
        ks = shared_rows(from_core) if kind else pl.ds(pl.multiple_of(from_core * k_half, 32), direct_rows)
        part = wox_v.at[c, ks, :]
        return remote(part, part, wo_fwd_send.at[c, kind], wo_fwd_recv.at[c, kind], sibling)

    chip_left, chip_right, chip_far = (chip + ring - 1) % ring, (chip + 1) % ring, (chip + 2) % ring

    for c in range(2):
        wo_part(c, 1).start()
    for c in range(2):
        wo_part(c, 0).start()

    def norm_rows(r0, count):
        xf = x_v[pl.ds(r0, count), :].astype(F32)
        inv = lax.rsqrt(jnp.mean(xf * xf, axis=-1, keepdims=True) + EPS)
        h_v[pl.ds(r0, count), :] = (xf * inv * gain_ref[...].astype(F32).reshape(1, width)).astype(BF)

    def norm_step(i, carry):
        norm_rows(pl.multiple_of(i * NORM_ROWS, NORM_ROWS), NORM_ROWS)
        return carry

    def rope(vals, rs=slice(None)):
        return (vals * cos_v[rs, :] + pltpu.roll(vals, HEAD // 2, 1) * sin_v[rs, :]).astype(BF)

    def own_to(rel, cc, head, peer):
        return remote(kv_v.at[0, 0, head], kv_v.at[rel, cc, head],
                      kv_send.at[rel, head], kv_recv.at[rel, cc, head], peer)

    def piece_sem(rel, head, late):
        return late_recv.at[rel] if late else kv_recv.at[rel, 0, head]

    def own_chunk(rel, head, peer, i, count=1, late=False):
        ks = slice(i * chunk, (i + count) * chunk)
        return remote(kv_v.at[0, 0, head, :, ks, :], kv_v.at[rel, 0, head, :, ks, :],
                      kv_send.at[rel, head], piece_sem(rel, head, late), peer)

    def left_v(head, ks=slice(None), late=False):
        return remote(kv_v.at[0, 0, head, 1, ks, :], kv_v.at[2, 0, head, 1, ks, :],
                      kv_send.at[2, head], piece_sem(2, head, late), x_left)

    half_chunks = LOAD_CHUNKS // 2
    key_halves = (slice(0, half_chunks * chunk), slice(half_chunks * chunk, rows))

    def far_k(head, ks=slice(None)):
        return remote(kv_v.at[1, 0, head, 0, ks, :], kv_v.at[3, 0, head, 0, ks, :], far_send.at[head, 0], far_recv.at[head, 0], x_right)

    def far_v(head, ks=slice(None)):
        return remote(kv_v.at[2, 0, head, 1, ks, :], kv_v.at[3, 0, head, 1, ks, :], far_send.at[head, 1], far_recv.at[head, 1], x_left)

    def fwd_sib(rel, head):
        return remote(kv_v.at[rel, 0, head], kv_v.at[rel, 1, head],
                      kv_fwd_send.at[rel, head], kv_recv.at[rel, 1, head], sibling)

    right_sends = chip < ring - 1

    x_loads[0].wait()
    with jax.named_scope('norm'):
        lax.fori_loop(0, chunk // NORM_ROWS, norm_step, 0)
    for copy in loads[:2]:
        copy.wait()
    for i in range(LOAD_CHUNKS):
        if i + 1 < LOAD_CHUNKS:
            x_loads[i + 1].wait()
        ks = slice(i * chunk, (i + 1) * chunk)
        with jax.named_scope('kv_proj'):
            kv_proj = jnp.dot(h_v[ks, :], wkv_v[...], preferred_element_type=F32)
            if i + 1 < LOAD_CHUNKS:
                for r in range(0, chunk, 16):
                    norm_rows((i + 1) * chunk + r, 16)
            for h in range(kv_heads):
                hc = slice(h * HEAD, (h + 1) * HEAD)
                k_head = rope(kv_proj[:, hc], ks)
                kv_v[0, 0, h, 0, ks, :] = k_head
                kc_v[ks, hc] = k_head
                v_head = kv_proj[:, kv_cols + h * HEAD:kv_cols + (h + 1) * HEAD].astype(BF)
                vc_v[ks, hc] = v_head
                kv_v[0, 0, h, 1, ks, :] = v_head.T

        @pl.when(right_sends)
        def _(i=i):
            own_chunk(1, 0, x_right, i).start()

        @pl.when(chip == 0)
        def _(i=i):
            own_chunk(2, 0, x_left, i).start()

        @pl.when(chip == 1)
        def _(i=i):
            left_v(0, slice(i * chunk, (i + 1) * chunk)).start()

    loads[3].start()

    @pl.when(core == 0)
    def _():
        own_to(0, 1, 0, sibling).start()
        own_to(0, 1, 1, sibling).start()

    def head_one(i):
        @pl.when(right_sends)
        def _():
            own_chunk(1, 1, x_right, i * half_chunks, half_chunks, i == 1).start()

        @pl.when(chip == 0)
        def _():
            own_chunk(2, 1, x_left, i * half_chunks, half_chunks, i == 1).start()

        @pl.when(chip == 1)
        def _():
            left_v(1, key_halves[i], i == 1).start()

    head_one(0)
    loads[2].wait()

    with jax.named_scope('q_proj'):
        q_pair = None
        for j in range(kv_heads * group_size // 2 + 1):
            last = q_pair
            if j < kv_heads * group_size // 2:
                q_pair = jnp.dot(h_v[...], wq_v[:, j * 2 * HEAD:(j + 1) * 2 * HEAD], preferred_element_type=F32)
            if j > 0:
                q_v[2 * j - 2] = rope(last[:, :HEAD]).T
                q_v[2 * j - 1] = rope(last[:, HEAD:]).T

    def attend(tiles, first):
        def start(tile):
            rel, ccs, head, qi, rs, r0 = tile
            keys = r0 + Q_TILE if first else rows
            q_t = q_v[qi, :, rs]
            s = jnp.concatenate([jnp.dot(kv_v[rel, cc, head, 0, :keys, :], q_t, preferred_element_type=F32) for cc in ccs], axis=0)
            if first:
                key_id = lax.broadcasted_iota(jnp.int32, s.shape, 0)
                row_id = lax.broadcasted_iota(jnp.int32, s.shape, 1) + r0
                s = jnp.where(key_id <= row_id, s, -jnp.inf)
            return s

        def soften(tile, s):
            rel, ccs, head, qi, rs, r0 = tile
            m_new = jnp.max(s, axis=0, keepdims=True)
            alpha = None
            if not first:
                m_old = m_v[qi, :, rs]
                m_new = jnp.maximum(m_old, m_new)
                alpha = jnp.exp2((m_old - m_new) * SCORE_EXP2)
            p = jnp.exp2((s - m_new) * SCORE_EXP2)
            l_new = jnp.sum(p, axis=0, keepdims=True)
            l_v[qi, :, rs] = l_new if first else l_v[qi, :, rs] * alpha + l_new
            m_v[qi, :, rs] = m_new
            return p.astype(BF), alpha

        def gather(tile, p, alpha):
            rel, ccs, head, qi, rs, r0 = tile
            keys = r0 + Q_TILE if first else rows
            v_t = jnp.concatenate([kv_v[rel, cc, head, 1, j * HEAD:(j + 1) * HEAD, :] for cc in ccs for j in range(keys // HEAD)], axis=1)
            o_new = jnp.dot(v_t, p, preferred_element_type=F32)
            acc_v[qi, :, rs] = o_new if first else acc_v[qi, :, rs] * alpha + o_new

        s = start(tiles[0])
        held = None
        for i in range(len(tiles) + 1):
            s_next = start(tiles[i + 1]) if i + 1 < len(tiles) else None
            if held is not None:
                gather(tiles[i - 1], *held)
            if i < len(tiles):
                held = soften(tiles[i], s)
            s = s_next

    def head_tiles(rel, ccs, head):
        return [(rel, ccs, head, head * group_size + g, slice(rt * Q_TILE, (rt + 1) * Q_TILE), rt * Q_TILE)
                for g in range(group_size) for rt in range(rows // Q_TILE)]

    def own_unit(head, carry):
        attend(head_tiles(0, (0,), head), True)
        return carry

    with jax.named_scope('own'):
        lax.fori_loop(0, kv_heads, own_unit, 0)

    def far_unit(rel, ccs, head):
        with jax.named_scope('far'):
            attend(head_tiles(rel, ccs, head), False)

    has_left = chip >= 1
    has_right = chip >= 3
    has_far = chip >= 2
    fwd_right = jnp.logical_and(chip >= 1, chip <= 2)

    def take_head_zero():
        @pl.when(has_left)
        def _():
            own_to(1, 0, 0, x_right).wait_recv()

            @pl.when(fwd_right)
            def _():
                far_k(0).start()

            fwd_sib(1, 0).start()

        @pl.when(has_right)
        def _():
            own_to(2, 0, 0, x_left).wait_recv()
            far_v(0).start()
            fwd_sib(2, 0).start()

        @pl.when(chip == 0)
        def _():
            left_v(0).wait_recv()
            far_v(0).start()

    def take_head_one(i):
        @pl.when(has_left)
        def _():
            own_chunk(1, 1, x_right, i * half_chunks, half_chunks, i == 1).wait_recv()

            @pl.when(fwd_right)
            def _():
                far_k(1, key_halves[i]).start()

            if i == 1:
                fwd_sib(1, 1).start()

        @pl.when(has_right)
        def _():
            own_chunk(2, 1, x_left, i * half_chunks, half_chunks, i == 1).wait_recv()
            far_v(1, key_halves[i]).start()
            if i == 1:
                fwd_sib(2, 1).start()

        @pl.when(chip == 0)
        def _():
            left_v(1, key_halves[i], i == 1).wait_recv()
            far_v(1, key_halves[i]).start()

    @pl.when(core == 1)
    def _():
        own_to(0, 1, 0, sibling).wait_recv()
        own_to(0, 1, 1, sibling).wait_recv()

    take_head_zero()
    head_one(1)

    ends = jnp.logical_or(chip == 0, chip == 3)

    def wx_late(c):
        @pl.when(fwd_right)
        def _():
            wx_own(0, c, chip).start()

        @pl.when(ends)
        def _():
            wx_own(1, c, chip).start()

    for c in range(2):
        wo_part(c, 1).wait_recv()

        @pl.when(ends)
        def _(c=c):
            wx_own(0, c, chip).start()

        @pl.when(fwd_right)
        def _(c=c):
            wx_own(1, c, chip).start()

    def sibling_unit(head, carry):
        far_unit(0, (1,), head)
        return carry

    @pl.when(core == 1)
    def _():
        lax.fori_loop(0, kv_heads, sibling_unit, 0)

    def seg(index):
        return pl.ds(pl.multiple_of(index * seg_rows, seg_rows), seg_rows)

    own_seg, far_seg = tp, (tp + 2) % ring
    mate_seg = ((tp + ring + turn) % ring, (tp + ring - turn) % ring)

    head_cols = group_size * HEAD

    def o_part(c, which, head):
        hc = slice(head * head_cols, (head + 1) * head_cols)
        return remote(o_v.at[seg(mate_seg[c] if which else far_seg), hc], ox_v.at[c, which, :, hc],
                      o_send.at[c, which, head], o_recv.at[c, which, head], y_mate[c])

    def finish_rows(head, rs):
        for qi in range(head * group_size, (head + 1) * group_size):
            o_v[rs, qi * HEAD:(qi + 1) * HEAD] = (acc_v[qi, :, rs] * (1.0 / l_v[qi, :, rs])).astype(BF).T

    loads[3].wait()

    def sib_wait(rel, head):
        remote(kv_v.at[rel, 0, head], kv_v.at[rel, 1, head], kv_fwd_send.at[rel, head], kv_recv.at[rel, 1, head], sibling).wait_recv()

    shift = (chip // (ring - 1)) * (1 - core)

    def side_unit(u, carry):
        head = u // 3
        rel = 1 + u % 3
        need = ((rel == 1) & has_left) | ((rel == 2) & has_right) | ((rel == 3) & has_far)

        @pl.when((u == 0) & has_left)
        def _():
            sib_wait(1, 0)

        at = u - shift

        @pl.when((at == 1) & has_far)
        def _():
            with jax.named_scope('far_h0'):
                far_k(0).wait_recv()
                far_v(0).wait_recv()
                fwd_sib(3, 0).start()

        @pl.when((u == 1) & has_right)
        def _():
            sib_wait(2, 0)

        @pl.when(u == 1)
        def _():
            take_head_one(0)

        @pl.when(at == 2)
        def _():
            with jax.named_scope('take_h1'):
                take_head_one(1)
                for c in range(2):
                    wx_late(c)

        @pl.when((u == 2) & has_far)
        def _():
            sib_wait(3, 0)

        @pl.when(u == 3)
        def _():
            finish_rows(0, slice(0, rows))
            for c in range(2):
                o_part(c, 0, 0).start()
            for c in range(2):
                o_part(c, 1, 0).start()

        @pl.when((u == 3) & (chip < 2))
        def _():
            with jax.named_scope('wx_wait'):
                for c in range(2):
                    for d in range(2):
                        wx_own(d, c, chip_right if d else chip_left).wait_recv()
                        wx_pass(d, c, chip_right if d else chip_left).start()

        @pl.when((u == 3) & has_left)
        def _():
            sib_wait(1, 1)

        @pl.when(need)
        def _():
            far_unit(rel, (0, 1), head)

        return carry

    lax.fori_loop(0, 4, side_unit, 0)

    @pl.when(has_far)
    def _():
        with jax.named_scope('far_h1'):
            far_k(1).wait_recv()
            far_v(1).wait_recv()
            fwd_sib(3, 1).start()

    @pl.when(has_far)
    def _():
        sib_wait(3, 1)

    @pl.when(has_right)
    def _():
        sib_wait(2, 1)

    def col(c, g):
        return pl.ds(pl.multiple_of(c * half + g * cols, cols), cols)

    def two_mates(c, g, own_rows, which):
        g0 = pl.multiple_of(g * cols, cols)
        return (jnp.dot(o_v[seg(own_rows), :], wo_v[:, col(c, g)], preferred_element_type=F32)
                + jnp.dot(ox_v[c, which], wox_v[c, :, pl.ds(g0, cols)], preferred_element_type=F32))

    def cross(c, g):
        return remote(part_v.at[c, g], recv_v.at[c, g], part_send.at[c, g], part_recv.at[c, g], y_mate[1 - c])

    def f1(c, g, d, owner):
        block = out_v.at[seg(owner), col(c, g)]
        return remote(block, block, f1_send.at[c, g, d], f1_recv.at[c, g, d], y_left if d else y_right)

    def f2(g, d, owner):
        block = out_v.at[seg(owner), col(d, g)]
        return remote(block, block, f2_send.at[g, d], f2_recv.at[g, d], y_left if d else y_right)

    def project_cross(g, carry):
        for c in range(2):
            part_v[c, g] = two_mates(c, g, mate_seg[1 - c], 0).astype(BF)
            cross(c, g).start()
        return carry

    def seg_step(j, carry):
        index = (tp + ring + 2 * ((3 - j) // 3) + turn * ((j % 3) % 2) - turn * (j // 2 - j // 3)) % ring
        rs = seg(index)

        @pl.when(j == 3)
        def _():
            with jax.named_scope('mates'):
                for c in range(2):
                    for kind in range(2):
                        wo_share(c, kind, 1 - core).wait_recv()
                    for head in range(kv_heads):
                        o_part(c, 0, head).wait_recv()
            with jax.named_scope('cross'):
                lax.fori_loop(0, CHUNKS, project_cross, 0)

        def seg_tiles(*rels):
            return [(rel, (0, 1), 1, group_size + g, rs, 0) for rel in rels for g in range(group_size)]

        @pl.when(has_right)
        def _():
            with jax.named_scope('far_seg'):
                attend(seg_tiles(2, 3), False)

        @pl.when(has_far & (chip < 3))
        def _():
            with jax.named_scope('far_seg'):
                attend(seg_tiles(3), False)

        finish_rows(1, rs)

        @pl.when(j == 0)
        def _():
            for c in range(2):
                o_part(c, 0, 1).start()
            with jax.named_scope('wo_wait'):
                for c in range(2):
                    wo_part(c, 0).wait_recv()
                    wo_share(c, 0, core).start()

        @pl.when(j == 1)
        def _():
            o_part(0, 1, 1).start()
            with jax.named_scope('sub_wait'):
                @pl.when(has_far)
                def _():
                    for d in range(2):
                        for c in range(2):
                            wx_own(d, c, chip_right if d else chip_left).wait_recv()

                for d, gets in ((0, fwd_right), (1, ends)):
                    @pl.when(gets)
                    def _(d=d):
                        for c in range(2):
                            wx_pass(d, c, chip_far).wait_recv()

                for c in range(2):
                    wo_share(c, 1, core).start()

        @pl.when(j == 2)
        def _():
            o_part(1, 1, 1).start()

        return carry

    with jax.named_scope('segs'):
        lax.fori_loop(0, ring, seg_step, 0)

    with jax.named_scope('caches'):
        k_out[...] = kc_v[...].reshape(k_out.shape)
        v_out[...] = vc_v[...].reshape(v_out.shape)

    for c in range(2):
        for head in range(kv_heads):
            o_part(c, 1, head).wait_recv()

    def project_own(g, carry):
        for c in range(2):
            attn = two_mates(c, g, own_seg, 1)
            cross(c, g).wait_recv()
            attn = attn + recv_v[c, g].astype(F32)
            out_v[seg(own_seg), col(c, g)] = (x_v[seg(own_seg), col(c, g)].astype(F32) + attn).astype(BF)
            for d in range(2):
                f1(c, g, d, own_seg).start()
        return carry

    with jax.named_scope('own_out'):
        lax.fori_loop(0, CHUNKS, project_own, 0)

    side_seg = ((tp + ring - 1) % ring, (tp + 1) % ring)

    def pass_on(g, carry):
        for d in range(2):
            f1(d, g, d, side_seg[d]).wait_recv()
            f2(g, d, side_seg[d]).start()
        return carry

    with jax.named_scope('pass_on'):
        lax.fori_loop(0, CHUNKS, pass_on, 0)

    def finish(g, carry):
        for d in range(2):
            f1(1 - d, g, d, side_seg[d]).wait_recv()
            f2(g, d, far_seg).wait_recv()
        return carry

    with jax.named_scope('finish'):
        lax.fori_loop(0, CHUNKS, finish, 0)

    def drain(g, carry):
        for d in range(2):
            cross(d, g).wait_send()
            f2(g, d, side_seg[d]).wait_send()
            for c in range(2):
                f1(c, g, d, own_seg).wait_send()
        return carry

    with jax.named_scope('drain'):
        lax.fori_loop(0, CHUNKS, drain, 0)
    for c in range(2):
        @pl.when(chip < 2)
        def _(c=c):
            for d in range(2):
                wx_pass(d, c, chip_right if d else chip_left).wait_send()

        for i in range(2):
            wo_part(c, i).wait_send()
            wx_own(i, c, chip).wait_send()
            wo_share(c, i, core).wait_send()
            for head in range(kv_heads):
                o_part(c, i, head).wait_send()

    @pl.when(core == 0)
    def _():
        own_to(0, 1, 0, sibling).wait_send()
        own_to(0, 1, 1, sibling).wait_send()

    for head in range(kv_heads):
        @pl.when(right_sends)
        def _(head=head):
            own_to(1, 0, head, x_right).wait_send()

        @pl.when(chip == 0)
        def _(head=head):
            own_to(2, 0, head, x_left).wait_send()

        @pl.when(chip == 1)
        def _(head=head):
            left_v(head).wait_send()

        @pl.when(fwd_right)
        def _(head=head):
            far_k(head).wait_send()

        @pl.when(jnp.logical_or(chip == 0, has_right))
        def _(head=head):
            far_v(head).wait_send()

        for rel, sent in ((1, has_left), (2, has_right), (3, has_far)):
            @pl.when(sent)
            def _(rel=rel, head=head):
                fwd_sib(rel, head).wait_send()


def solution(mesh):
    ring = mesh.shape['tp']
    if mesh.shape['cp'] != 2 * ring or ring != 4:
        raise ValueError('mesh')
    row_spec = P(('dp', 'cp'), None)
    cache_spec = P(('dp', 'cp'), 'tp', None)
    head_cols = P(None, 'tp')

    def local_block(hidden, positions, norm_gain, w_query, w_key, w_value, w_out):
        rows, width = hidden.shape
        kv_heads = w_key.shape[1] // HEAD
        q_heads = w_query.shape[1] // HEAD
        seg_rows, half = rows // ring, width // 2
        cols = half // CHUNKS
        dma = pltpu.SemaphoreType.DMA
        out, k_new, v_new = pl.pallas_call(
            lambda *refs: block_kernel(ring, kv_heads, q_heads // kv_heads, *refs),
            out_shape=(
                pltpu.VMEM((rows, width), BF),
                pltpu.VMEM((rows, kv_heads, HEAD), BF),
                pltpu.VMEM((rows, kv_heads, HEAD), BF),
            ),
            in_specs=[pl.BlockSpec(memory_space=pl.ANY)] + [pl.BlockSpec(memory_space=pltpu.VMEM)] * 3
            + [pl.BlockSpec(memory_space=pl.ANY)] * 4,
            out_specs=[pl.BlockSpec(memory_space=pltpu.VMEM)] * 3,
            scratch_shapes=[
                pltpu.VMEM((rows, width), BF),
                pltpu.VMEM((rows, width), BF),
                pltpu.VMEM(w_query.shape, BF),
                pltpu.VMEM((width, 2 * kv_heads * HEAD), BF),
                pltpu.VMEM(w_out.shape, BF),
                pltpu.VMEM((rows, HEAD), F32),
                pltpu.VMEM((rows, HEAD), F32),
                pltpu.VMEM((rows, kv_heads * HEAD), BF),
                pltpu.VMEM((rows, kv_heads * HEAD), BF),
                pltpu.VMEM((q_heads, HEAD, rows), BF),
                pltpu.VMEM((4, 2, kv_heads, 2, rows, HEAD), BF),
                pltpu.VMEM((q_heads, 1, rows), F32),
                pltpu.VMEM((q_heads, 1, rows), F32),
                pltpu.VMEM((q_heads, HEAD, rows), F32),
                pltpu.VMEM((rows, q_heads * HEAD), BF),
                pltpu.VMEM((2, q_heads * HEAD, half), BF),
                pltpu.VMEM((2, 2, seg_rows, q_heads * HEAD), BF),
                pltpu.VMEM((2, CHUNKS, seg_rows, cols), BF),
                pltpu.VMEM((2, CHUNKS, seg_rows, cols), BF),
                dma((4 + LOAD_CHUNKS,)),
                dma((3, kv_heads)),
                dma((4, 2, kv_heads)),
                dma((4, kv_heads)),
                dma((kv_heads, 2)), dma((kv_heads, 2)), dma((3,)),
                dma((2, 2)), dma((2, 2)), dma((2, 2)), dma((2, 2)), dma((2, 2)), dma((2, 2)), dma((2, 2)), dma((2, 2)),
                dma((2, 2, kv_heads)), dma((2, 2, kv_heads)),
                dma((2, CHUNKS)), dma((2, CHUNKS)),
                dma((2, CHUNKS, 2)), dma((2, CHUNKS, 2)),
                dma((CHUNKS, 2)), dma((CHUNKS, 2)),
            ],
            compiler_params=pltpu.CompilerParams(collective_id=0, has_side_effects=True, vmem_limit_bytes=60 * 1024 * 1024),
            name='attn_block',
        )(hidden, positions, norm_gain, jnp.asarray(inverse_freq()), w_query, w_key, w_value, w_out)
        return out, k_new, v_new

    return jax.shard_map(local_block, mesh=mesh,
                         in_specs=(row_spec, P(('dp', 'cp')), P(None), head_cols, head_cols, head_cols, P('tp', None)),
                         out_specs=(row_spec, cache_spec, cache_spec), check_vma=False)
```

```python
import math
import jax
import jax.numpy as jnp
import numpy as np
from jax import lax
from jax.experimental import pallas as pl
from jax.experimental.pallas import tpu as pltpu
from jax.sharding import PartitionSpec as P

HEAD = 128
EPS = 1e-5
LOG_THETA = math.log(1000000.0)
SCORE_EXP2 = math.log2(math.e) / math.sqrt(HEAD)
BF = jnp.bfloat16
F32 = jnp.float32
CHUNKS = 3
Q_TILE = 256
NORM_ROWS = 32
LOAD_CHUNKS = 4
SHARED_ROWS = 96


def inverse_freq():
    half = np.exp(np.arange(HEAD // 2, dtype=np.float64) * (-2.0 * LOG_THETA / HEAD)).astype(np.float32)
    return np.concatenate([half, half])[None, :]


def block_kernel(ring, kv_heads, group_size,
                 x_hbm, pos_hbm, gain_hbm, freq_hbm, wq_hbm, wk_hbm, wv_hbm, wo_hbm,
                 out_v, k_out, v_out,
                 pos_ref, gain_ref, freq_ref, x_v, h_v, wq_v, wkv_v, wo_v, cos_v, sin_v, kc_v, vc_v, q_v, kv_v, m_v, l_v, acc_v, o_v,
                 wox_v, ox_v, part_v, recv_v,
                 load_sem, kv_send, kv_recv, kv_fwd_send, far_send, far_recv, late_recv,
                 wo_send, wo_recv, wx_send, wx_recv, wf_send, wf_recv, wo_fwd_send, wo_fwd_recv, o_send, o_recv, part_send, part_recv,
                 f1_send, f1_recv, f2_send, f2_recv):
    rows, width = x_v.shape
    cp = lax.axis_index('cp')
    tp = lax.axis_index('tp')
    chip = cp // 2
    core = cp % 2
    seg_rows = rows // ring
    half = width // 2
    cols = half // CHUNKS
    k_half = wo_v.shape[0] // 2

    x_right = {'cp': ((chip + 1) % ring) * 2 + core}
    x_left = {'cp': ((chip + ring - 1) % ring) * 2 + core}
    sibling = {'cp': chip * 2 + 1 - core}
    y_right = {'tp': (tp + 1) % ring}
    y_left = {'tp': (tp + ring - 1) % ring}
    turn = 1 - 2 * (tp % 2)
    y_mate = ({'tp': (tp + ring + turn) % ring}, {'tp': (tp + ring - turn) % ring})

    barrier = pltpu.get_barrier_semaphore()
    for peer in (x_right, x_left, sibling, y_right, y_left):
        pl.semaphore_signal(barrier, inc=1, device_id=peer, device_id_type=pl.DeviceIdType.MESH)

    kv_cols = kv_heads * HEAD
    chunk = rows // LOAD_CHUNKS
    x_loads = [pltpu.make_async_copy(x_hbm.at[i * chunk:(i + 1) * chunk, :], x_v.at[i * chunk:(i + 1) * chunk, :],
                                     load_sem.at[4 + i]) for i in range(LOAD_CHUNKS)]
    loads = [
        pltpu.make_async_copy(wk_hbm, wkv_v.at[0], load_sem.at[0]),
        pltpu.make_async_copy(wv_hbm, wkv_v.at[1], load_sem.at[1]),
        pltpu.make_async_copy(wq_hbm, wq_v, load_sem.at[2]),
        pltpu.make_async_copy(wo_hbm, wo_v, load_sem.at[3]),
    ]
    small = [pltpu.make_async_copy(src, dst, load_sem.at[4 + LOAD_CHUNKS + i])
             for i, (src, dst) in enumerate(((pos_hbm, pos_ref), (freq_hbm, freq_ref), (gain_hbm, gain_ref)))]
    for copy in small + x_loads[:1] + loads[:2] + x_loads[1:]:
        copy.start()

    with jax.named_scope('load_wait'):
        for copy in small:
            copy.wait()
        pos = pos_ref[...].astype(F32).reshape(rows // HEAD, HEAD)
        pos = jnp.concatenate([pos, jnp.zeros((8 - rows // HEAD, HEAD), F32)], axis=0).T
        first = lax.broadcasted_iota(jnp.int32, (1, HEAD), 1) < HEAD // 2
        def tables(i):
            k = i + rows // HEAD // 2
            angles = jnp.where(first, pos[:, i:i + 1], pos[:, k:k + 1]) * freq_ref[...]
            cos_t, sin_t = jnp.cos(angles), jnp.sin(angles)
            cos_r, sin_r = pltpu.roll(cos_t, HEAD // 2, 1), pltpu.roll(sin_t, HEAD // 2, 1)
            for row, lo_c, hi_c, lo_s, hi_s in ((i, cos_t, cos_r, sin_t, sin_r), (k, cos_r, cos_t, sin_r, sin_t)):
                cos_v[row * HEAD:(row + 1) * HEAD, :] = jnp.where(first, lo_c, hi_c)
                sin_v[row * HEAD:(row + 1) * HEAD, :] = jnp.where(first, -lo_s, hi_s)

        for i in range(rows // HEAD // 2):
            tables(i)

    def remote(src, dst, send, recv, peer):
        return pltpu.make_async_remote_copy(src_ref=src, dst_ref=dst, send_sem=send, recv_sem=recv,
                                            device_id=peer, device_id_type=pl.DeviceIdType.MESH)

    with jax.named_scope('barrier'):
        pl.semaphore_wait(barrier, 5)

    base = core * k_half
    direct_rows = k_half - SHARED_ROWS
    sub_cols = half // ring

    def shared_rows(from_core):
        return pl.ds(pl.multiple_of(from_core * k_half + direct_rows, 32), SHARED_ROWS)

    def sub_at(c, index):
        return wox_v.at[c, shared_rows(core), pl.ds(pl.multiple_of(index * sub_cols, sub_cols), sub_cols)]

    def wo_part(c, kind):
        if kind:
            src = wo_hbm.at[shared_rows(core), pl.ds(pl.multiple_of(c * half + chip * sub_cols, sub_cols), sub_cols)]
            dst = sub_at(c, chip)
        else:
            ks = pl.ds(pl.multiple_of(base, 32), direct_rows)
            src, dst = wo_hbm.at[ks, c * half:(c + 1) * half], wox_v.at[c, ks, :]
        return remote(src, dst, wo_send.at[c, kind], wo_recv.at[c, kind], y_mate[c])

    def wx_own(d, c, index):
        return remote(sub_at(c, index), sub_at(c, index), wx_send.at[d, c], wx_recv.at[d, c], x_left if d else x_right)

    def wx_pass(d, c, index):
        return remote(sub_at(c, index), sub_at(c, index), wf_send.at[d, c], wf_recv.at[d, c], x_left if d else x_right)

    def wo_share(c, kind, from_core):
        ks = shared_rows(from_core) if kind else pl.ds(pl.multiple_of(from_core * k_half, 32), direct_rows)
        part = wox_v.at[c, ks, :]
        return remote(part, part, wo_fwd_send.at[c, kind], wo_fwd_recv.at[c, kind], sibling)

    chip_left, chip_right, chip_far = (chip + ring - 1) % ring, (chip + 1) % ring, (chip + 2) % ring

    for c in range(2):
        wo_part(c, 1).start()
    for c in range(2):
        wo_part(c, 0).start()

    def norm_rows(r0, count):
        xf = x_v[pl.ds(r0, count), :].astype(F32)
        inv = lax.rsqrt(jnp.mean(xf * xf, axis=-1, keepdims=True) + EPS)
        h_v[pl.ds(r0, count), :] = (xf * inv * gain_ref[...].astype(F32).reshape(1, width)).astype(BF)

    def norm_step(i, carry):
        norm_rows(pl.multiple_of(i * NORM_ROWS, NORM_ROWS), NORM_ROWS)
        return carry

    def rope(vals, rs=slice(None)):
        return (vals * cos_v[rs, :] + pltpu.roll(vals, HEAD // 2, 1) * sin_v[rs, :]).astype(BF)

    def own_to(rel, cc, head, peer):
        return remote(kv_v.at[0, 0, head], kv_v.at[rel, cc, head],
                      kv_send.at[rel, head], kv_recv.at[rel, cc, head], peer)

    def piece_sem(rel, head, late):
        return late_recv.at[rel] if late else kv_recv.at[rel, 0, head]

    def own_chunk(rel, head, peer, i, count=1, late=False):
        ks = slice(i * chunk, (i + count) * chunk)
        return remote(kv_v.at[0, 0, head, :, ks, :], kv_v.at[rel, 0, head, :, ks, :],
                      kv_send.at[rel, head], piece_sem(rel, head, late), peer)

    def left_v(head, ks=slice(None), late=False):
        return remote(kv_v.at[0, 0, head, 1, ks, :], kv_v.at[2, 0, head, 1, ks, :],
                      kv_send.at[2, head], piece_sem(2, head, late), x_left)

    half_chunks = LOAD_CHUNKS // 2
    key_halves = (slice(0, half_chunks * chunk), slice(half_chunks * chunk, rows))

    def far_k(head, ks=slice(None)):
        return remote(kv_v.at[1, 0, head, 0, ks, :], kv_v.at[3, 0, head, 0, ks, :], far_send.at[head, 0], far_recv.at[head, 0], x_right)

    def far_v(head, ks=slice(None)):
        return remote(kv_v.at[2, 0, head, 1, ks, :], kv_v.at[3, 0, head, 1, ks, :], far_send.at[head, 1], far_recv.at[head, 1], x_left)

    def fwd_sib(rel, head):
        return remote(kv_v.at[rel, 0, head], kv_v.at[rel, 1, head],
                      kv_fwd_send.at[rel, head], kv_recv.at[rel, 1, head], sibling)

    right_sends = chip < ring - 1

    x_loads[0].wait()
    with jax.named_scope('norm'):
        lax.fori_loop(0, chunk // NORM_ROWS, norm_step, 0)
    loads[2].start()
    for copy in loads[:2]:
        copy.wait()
    steps = ((0, 1), (1, 1), (2, LOAD_CHUNKS - 2))
    for n, (i, count) in enumerate(steps):
        ahead = steps[n + 1] if n + 1 < len(steps) else (0, 0)
        for k in range(ahead[0], sum(ahead)):
            x_loads[k].wait()
        ks = slice(i * chunk, (i + count) * chunk)
        with jax.named_scope('kv_proj'):
            k_proj, v_proj = (jnp.dot(h_v[ks, :], wkv_v[w], preferred_element_type=F32) for w in range(2))
            for r in range(ahead[0] * chunk, sum(ahead) * chunk, 16):
                norm_rows(r, 16)
            for h in range(kv_heads):
                hc = slice(h * HEAD, (h + 1) * HEAD)
                k_head = rope(k_proj[:, hc], ks)
                kv_v[0, 0, h, 0, ks, :] = k_head
                kc_v[ks, hc] = k_head
                v_head = v_proj[:, hc].astype(BF)
                vc_v[ks, hc] = v_head
                for k in range(count):
                    kv_v[0, 0, h, 1, (i + k) * chunk:(i + k + 1) * chunk, :] = v_head[k * chunk:(k + 1) * chunk, :].T

        @pl.when(right_sends)
        def _(i=i, count=count):
            own_chunk(1, 0, x_right, i, count).start()

        @pl.when(chip == 0)
        def _(i=i, count=count):
            own_chunk(2, 0, x_left, i, count).start()

        @pl.when(chip == 1)
        def _(ks=ks):
            left_v(0, ks).start()

    loads[3].start()

    @pl.when(core == 0)
    def _():
        own_to(0, 1, 0, sibling).start()
        own_to(0, 1, 1, sibling).start()

    def head_one(i):
        @pl.when(right_sends)
        def _():
            own_chunk(1, 1, x_right, i * half_chunks, half_chunks, i == 1).start()

        @pl.when(chip == 0)
        def _():
            own_chunk(2, 1, x_left, i * half_chunks, half_chunks, i == 1).start()

        @pl.when(chip == 1)
        def _():
            left_v(1, key_halves[i], i == 1).start()

    head_one(0)
    loads[2].wait()

    with jax.named_scope('q_proj'):
        q_pair = None
        for j in range(kv_heads * group_size // 2 + 1):
            last = q_pair
            if j < kv_heads * group_size // 2:
                q_pair = jnp.dot(h_v[...], wq_v[:, j * 2 * HEAD:(j + 1) * 2 * HEAD], preferred_element_type=F32)
            if j > 0:
                q_v[2 * j - 2] = rope(last[:, :HEAD]).T
                q_v[2 * j - 1] = rope(last[:, HEAD:]).T

    def attend(tiles, first):
        def start(tile):
            rel, ccs, head, qi, rs, r0 = tile
            keys = r0 + Q_TILE if first else rows
            q_t = q_v[qi, :, rs]
            s = jnp.concatenate([jnp.dot(kv_v[rel, cc, head, 0, :keys, :], q_t, preferred_element_type=F32) for cc in ccs], axis=0)
            if first:
                key_id = lax.broadcasted_iota(jnp.int32, s.shape, 0)
                row_id = lax.broadcasted_iota(jnp.int32, s.shape, 1) + r0
                s = jnp.where(key_id <= row_id, s, -jnp.inf)
            return s

        def soften(tile, s):
            rel, ccs, head, qi, rs, r0 = tile
            m_new = jnp.max(s, axis=0, keepdims=True)
            alpha = None
            if not first:
                m_old = m_v[qi, :, rs]
                m_new = jnp.maximum(m_old, m_new)
                alpha = jnp.exp2((m_old - m_new) * SCORE_EXP2)
            p = jnp.exp2((s - m_new) * SCORE_EXP2)
            l_new = jnp.sum(p, axis=0, keepdims=True)
            l_v[qi, :, rs] = l_new if first else l_v[qi, :, rs] * alpha + l_new
            m_v[qi, :, rs] = m_new
            return p.astype(BF), alpha

        def gather(tile, p, alpha):
            rel, ccs, head, qi, rs, r0 = tile
            keys = r0 + Q_TILE if first else rows
            v_t = jnp.concatenate([kv_v[rel, cc, head, 1, j * HEAD:(j + 1) * HEAD, :] for cc in ccs for j in range(keys // HEAD)], axis=1)
            o_new = jnp.dot(v_t, p, preferred_element_type=F32)
            acc_v[qi, :, rs] = o_new if first else acc_v[qi, :, rs] * alpha + o_new

        s = start(tiles[0])
        held = None
        for i in range(len(tiles) + 1):
            s_next = start(tiles[i + 1]) if i + 1 < len(tiles) else None
            if held is not None:
                gather(tiles[i - 1], *held)
            if i < len(tiles):
                held = soften(tiles[i], s)
            s = s_next

    def head_tiles(rel, ccs, head):
        return [(rel, ccs, head, head * group_size + g, slice(rt * Q_TILE, (rt + 1) * Q_TILE), rt * Q_TILE)
                for g in range(group_size) for rt in range(rows // Q_TILE)]

    def own_unit(head, carry):
        attend(head_tiles(0, (0,), head), True)
        return carry

    with jax.named_scope('own'):
        lax.fori_loop(0, kv_heads, own_unit, 0)

    def far_unit(rel, ccs, head):
        with jax.named_scope('far'):
            attend(head_tiles(rel, ccs, head), False)

    has_left = chip >= 1
    has_right = chip >= 3
    has_far = chip >= 2
    fwd_right = jnp.logical_and(chip >= 1, chip <= 2)

    def take_head_zero():
        @pl.when(has_left)
        def _():
            own_to(1, 0, 0, x_right).wait_recv()

            @pl.when(fwd_right)
            def _():
                far_k(0).start()

            fwd_sib(1, 0).start()

        @pl.when(has_right)
        def _():
            own_to(2, 0, 0, x_left).wait_recv()
            far_v(0).start()
            fwd_sib(2, 0).start()

        @pl.when(chip == 0)
        def _():
            left_v(0).wait_recv()
            far_v(0).start()

    def take_head_one(i):
        @pl.when(has_left)
        def _():
            own_chunk(1, 1, x_right, i * half_chunks, half_chunks, i == 1).wait_recv()

            @pl.when(fwd_right)
            def _():
                far_k(1, key_halves[i]).start()

            if i == 1:
                fwd_sib(1, 1).start()

        @pl.when(has_right)
        def _():
            own_chunk(2, 1, x_left, i * half_chunks, half_chunks, i == 1).wait_recv()
            far_v(1, key_halves[i]).start()
            if i == 1:
                fwd_sib(2, 1).start()

        @pl.when(chip == 0)
        def _():
            left_v(1, key_halves[i], i == 1).wait_recv()
            far_v(1, key_halves[i]).start()

    @pl.when(core == 1)
    def _():
        own_to(0, 1, 0, sibling).wait_recv()
        own_to(0, 1, 1, sibling).wait_recv()

    take_head_zero()
    head_one(1)

    ends = jnp.logical_or(chip == 0, chip == 3)

    def wx_late(c):
        @pl.when(fwd_right)
        def _():
            wx_own(0, c, chip).start()

        @pl.when(ends)
        def _():
            wx_own(1, c, chip).start()

    for c in range(2):
        wo_part(c, 1).wait_recv()

        @pl.when(ends)
        def _(c=c):
            wx_own(0, c, chip).start()

        @pl.when(fwd_right)
        def _(c=c):
            wx_own(1, c, chip).start()

    def sibling_unit(head, carry):
        far_unit(0, (1,), head)
        return carry

    @pl.when(core == 1)
    def _():
        lax.fori_loop(0, kv_heads, sibling_unit, 0)

    def seg(index):
        return pl.ds(pl.multiple_of(index * seg_rows, seg_rows), seg_rows)

    own_seg, far_seg = tp, (tp + 2) % ring
    mate_seg = ((tp + ring + turn) % ring, (tp + ring - turn) % ring)

    head_cols = group_size * HEAD

    def o_part(c, which, head):
        hc = slice(head * head_cols, (head + 1) * head_cols)
        return remote(o_v.at[seg(mate_seg[c] if which else far_seg), hc], ox_v.at[c, which, :, hc],
                      o_send.at[c, which, head], o_recv.at[c, which, head], y_mate[c])

    def finish_rows(head, rs):
        for qi in range(head * group_size, (head + 1) * group_size):
            o_v[rs, qi * HEAD:(qi + 1) * HEAD] = (acc_v[qi, :, rs] * (1.0 / l_v[qi, :, rs])).astype(BF).T

    loads[3].wait()

    def sib_wait(rel, head):
        remote(kv_v.at[rel, 0, head], kv_v.at[rel, 1, head], kv_fwd_send.at[rel, head], kv_recv.at[rel, 1, head], sibling).wait_recv()

    shift = (chip // (ring - 1)) * (1 - core)

    def side_unit(u, carry):
        head = u // 3
        rel = 1 + u % 3
        need = ((rel == 1) & has_left) | ((rel == 2) & has_right) | ((rel == 3) & has_far)

        @pl.when((u == 0) & has_left)
        def _():
            sib_wait(1, 0)

        at = u - shift

        @pl.when((at == 1) & has_far)
        def _():
            with jax.named_scope('far_h0'):
                far_k(0).wait_recv()
                far_v(0).wait_recv()
                fwd_sib(3, 0).start()

        @pl.when((u == 1) & has_right)
        def _():
            sib_wait(2, 0)

        @pl.when(u == 1)
        def _():
            take_head_one(0)

        @pl.when(at == 2)
        def _():
            with jax.named_scope('take_h1'):
                take_head_one(1)
                for c in range(2):
                    wx_late(c)

        @pl.when((u == 2) & has_far)
        def _():
            sib_wait(3, 0)

        @pl.when(u == 3)
        def _():
            finish_rows(0, slice(0, rows))
            for c in range(2):
                o_part(c, 0, 0).start()
            for c in range(2):
                o_part(c, 1, 0).start()

        @pl.when((u == 3) & (chip < 2))
        def _():
            with jax.named_scope('wx_wait'):
                for c in range(2):
                    for d in range(2):
                        wx_own(d, c, chip_right if d else chip_left).wait_recv()
                        wx_pass(d, c, chip_right if d else chip_left).start()

        @pl.when((u == 3) & has_left)
        def _():
            sib_wait(1, 1)

        @pl.when(need)
        def _():
            far_unit(rel, (0, 1), head)

        return carry

    lax.fori_loop(0, 4, side_unit, 0)

    @pl.when(has_far)
    def _():
        with jax.named_scope('far_h1'):
            far_k(1).wait_recv()
            far_v(1).wait_recv()
            fwd_sib(3, 1).start()

    @pl.when(has_right)
    def _():
        sib_wait(2, 1)

    def col(c, g):
        return pl.ds(pl.multiple_of(c * half + g * cols, cols), cols)

    def two_mates(c, g, own_rows, which):
        g0 = pl.multiple_of(g * cols, cols)
        return (jnp.dot(o_v[seg(own_rows), :], wo_v[:, col(c, g)], preferred_element_type=F32)
                + jnp.dot(ox_v[c, which], wox_v[c, :, pl.ds(g0, cols)], preferred_element_type=F32))

    def cross(c, g):
        return remote(part_v.at[c, g], recv_v.at[c, g], part_send.at[c, g], part_recv.at[c, g], y_mate[1 - c])

    def f1(c, g, d, owner):
        block = out_v.at[seg(owner), col(c, g)]
        return remote(block, block, f1_send.at[c, g, d], f1_recv.at[c, g, d], y_left if d else y_right)

    def f2(g, d, owner):
        block = out_v.at[seg(owner), col(d, g)]
        return remote(block, block, f2_send.at[g, d], f2_recv.at[g, d], y_left if d else y_right)

    def project_cross(g, carry):
        for c in range(2):
            part_v[c, g] = two_mates(c, g, mate_seg[1 - c], 0).astype(BF)
            cross(c, g).start()
        return carry

    def seg_step(j, carry):
        index = (tp + ring + 2 * ((3 - j) // 3) + turn * ((j % 3) % 2) - turn * (j // 2 - j // 3)) % ring
        rs = seg(index)

        @pl.when(j == 3)
        def _():
            with jax.named_scope('mates'):
                for c in range(2):
                    for kind in range(2):
                        wo_share(c, kind, 1 - core).wait_recv()
                    for head in range(kv_heads):
                        o_part(c, 0, head).wait_recv()
            with jax.named_scope('cross'):
                lax.fori_loop(0, CHUNKS, project_cross, 0)

        def seg_tiles(*rels):
            return [(rel, (0, 1), 1, group_size + g, rs, 0) for rel in rels for g in range(group_size)]

        @pl.when(has_right)
        def _():
            with jax.named_scope('right_seg'):
                attend(seg_tiles(2), False)

        @pl.when((j == 0) & has_far)
        def _():
            sib_wait(3, 1)

        @pl.when(has_far)
        def _():
            with jax.named_scope('far_seg'):
                attend(seg_tiles(3), False)

        finish_rows(1, rs)

        @pl.when(j == 0)
        def _():
            for c in range(2):
                o_part(c, 0, 1).start()
            with jax.named_scope('wo_wait'):
                for c in range(2):
                    wo_part(c, 0).wait_recv()
                    wo_share(c, 0, core).start()

        @pl.when(j == 1)
        def _():
            o_part(0, 1, 1).start()
            with jax.named_scope('sub_wait'):
                @pl.when(has_far)
                def _():
                    for d in range(2):
                        for c in range(2):
                            wx_own(d, c, chip_right if d else chip_left).wait_recv()

                for d, gets in ((0, fwd_right), (1, ends)):
                    @pl.when(gets)
                    def _(d=d):
                        for c in range(2):
                            wx_pass(d, c, chip_far).wait_recv()

                for c in range(2):
                    wo_share(c, 1, core).start()

        @pl.when(j == 2)
        def _():
            o_part(1, 1, 1).start()

        return carry

    with jax.named_scope('segs'):
        lax.fori_loop(0, ring, seg_step, 0)

    with jax.named_scope('caches'):
        k_out[...] = kc_v[...].reshape(k_out.shape)
        v_out[...] = vc_v[...].reshape(v_out.shape)

    for c in range(2):
        for head in range(kv_heads):
            o_part(c, 1, head).wait_recv()

    def project_own(g, carry):
        for c in range(2):
            attn = two_mates(c, g, own_seg, 1)
            cross(c, g).wait_recv()
            attn = attn + recv_v[c, g].astype(F32)
            out_v[seg(own_seg), col(c, g)] = (x_v[seg(own_seg), col(c, g)].astype(F32) + attn).astype(BF)
            for d in range(2):
                f1(c, g, d, own_seg).start()
        return carry

    with jax.named_scope('own_out'):
        lax.fori_loop(0, CHUNKS, project_own, 0)

    side_seg = ((tp + ring - 1) % ring, (tp + 1) % ring)

    def pass_on(g, carry):
        for d in range(2):
            f1(d, g, d, side_seg[d]).wait_recv()
            f2(g, d, side_seg[d]).start()
        return carry

    with jax.named_scope('pass_on'):
        lax.fori_loop(0, CHUNKS, pass_on, 0)

    def finish(g, carry):
        for d in range(2):
            f1(1 - d, g, d, side_seg[d]).wait_recv()
            f2(g, d, far_seg).wait_recv()
        return carry

    with jax.named_scope('finish'):
        lax.fori_loop(0, CHUNKS, finish, 0)

    def drain(g, carry):
        for d in range(2):
            cross(d, g).wait_send()
            f2(g, d, side_seg[d]).wait_send()
            for c in range(2):
                f1(c, g, d, own_seg).wait_send()
        return carry

    with jax.named_scope('drain'):
        lax.fori_loop(0, CHUNKS, drain, 0)
    for c in range(2):
        @pl.when(chip < 2)
        def _(c=c):
            for d in range(2):
                wx_pass(d, c, chip_right if d else chip_left).wait_send()

        for i in range(2):
            wo_part(c, i).wait_send()
            wx_own(i, c, chip).wait_send()
            wo_share(c, i, core).wait_send()
            for head in range(kv_heads):
                o_part(c, i, head).wait_send()

    @pl.when(core == 0)
    def _():
        own_to(0, 1, 0, sibling).wait_send()
        own_to(0, 1, 1, sibling).wait_send()

    for head in range(kv_heads):
        @pl.when(right_sends)
        def _(head=head):
            own_to(1, 0, head, x_right).wait_send()

        @pl.when(chip == 0)
        def _(head=head):
            own_to(2, 0, head, x_left).wait_send()

        @pl.when(chip == 1)
        def _(head=head):
            left_v(head).wait_send()

        @pl.when(fwd_right)
        def _(head=head):
            far_k(head).wait_send()

        @pl.when(jnp.logical_or(chip == 0, has_right))
        def _(head=head):
            far_v(head).wait_send()

        for rel, sent in ((1, has_left), (2, has_right), (3, has_far)):
            @pl.when(sent)
            def _(rel=rel, head=head):
                fwd_sib(rel, head).wait_send()


def copy_out(*refs):
    count = len(refs) // 2
    sems = refs[-1]
    copies = [pltpu.make_async_copy(refs[i], refs[count + i], sems.at[i]) for i in range(count)]
    for copy in copies:
        copy.start()
    for copy in copies:
        copy.wait()


def solution(mesh):
    ring = mesh.shape['tp']
    if mesh.shape['cp'] != 2 * ring or ring != 4:
        raise ValueError('mesh')
    row_spec = P(('dp', 'cp'), None)
    cache_spec = P(('dp', 'cp'), 'tp', None)
    head_cols = P(None, 'tp')

    def local_block(hidden, positions, norm_gain, w_query, w_key, w_value, w_out):
        rows, width = hidden.shape
        kv_heads = w_key.shape[1] // HEAD
        q_heads = w_query.shape[1] // HEAD
        seg_rows, half = rows // ring, width // 2
        cols = half // CHUNKS
        dma = pltpu.SemaphoreType.DMA
        out, k_new, v_new = pl.pallas_call(
            lambda *refs: block_kernel(ring, kv_heads, q_heads // kv_heads, *refs),
            out_shape=(
                pltpu.VMEM((rows, width), BF),
                pltpu.VMEM((rows, kv_heads, HEAD), BF),
                pltpu.VMEM((rows, kv_heads, HEAD), BF),
            ),
            in_specs=[pl.BlockSpec(memory_space=pl.ANY)] * 8,
            out_specs=[pl.BlockSpec(memory_space=pltpu.VMEM)] * 3,
            scratch_shapes=[
                pltpu.VMEM((rows,), jnp.int32),
                pltpu.VMEM((width,), BF),
                pltpu.VMEM((1, HEAD), F32),
                pltpu.VMEM((rows, width), BF),
                pltpu.VMEM((rows, width), BF),
                pltpu.VMEM(w_query.shape, BF),
                pltpu.VMEM((2, width, kv_heads * HEAD), BF),
                pltpu.VMEM(w_out.shape, BF),
                pltpu.VMEM((rows, HEAD), F32),
                pltpu.VMEM((rows, HEAD), F32),
                pltpu.VMEM((rows, kv_heads * HEAD), BF),
                pltpu.VMEM((rows, kv_heads * HEAD), BF),
                pltpu.VMEM((q_heads, HEAD, rows), BF),
                pltpu.VMEM((4, 2, kv_heads, 2, rows, HEAD), BF),
                pltpu.VMEM((q_heads, 1, rows), F32),
                pltpu.VMEM((q_heads, 1, rows), F32),
                pltpu.VMEM((q_heads, HEAD, rows), F32),
                pltpu.VMEM((rows, q_heads * HEAD), BF),
                pltpu.VMEM((2, q_heads * HEAD, half), BF),
                pltpu.VMEM((2, 2, seg_rows, q_heads * HEAD), BF),
                pltpu.VMEM((2, CHUNKS, seg_rows, cols), BF),
                pltpu.VMEM((2, CHUNKS, seg_rows, cols), BF),
                dma((7 + LOAD_CHUNKS,)),
                dma((3, kv_heads)),
                dma((4, 2, kv_heads)),
                dma((4, kv_heads)),
                dma((kv_heads, 2)), dma((kv_heads, 2)), dma((3,)),
                dma((2, 2)), dma((2, 2)), dma((2, 2)), dma((2, 2)), dma((2, 2)), dma((2, 2)), dma((2, 2)), dma((2, 2)),
                dma((2, 2, kv_heads)), dma((2, 2, kv_heads)),
                dma((2, CHUNKS)), dma((2, CHUNKS)),
                dma((2, CHUNKS, 2)), dma((2, CHUNKS, 2)),
                dma((CHUNKS, 2)), dma((CHUNKS, 2)),
            ],
            compiler_params=pltpu.CompilerParams(collective_id=0, has_side_effects=True, vmem_limit_bytes=60 * 1024 * 1024),
            name='attn_block',
        )(hidden, positions, norm_gain, jnp.asarray(inverse_freq()), w_query, w_key, w_value, w_out)
        results = [pltpu.with_memory_space_constraint(r, pltpu.VMEM) for r in (out, k_new, v_new)]
        return pl.pallas_call(
            copy_out,
            out_shape=tuple(jax.ShapeDtypeStruct(r.shape, r.dtype) for r in results),
            in_specs=[pl.BlockSpec(memory_space=pltpu.VMEM)] * 3,
            out_specs=[pl.BlockSpec(memory_space=pl.ANY)] * 3,
            scratch_shapes=[dma((3,))],
            compiler_params=pltpu.CompilerParams(vmem_limit_bytes=8 * 1024 * 1024),
            name='copy_out',
        )(*results)

    return jax.shard_map(local_block, mesh=mesh,
                         in_specs=(row_spec, P(('dp', 'cp')), P(None), head_cols, head_cols, head_cols, P('tp', None)),
                         out_specs=(row_spec, cache_spec, cache_spec), check_vma=False)
```

```python
import math
import jax
import jax.numpy as jnp
import numpy as np
from jax import lax
from jax.experimental import pallas as pl
from jax.experimental.pallas import tpu as pltpu
from jax.sharding import PartitionSpec as P

HEAD = 128
EPS = 1e-5
LOG_THETA = math.log(1000000.0)
SCORE_EXP2 = math.log2(math.e) / math.sqrt(HEAD)
BF = jnp.bfloat16
F32 = jnp.float32
CHUNKS = 3
Q_TILE = 256
NORM_ROWS = 32
LOAD_CHUNKS = 4
SHARED_ROWS = 96


def inverse_freq():
    half = np.exp(np.arange(HEAD // 2, dtype=np.float64) * (-2.0 * LOG_THETA / HEAD)).astype(np.float32)
    return np.concatenate([half, half])[None, :]


def block_kernel(ring, kv_heads, group_size,
                 x_hbm, pos_hbm, gain_hbm, freq_hbm, wq_hbm, wk_hbm, wv_hbm, wo_hbm,
                 out_v, k_out, v_out,
                 pos_ref, gain_ref, freq_ref, x_v, h_v, wq_v, wkv_v, wo_v, cos_v, sin_v, kc_v, vc_v, q_v, kv_v, m_v, l_v, acc_v, o_v,
                 wox_v, ox_v, part_v, recv_v,
                 load_sem, kv_send, kv_recv, kv_fwd_send, far_send, far_recv, late_recv,
                 wo_send, wo_recv, wx_send, wx_recv, wf_send, wf_recv, wo_fwd_send, wo_fwd_recv, o_send, o_recv, part_send, part_recv,
                 f1_send, f1_recv, f2_send, f2_recv):
    rows, width = x_v.shape
    cp = lax.axis_index('cp')
    tp = lax.axis_index('tp')
    chip = cp // 2
    core = cp % 2
    seg_rows = rows // ring
    half = width // 2
    cols = half // CHUNKS
    k_half = wo_v.shape[0] // 2

    x_right = {'cp': ((chip + 1) % ring) * 2 + core}
    x_left = {'cp': ((chip + ring - 1) % ring) * 2 + core}
    sibling = {'cp': chip * 2 + 1 - core}
    y_right = {'tp': (tp + 1) % ring}
    y_left = {'tp': (tp + ring - 1) % ring}
    turn = 1 - 2 * (tp % 2)
    y_mate = ({'tp': (tp + ring + turn) % ring}, {'tp': (tp + ring - turn) % ring})

    barrier = pltpu.get_barrier_semaphore()
    for peer in (x_right, x_left, sibling, y_right, y_left):
        pl.semaphore_signal(barrier, inc=1, device_id=peer, device_id_type=pl.DeviceIdType.MESH)

    kv_cols = kv_heads * HEAD
    chunk = rows // LOAD_CHUNKS
    x_loads = [pltpu.make_async_copy(x_hbm.at[i * chunk:(i + 1) * chunk, :], x_v.at[i * chunk:(i + 1) * chunk, :],
                                     load_sem.at[4 + i]) for i in range(LOAD_CHUNKS)]
    loads = [
        pltpu.make_async_copy(wk_hbm, wkv_v.at[0], load_sem.at[0]),
        pltpu.make_async_copy(wv_hbm, wkv_v.at[1], load_sem.at[1]),
        pltpu.make_async_copy(wq_hbm, wq_v, load_sem.at[2]),
        pltpu.make_async_copy(wo_hbm, wo_v, load_sem.at[3]),
    ]
    small = [pltpu.make_async_copy(src, dst, load_sem.at[4 + LOAD_CHUNKS + i])
             for i, (src, dst) in enumerate(((pos_hbm, pos_ref), (freq_hbm, freq_ref), (gain_hbm, gain_ref)))]
    for copy in small + x_loads[:1] + loads[:2] + x_loads[1:]:
        copy.start()

    with jax.named_scope('load_wait'):
        for copy in small:
            copy.wait()
        pos = pos_ref[...].astype(F32).reshape(rows // HEAD, HEAD)
        pos = jnp.concatenate([pos, jnp.zeros((8 - rows // HEAD, HEAD), F32)], axis=0).T
        first = lax.broadcasted_iota(jnp.int32, (1, HEAD), 1) < HEAD // 2
        def tables(i):
            k = i + rows // HEAD // 2
            angles = jnp.where(first, pos[:, i:i + 1], pos[:, k:k + 1]) * freq_ref[...]
            cos_t, sin_t = jnp.cos(angles), jnp.sin(angles)
            cos_r, sin_r = pltpu.roll(cos_t, HEAD // 2, 1), pltpu.roll(sin_t, HEAD // 2, 1)
            for row, lo_c, hi_c, lo_s, hi_s in ((i, cos_t, cos_r, sin_t, sin_r), (k, cos_r, cos_t, sin_r, sin_t)):
                cos_v[row * HEAD:(row + 1) * HEAD, :] = jnp.where(first, lo_c, hi_c)
                sin_v[row * HEAD:(row + 1) * HEAD, :] = jnp.where(first, -lo_s, hi_s)

        for i in range(rows // HEAD // 2):
            tables(i)

    def remote(src, dst, send, recv, peer):
        return pltpu.make_async_remote_copy(src_ref=src, dst_ref=dst, send_sem=send, recv_sem=recv,
                                            device_id=peer, device_id_type=pl.DeviceIdType.MESH)

    with jax.named_scope('barrier'):
        pl.semaphore_wait(barrier, 5)

    base = core * k_half
    direct_rows = k_half - SHARED_ROWS
    sub_cols = half // ring

    def shared_rows(from_core):
        return pl.ds(pl.multiple_of(from_core * k_half + direct_rows, 32), SHARED_ROWS)

    def sub_at(c, index):
        return wox_v.at[c, shared_rows(core), pl.ds(pl.multiple_of(index * sub_cols, sub_cols), sub_cols)]

    def wo_part(c, kind):
        if kind:
            src = wo_hbm.at[shared_rows(core), pl.ds(pl.multiple_of(c * half + chip * sub_cols, sub_cols), sub_cols)]
            dst = sub_at(c, chip)
        else:
            ks = pl.ds(pl.multiple_of(base, 32), direct_rows)
            src, dst = wo_hbm.at[ks, c * half:(c + 1) * half], wox_v.at[c, ks, :]
        return remote(src, dst, wo_send.at[c, kind], wo_recv.at[c, kind], y_mate[c])

    def wx_own(d, c, index):
        return remote(sub_at(c, index), sub_at(c, index), wx_send.at[d, c], wx_recv.at[d, c], x_left if d else x_right)

    def wx_pass(d, c, index):
        return remote(sub_at(c, index), sub_at(c, index), wf_send.at[d, c], wf_recv.at[d, c], x_left if d else x_right)

    def all_bytes(ref, send, recv):
        return remote(ref, ref, send, recv, sibling)

    def wo_share(c, kind, from_core):
        ks = shared_rows(from_core) if kind else pl.ds(pl.multiple_of(from_core * k_half, 32), direct_rows)
        part = wox_v.at[c, ks, :]
        return remote(part, part, wo_fwd_send, wo_fwd_recv, sibling)

    chip_left, chip_right, chip_far = (chip + ring - 1) % ring, (chip + 1) % ring, (chip + 2) % ring

    for c in range(2):
        wo_part(c, 1).start()
    for c in range(2):
        wo_part(c, 0).start()

    def norm_rows(r0, count):
        xf = x_v[pl.ds(r0, count), :].astype(F32)
        inv = lax.rsqrt(jnp.mean(xf * xf, axis=-1, keepdims=True) + EPS)
        h_v[pl.ds(r0, count), :] = (xf * inv * gain_ref[...].astype(F32).reshape(1, width)).astype(BF)

    def norm_step(i, carry):
        norm_rows(pl.multiple_of(i * NORM_ROWS, NORM_ROWS), NORM_ROWS)
        return carry

    def rope(vals, rs=slice(None)):
        return (vals * cos_v[rs, :] + pltpu.roll(vals, HEAD // 2, 1) * sin_v[rs, :]).astype(BF)

    def own_to(rel, cc, head, peer):
        return remote(kv_v.at[0, 0, head], kv_v.at[rel, cc, head],
                      kv_send.at[rel, head], kv_recv.at[rel, cc, head], peer)

    def piece_sem(rel, head, late):
        return late_recv.at[rel] if late else kv_recv.at[rel, 0, head]

    def own_chunk(rel, head, peer, i, count=1, late=False):
        ks = slice(i * chunk, (i + count) * chunk)
        return remote(kv_v.at[0, 0, head, :, ks, :], kv_v.at[rel, 0, head, :, ks, :],
                      kv_send.at[rel, head], piece_sem(rel, head, late), peer)

    def left_v(head, ks=slice(None), late=False):
        return remote(kv_v.at[0, 0, head, 1, ks, :], kv_v.at[2, 0, head, 1, ks, :],
                      kv_send.at[2, head], piece_sem(2, head, late), x_left)

    half_chunks = LOAD_CHUNKS // 2
    key_halves = (slice(0, half_chunks * chunk), slice(half_chunks * chunk, rows))

    def far_k(head, ks=slice(None)):
        return remote(kv_v.at[1, 0, head, 0, ks, :], kv_v.at[3, 0, head, 0, ks, :], far_send.at[head, 0], far_recv.at[head, 0], x_right)

    def far_v(head, ks=slice(None)):
        return remote(kv_v.at[2, 0, head, 1, ks, :], kv_v.at[3, 0, head, 1, ks, :], far_send.at[head, 1], far_recv.at[head, 1], x_left)

    def fwd_sib(rel, head):
        return remote(kv_v.at[rel, 0, head], kv_v.at[rel, 1, head],
                      kv_fwd_send.at[rel, head], kv_recv.at[rel, 1, head], sibling)

    right_sends = chip < ring - 1

    x_loads[0].wait()
    with jax.named_scope('norm'):
        lax.fori_loop(0, chunk // NORM_ROWS, norm_step, 0)
    loads[2].start()
    for copy in loads[:2]:
        copy.wait()
    steps = ((0, 1), (1, 1), (2, LOAD_CHUNKS - 2))
    for n, (i, count) in enumerate(steps):
        ahead = steps[n + 1] if n + 1 < len(steps) else (0, 0)
        for k in range(ahead[0], sum(ahead)):
            x_loads[k].wait()
        ks = slice(i * chunk, (i + count) * chunk)
        with jax.named_scope('kv_proj'):
            k_proj, v_proj = (jnp.dot(h_v[ks, :], wkv_v[w], preferred_element_type=F32) for w in range(2))
            for r in range(ahead[0] * chunk, sum(ahead) * chunk, 16):
                norm_rows(r, 16)
            for h in range(kv_heads):
                hc = slice(h * HEAD, (h + 1) * HEAD)
                k_head = rope(k_proj[:, hc], ks)
                kv_v[0, 0, h, 0, ks, :] = k_head
                kc_v[ks, hc] = k_head
                v_head = v_proj[:, hc].astype(BF)
                vc_v[ks, hc] = v_head
                for k in range(count):
                    kv_v[0, 0, h, 1, (i + k) * chunk:(i + k + 1) * chunk, :] = v_head[k * chunk:(k + 1) * chunk, :].T

        @pl.when(right_sends)
        def _(i=i, count=count):
            own_chunk(1, 0, x_right, i, count).start()

        @pl.when(chip == 0)
        def _(i=i, count=count):
            own_chunk(2, 0, x_left, i, count).start()

        @pl.when(chip == 1)
        def _(ks=ks):
            left_v(0, ks).start()

    loads[3].start()

    @pl.when(core == 0)
    def _():
        own_to(0, 1, 0, sibling).start()
        own_to(0, 1, 1, sibling).start()

    def head_one(i):
        @pl.when(right_sends)
        def _():
            own_chunk(1, 1, x_right, i * half_chunks, half_chunks, i == 1).start()

        @pl.when(chip == 0)
        def _():
            own_chunk(2, 1, x_left, i * half_chunks, half_chunks, i == 1).start()

        @pl.when(chip == 1)
        def _():
            left_v(1, key_halves[i], i == 1).start()

    head_one(0)
    loads[2].wait()

    with jax.named_scope('q_proj'):
        q_pair = None
        for j in range(kv_heads * group_size // 2 + 1):
            last = q_pair
            if j < kv_heads * group_size // 2:
                q_pair = jnp.dot(h_v[...], wq_v[:, j * 2 * HEAD:(j + 1) * 2 * HEAD], preferred_element_type=F32)
            if j > 0:
                q_v[2 * j - 2] = rope(last[:, :HEAD]).T
                q_v[2 * j - 1] = rope(last[:, HEAD:]).T

    def attend(tiles, first):
        def start(tile):
            rel, ccs, head, qi, rs, r0 = tile
            keys = r0 + Q_TILE if first else rows
            q_t = q_v[qi, :, rs]
            s = jnp.concatenate([jnp.dot(kv_v[rel, cc, head, 0, :keys, :], q_t, preferred_element_type=F32) for cc in ccs], axis=0)
            if first:
                key_id = lax.broadcasted_iota(jnp.int32, s.shape, 0)
                row_id = lax.broadcasted_iota(jnp.int32, s.shape, 1) + r0
                s = jnp.where(key_id <= row_id, s, -jnp.inf)
            return s

        def soften(tile, s):
            rel, ccs, head, qi, rs, r0 = tile
            m_new = jnp.max(s, axis=0, keepdims=True)
            alpha = None
            if not first:
                m_old = m_v[qi, :, rs]
                m_new = jnp.maximum(m_old, m_new)
                alpha = jnp.exp2((m_old - m_new) * SCORE_EXP2)
            p = jnp.exp2((s - m_new) * SCORE_EXP2)
            l_new = jnp.sum(p, axis=0, keepdims=True)
            l_v[qi, :, rs] = l_new if first else l_v[qi, :, rs] * alpha + l_new
            m_v[qi, :, rs] = m_new
            return p.astype(BF), alpha

        def gather(tile, p, alpha):
            rel, ccs, head, qi, rs, r0 = tile
            keys = r0 + Q_TILE if first else rows
            v_t = jnp.concatenate([kv_v[rel, cc, head, 1, j * HEAD:(j + 1) * HEAD, :] for cc in ccs for j in range(keys // HEAD)], axis=1)
            o_new = jnp.dot(v_t, p, preferred_element_type=F32)
            acc_v[qi, :, rs] = o_new if first else acc_v[qi, :, rs] * alpha + o_new

        s = start(tiles[0])
        held = None
        for i in range(len(tiles) + 1):
            s_next = start(tiles[i + 1]) if i + 1 < len(tiles) else None
            if held is not None:
                gather(tiles[i - 1], *held)
            if i < len(tiles):
                held = soften(tiles[i], s)
            s = s_next

    def head_tiles(rel, ccs, head):
        return [(rel, ccs, head, head * group_size + g, slice(rt * Q_TILE, (rt + 1) * Q_TILE), rt * Q_TILE)
                for g in range(group_size) for rt in range(rows // Q_TILE)]

    def own_unit(head, carry):
        attend(head_tiles(0, (0,), head), True)
        return carry

    with jax.named_scope('own'):
        lax.fori_loop(0, kv_heads, own_unit, 0)

    def far_unit(rel, ccs, head):
        with jax.named_scope('far'):
            attend(head_tiles(rel, ccs, head), False)

    has_left = chip >= 1
    has_right = chip >= 3
    has_far = chip >= 2
    fwd_right = jnp.logical_and(chip >= 1, chip <= 2)

    def take_head_zero():
        @pl.when(has_left)
        def _():
            own_to(1, 0, 0, x_right).wait_recv()

            @pl.when(fwd_right)
            def _():
                far_k(0).start()

            fwd_sib(1, 0).start()

        @pl.when(has_right)
        def _():
            own_to(2, 0, 0, x_left).wait_recv()
            far_v(0).start()
            fwd_sib(2, 0).start()

        @pl.when(chip == 0)
        def _():
            left_v(0).wait_recv()
            far_v(0).start()

    def take_head_one(i):
        @pl.when(has_left)
        def _():
            own_chunk(1, 1, x_right, i * half_chunks, half_chunks, i == 1).wait_recv()

            @pl.when(fwd_right)
            def _():
                far_k(1, key_halves[i]).start()

            if i == 1:
                fwd_sib(1, 1).start()

        @pl.when(has_right)
        def _():
            own_chunk(2, 1, x_left, i * half_chunks, half_chunks, i == 1).wait_recv()
            far_v(1, key_halves[i]).start()
            if i == 1:
                fwd_sib(2, 1).start()

        @pl.when(chip == 0)
        def _():
            left_v(1, key_halves[i], i == 1).wait_recv()
            far_v(1, key_halves[i]).start()

    @pl.when(core == 1)
    def _():
        own_to(0, 1, 0, sibling).wait_recv()
        own_to(0, 1, 1, sibling).wait_recv()

    take_head_zero()
    head_one(1)

    ends = jnp.logical_or(chip == 0, chip == 3)

    def wx_late(c):
        @pl.when(fwd_right)
        def _():
            wx_own(0, c, chip).start()

        @pl.when(ends)
        def _():
            wx_own(1, c, chip).start()

    for c in range(2):
        wo_part(c, 1).wait_recv()

        @pl.when(ends)
        def _(c=c):
            wx_own(0, c, chip).start()

        @pl.when(fwd_right)
        def _(c=c):
            wx_own(1, c, chip).start()

    def sibling_unit(head, carry):
        far_unit(0, (1,), head)
        return carry

    @pl.when(core == 1)
    def _():
        lax.fori_loop(0, kv_heads, sibling_unit, 0)

    def seg(index):
        return pl.ds(pl.multiple_of(index * seg_rows, seg_rows), seg_rows)

    own_seg, far_seg = tp, (tp + 2) % ring
    mate_seg = ((tp + ring + turn) % ring, (tp + ring - turn) % ring)

    head_cols = group_size * HEAD

    def o_part(c, which, head):
        hc = slice(head * head_cols, (head + 1) * head_cols)
        return remote(o_v.at[seg(mate_seg[c] if which else far_seg), hc], ox_v.at[c, which, :, hc],
                      o_send, o_recv.at[which], y_mate[c])

    def finish_rows(head, rs):
        for qi in range(head * group_size, (head + 1) * group_size):
            o_v[rs, qi * HEAD:(qi + 1) * HEAD] = (acc_v[qi, :, rs] * (1.0 / l_v[qi, :, rs])).astype(BF).T

    loads[3].wait()

    def sib_wait(rel, head):
        remote(kv_v.at[rel, 0, head], kv_v.at[rel, 1, head], kv_fwd_send.at[rel, head], kv_recv.at[rel, 1, head], sibling).wait_recv()

    shift = (chip // (ring - 1)) * (1 - core)

    def side_unit(u, carry):
        head = u // 3
        rel = 1 + u % 3
        need = ((rel == 1) & has_left) | ((rel == 2) & has_right) | ((rel == 3) & has_far)

        @pl.when((u == 0) & has_left)
        def _():
            sib_wait(1, 0)

        at = u - shift

        @pl.when((at == 1) & has_far)
        def _():
            with jax.named_scope('far_h0'):
                far_k(0).wait_recv()
                far_v(0).wait_recv()
                fwd_sib(3, 0).start()

        @pl.when((u == 1) & has_right)
        def _():
            sib_wait(2, 0)

        @pl.when(u == 1)
        def _():
            take_head_one(0)

        @pl.when(at == 2)
        def _():
            with jax.named_scope('take_h1'):
                take_head_one(1)
                for c in range(2):
                    wx_late(c)

        @pl.when((u == 2) & has_far)
        def _():
            sib_wait(3, 0)

        @pl.when(u == 3)
        def _():
            finish_rows(0, slice(0, rows))
            for c in range(2):
                o_part(c, 0, 0).start()
            for c in range(2):
                o_part(c, 1, 0).start()

        @pl.when((u == 3) & (chip < 2))
        def _():
            with jax.named_scope('wx_wait'):
                for c in range(2):
                    for d in range(2):
                        wx_own(d, c, chip_right if d else chip_left).wait_recv()
                        wx_pass(d, c, chip_right if d else chip_left).start()

        @pl.when((u == 3) & has_left)
        def _():
            sib_wait(1, 1)

        @pl.when(need)
        def _():
            far_unit(rel, (0, 1), head)

        return carry

    lax.fori_loop(0, 4, side_unit, 0)

    @pl.when(has_far)
    def _():
        with jax.named_scope('far_h1'):
            far_k(1).wait_recv()
            far_v(1).wait_recv()
            fwd_sib(3, 1).start()

    @pl.when(has_right)
    def _():
        sib_wait(2, 1)

    def col(c, g):
        return pl.ds(pl.multiple_of(c * half + g * cols, cols), cols)

    def two_mates(c, g, own_rows, which):
        g0 = pl.multiple_of(g * cols, cols)
        return (jnp.dot(o_v[seg(own_rows), :], wo_v[:, col(c, g)], preferred_element_type=F32)
                + jnp.dot(ox_v[c, which], wox_v[c, :, pl.ds(g0, cols)], preferred_element_type=F32))

    def cross(c, g):
        return remote(part_v.at[c, g], recv_v.at[c, g], part_send, part_recv.at[c, g], y_mate[1 - c])

    def f1(c, g, d, owner):
        block = out_v.at[seg(owner), col(c, g)]
        return remote(block, block, f1_send, f1_recv.at[c, g, d], y_left if d else y_right)

    def f2(g, d, owner):
        block = out_v.at[seg(owner), col(d, g)]
        return remote(block, block, f2_send, f2_recv, y_left if d else y_right)

    def project_cross(g, carry):
        for c in range(2):
            part_v[c, g] = two_mates(c, g, mate_seg[1 - c], 0).astype(BF)
            cross(c, g).start()
        return carry

    def seg_step(j, carry):
        index = (tp + ring + 2 * ((3 - j) // 3) + turn * ((j % 3) % 2) - turn * (j // 2 - j // 3)) % ring
        rs = seg(index)

        @pl.when(j == 3)
        def _():
            with jax.named_scope('mates'):
                all_bytes(wox_v.at[:, :k_half, :], wo_fwd_send, wo_fwd_recv).wait_recv()
                all_bytes(ox_v.at[:, 0], o_send, o_recv.at[0]).wait_recv()

            with jax.named_scope('cross'):
                lax.fori_loop(0, CHUNKS, project_cross, 0)

        def seg_tiles(*rels):
            return [(rel, (0, 1), 1, group_size + g, rs, 0) for rel in rels for g in range(group_size)]

        @pl.when(has_right)
        def _():
            with jax.named_scope('right_seg'):
                attend(seg_tiles(2), False)

        @pl.when((j == 0) & has_far)
        def _():
            sib_wait(3, 1)

        @pl.when(has_far)
        def _():
            with jax.named_scope('far_seg'):
                attend(seg_tiles(3), False)

        finish_rows(1, rs)

        @pl.when(j == 0)
        def _():
            for c in range(2):
                o_part(c, 0, 1).start()
            with jax.named_scope('wo_wait'):
                for c in range(2):
                    wo_part(c, 0).wait_recv()
                    wo_share(c, 0, core).start()

        @pl.when(j == 1)
        def _():
            o_part(0, 1, 1).start()
            with jax.named_scope('sub_wait'):
                @pl.when(has_far)
                def _():
                    for d in range(2):
                        for c in range(2):
                            wx_own(d, c, chip_right if d else chip_left).wait_recv()

                for d, gets in ((0, fwd_right), (1, ends)):
                    @pl.when(gets)
                    def _(d=d):
                        for c in range(2):
                            wx_pass(d, c, chip_far).wait_recv()

                for c in range(2):
                    wo_share(c, 1, core).start()

        @pl.when(j == 2)
        def _():
            o_part(1, 1, 1).start()

        return carry

    with jax.named_scope('segs'):
        lax.fori_loop(0, ring, seg_step, 0)

    with jax.named_scope('caches'):
        k_out[...] = kc_v[...].reshape(k_out.shape)
        v_out[...] = vc_v[...].reshape(v_out.shape)

    all_bytes(ox_v.at[:, 1], o_send, o_recv.at[1]).wait_recv()

    def project_own(g, carry):
        for c in range(2):
            attn = two_mates(c, g, own_seg, 1)
            cross(c, g).wait_recv()
            attn = attn + recv_v[c, g].astype(F32)
            out_v[seg(own_seg), col(c, g)] = (x_v[seg(own_seg), col(c, g)].astype(F32) + attn).astype(BF)
            for d in range(2):
                f1(c, g, d, own_seg).start()
        return carry

    with jax.named_scope('own_out'):
        lax.fori_loop(0, CHUNKS, project_own, 0)

    side_seg = ((tp + ring - 1) % ring, (tp + 1) % ring)

    def pass_on(g, carry):
        for d in range(2):
            f1(d, g, d, side_seg[d]).wait_recv()
            f2(g, d, side_seg[d]).start()
        return carry

    with jax.named_scope('pass_on'):
        lax.fori_loop(0, CHUNKS, pass_on, 0)

    def finish(g, carry):
        for d in range(2):
            f1(1 - d, g, d, side_seg[d]).wait_recv()
        return carry

    with jax.named_scope('finish'):
        lax.fori_loop(0, CHUNKS, finish, 0)

    with jax.named_scope('drain'):
        own_rows = out_v.at[:seg_rows, :]
        all_bytes(own_rows, f2_send, f2_recv).wait_recv()
        all_bytes(own_rows, f2_send, f2_recv).wait_send()
        all_bytes(out_v.at[:2 * seg_rows, :], f1_send, f2_recv).wait_send()
        all_bytes(part_v, part_send, f2_recv).wait_send()
        all_bytes(ox_v, o_send, f2_recv).wait_send()
        all_bytes(wox_v.at[:, :k_half, :], wo_fwd_send, f2_recv).wait_send()
    for c in range(2):
        @pl.when(chip < 2)
        def _(c=c):
            for d in range(2):
                wx_pass(d, c, chip_right if d else chip_left).wait_send()

        for i in range(2):
            wo_part(c, i).wait_send()
            wx_own(i, c, chip).wait_send()

    @pl.when(core == 0)
    def _():
        own_to(0, 1, 0, sibling).wait_send()
        own_to(0, 1, 1, sibling).wait_send()

    for head in range(kv_heads):
        @pl.when(right_sends)
        def _(head=head):
            own_to(1, 0, head, x_right).wait_send()

        @pl.when(chip == 0)
        def _(head=head):
            own_to(2, 0, head, x_left).wait_send()

        @pl.when(chip == 1)
        def _(head=head):
            left_v(head).wait_send()

        @pl.when(fwd_right)
        def _(head=head):
            far_k(head).wait_send()

        @pl.when(jnp.logical_or(chip == 0, has_right))
        def _(head=head):
            far_v(head).wait_send()

        for rel, sent in ((1, has_left), (2, has_right), (3, has_far)):
            @pl.when(sent)
            def _(rel=rel, head=head):
                fwd_sib(rel, head).wait_send()


def copy_out(*refs):
    count = len(refs) // 2
    sems = refs[-1]
    copies = [pltpu.make_async_copy(refs[i], refs[count + i], sems.at[i]) for i in range(count)]
    for copy in copies:
        copy.start()
    for copy in copies:
        copy.wait()


def solution(mesh):
    ring = mesh.shape['tp']
    if mesh.shape['cp'] != 2 * ring or ring != 4:
        raise ValueError('mesh')
    row_spec = P(('dp', 'cp'), None)
    cache_spec = P(('dp', 'cp'), 'tp', None)
    head_cols = P(None, 'tp')

    def local_block(hidden, positions, norm_gain, w_query, w_key, w_value, w_out):
        rows, width = hidden.shape
        kv_heads = w_key.shape[1] // HEAD
        q_heads = w_query.shape[1] // HEAD
        seg_rows, half = rows // ring, width // 2
        cols = half // CHUNKS
        dma = pltpu.SemaphoreType.DMA
        out, k_new, v_new = pl.pallas_call(
            lambda *refs: block_kernel(ring, kv_heads, q_heads // kv_heads, *refs),
            out_shape=(
                pltpu.VMEM((rows, width), BF),
                pltpu.VMEM((rows, kv_heads, HEAD), BF),
                pltpu.VMEM((rows, kv_heads, HEAD), BF),
            ),
            in_specs=[pl.BlockSpec(memory_space=pl.ANY)] * 8,
            out_specs=[pl.BlockSpec(memory_space=pltpu.VMEM)] * 3,
            scratch_shapes=[
                pltpu.VMEM((rows,), jnp.int32),
                pltpu.VMEM((width,), BF),
                pltpu.VMEM((1, HEAD), F32),
                pltpu.VMEM((rows, width), BF),
                pltpu.VMEM((rows, width), BF),
                pltpu.VMEM(w_query.shape, BF),
                pltpu.VMEM((2, width, kv_heads * HEAD), BF),
                pltpu.VMEM(w_out.shape, BF),
                pltpu.VMEM((rows, HEAD), F32),
                pltpu.VMEM((rows, HEAD), F32),
                pltpu.VMEM((rows, kv_heads * HEAD), BF),
                pltpu.VMEM((rows, kv_heads * HEAD), BF),
                pltpu.VMEM((q_heads, HEAD, rows), BF),
                pltpu.VMEM((4, 2, kv_heads, 2, rows, HEAD), BF),
                pltpu.VMEM((q_heads, 1, rows), F32),
                pltpu.VMEM((q_heads, 1, rows), F32),
                pltpu.VMEM((q_heads, HEAD, rows), F32),
                pltpu.VMEM((rows, q_heads * HEAD), BF),
                pltpu.VMEM((2, q_heads * HEAD, half), BF),
                pltpu.VMEM((2, 2, seg_rows, q_heads * HEAD), BF),
                pltpu.VMEM((2, CHUNKS, seg_rows, cols), BF),
                pltpu.VMEM((2, CHUNKS, seg_rows, cols), BF),
                dma((7 + LOAD_CHUNKS,)),
                dma((3, kv_heads)),
                dma((4, 2, kv_heads)),
                dma((4, kv_heads)),
                dma((kv_heads, 2)), dma((kv_heads, 2)), dma((3,)),
                dma((2, 2)), dma((2, 2)), dma((2, 2)), dma((2, 2)), dma((2, 2)), dma((2, 2)), dma(()), dma(()),
                dma(()), dma((2,)),
                dma(()), dma((2, CHUNKS)),
                dma(()), dma((2, CHUNKS, 2)),
                dma(()), dma(()),
            ],
            compiler_params=pltpu.CompilerParams(collective_id=0, has_side_effects=True, vmem_limit_bytes=60 * 1024 * 1024),
            name='attn_block',
        )(hidden, positions, norm_gain, jnp.asarray(inverse_freq()), w_query, w_key, w_value, w_out)
        results = [pltpu.with_memory_space_constraint(r, pltpu.VMEM) for r in (out, k_new, v_new)]
        return pl.pallas_call(
            copy_out,
            out_shape=tuple(jax.ShapeDtypeStruct(r.shape, r.dtype) for r in results),
            in_specs=[pl.BlockSpec(memory_space=pltpu.VMEM)] * 3,
            out_specs=[pl.BlockSpec(memory_space=pl.ANY)] * 3,
            scratch_shapes=[dma((3,))],
            compiler_params=pltpu.CompilerParams(vmem_limit_bytes=8 * 1024 * 1024),
            name='copy_out',
        )(*results)

    return jax.shard_map(local_block, mesh=mesh,
                         in_specs=(row_spec, P(('dp', 'cp')), P(None), head_cols, head_cols, head_cols, P('tp', None)),
                         out_specs=(row_spec, cache_spec, cache_spec), check_vma=False)
```

```python
import math
import jax
import jax.numpy as jnp
import numpy as np
from jax import lax
from jax.experimental import pallas as pl
from jax.experimental.pallas import tpu as pltpu
from jax.sharding import PartitionSpec as P

HEAD = 128
EPS = 1e-5
LOG_THETA = math.log(1000000.0)
SCORE_EXP2 = math.log2(math.e) / math.sqrt(HEAD)
BF = jnp.bfloat16
F32 = jnp.float32
CHUNKS = 3
Q_TILE = 256
NORM_ROWS = 32
LOAD_CHUNKS = 4
SHARED_ROWS = 96


def inverse_freq():
    half = np.exp(np.arange(HEAD // 2, dtype=np.float64) * (-2.0 * LOG_THETA / HEAD)).astype(np.float32)
    return np.concatenate([half, half])[None, :]


def block_kernel(ring, kv_heads, group_size,
                 x_hbm, pos_hbm, gain_hbm, freq_hbm, wq_hbm, wk_hbm, wv_hbm, wo_hbm,
                 out_v, k_out, v_out,
                 pos_ref, gain_ref, freq_ref, x_v, h_v, wq_v, wkv_v, wo_v, cos_v, sin_v, kc_v, vc_v, q_v, kv_v, m_v, l_v, acc_v, o_v,
                 wox_v, ox_v, part_v, recv_v,
                 load_sem, kv_send, kv_recv, kv_fwd_send, far_send, far_recv, late_recv,
                 wo_send, wo_recv, wx_send, wx_recv, wf_send, wf_recv, wo_fwd_send, wo_fwd_recv, o_send, o_recv, part_send, part_recv,
                 f1_send, f1_recv, f1_late, f2_send, f2_recv):
    rows, width = x_v.shape
    cp = lax.axis_index('cp')
    tp = lax.axis_index('tp')
    chip = cp // 2
    core = cp % 2
    seg_rows = rows // ring
    half = width // 2
    cols = half // CHUNKS
    k_half = wo_v.shape[0] // 2

    x_right = {'cp': ((chip + 1) % ring) * 2 + core}
    x_left = {'cp': ((chip + ring - 1) % ring) * 2 + core}
    sibling = {'cp': chip * 2 + 1 - core}
    y_right = {'tp': (tp + 1) % ring}
    y_left = {'tp': (tp + ring - 1) % ring}
    turn = 1 - 2 * (tp % 2)
    y_mate = ({'tp': (tp + ring + turn) % ring}, {'tp': (tp + ring - turn) % ring})

    barrier = pltpu.get_barrier_semaphore()
    for peer in (x_right, x_left, sibling, y_right, y_left):
        pl.semaphore_signal(barrier, inc=1, device_id=peer, device_id_type=pl.DeviceIdType.MESH)

    kv_cols = kv_heads * HEAD
    chunk = rows // LOAD_CHUNKS
    x_loads = [pltpu.make_async_copy(x_hbm.at[i * chunk:(i + 1) * chunk, :], x_v.at[i * chunk:(i + 1) * chunk, :],
                                     load_sem.at[4 + i]) for i in range(LOAD_CHUNKS)]
    loads = [
        pltpu.make_async_copy(wk_hbm, wkv_v.at[0], load_sem.at[0]),
        pltpu.make_async_copy(wv_hbm, wkv_v.at[1], load_sem.at[1]),
        pltpu.make_async_copy(wq_hbm, wq_v, load_sem.at[2]),
        pltpu.make_async_copy(wo_hbm, wo_v, load_sem.at[3]),
    ]
    small = [pltpu.make_async_copy(src, dst, load_sem.at[4 + LOAD_CHUNKS + i])
             for i, (src, dst) in enumerate(((pos_hbm, pos_ref), (freq_hbm, freq_ref), (gain_hbm, gain_ref)))]
    for copy in small + x_loads[:1] + loads[:2] + x_loads[1:]:
        copy.start()

    with jax.named_scope('load_wait'):
        for copy in small:
            copy.wait()
        pos = pos_ref[...].astype(F32).reshape(rows // HEAD, HEAD)
        pos = jnp.concatenate([pos, jnp.zeros((8 - rows // HEAD, HEAD), F32)], axis=0).T
        first = lax.broadcasted_iota(jnp.int32, (1, HEAD), 1) < HEAD // 2
        def tables(i):
            k = i + rows // HEAD // 2
            angles = jnp.where(first, pos[:, i:i + 1], pos[:, k:k + 1]) * freq_ref[...]
            cos_t, sin_t = jnp.cos(angles), jnp.sin(angles)
            cos_r, sin_r = pltpu.roll(cos_t, HEAD // 2, 1), pltpu.roll(sin_t, HEAD // 2, 1)
            for row, lo_c, hi_c, lo_s, hi_s in ((i, cos_t, cos_r, sin_t, sin_r), (k, cos_r, cos_t, sin_r, sin_t)):
                cos_v[row * HEAD:(row + 1) * HEAD, :] = jnp.where(first, lo_c, hi_c)
                sin_v[row * HEAD:(row + 1) * HEAD, :] = jnp.where(first, -lo_s, hi_s)

        for i in range(rows // HEAD // 2):
            tables(i)

    def remote(src, dst, send, recv, peer):
        return pltpu.make_async_remote_copy(src_ref=src, dst_ref=dst, send_sem=send, recv_sem=recv,
                                            device_id=peer, device_id_type=pl.DeviceIdType.MESH)

    with jax.named_scope('barrier'):
        pl.semaphore_wait(barrier, 5)

    base = core * k_half
    direct_rows = k_half - SHARED_ROWS
    sub_cols = half // ring

    def shared_rows(from_core):
        return pl.ds(pl.multiple_of(from_core * k_half + direct_rows, 32), SHARED_ROWS)

    def sub_at(c, index):
        return wox_v.at[c, shared_rows(core), pl.ds(pl.multiple_of(index * sub_cols, sub_cols), sub_cols)]

    def wo_part(c, kind):
        if kind:
            src = wo_hbm.at[shared_rows(core), pl.ds(pl.multiple_of(c * half + chip * sub_cols, sub_cols), sub_cols)]
            dst = sub_at(c, chip)
        else:
            ks = pl.ds(pl.multiple_of(base, 32), direct_rows)
            src, dst = wo_hbm.at[ks, c * half:(c + 1) * half], wox_v.at[c, ks, :]
        return remote(src, dst, wo_send, wo_recv.at[c, kind], y_mate[c])

    def wx_own(d, c, index):
        return remote(sub_at(c, index), sub_at(c, index), wx_send, wx_recv.at[d, c], x_left if d else x_right)

    def wx_pass(d, c, index):
        return remote(sub_at(c, index), sub_at(c, index), wf_send, wf_recv.at[d, c], x_left if d else x_right)

    def all_bytes(ref, send, recv):
        return remote(ref, ref, send, recv, sibling)

    def wo_share(c, kind, from_core):
        ks = shared_rows(from_core) if kind else pl.ds(pl.multiple_of(from_core * k_half, 32), direct_rows)
        part = wox_v.at[c, ks, :]
        return remote(part, part, wo_fwd_send, wo_fwd_recv, sibling)

    chip_left, chip_right, chip_far = (chip + ring - 1) % ring, (chip + 1) % ring, (chip + 2) % ring

    for c in range(2):
        wo_part(c, 1).start()
    for c in range(2):
        wo_part(c, 0).start()

    def norm_rows(r0, count):
        xf = x_v[pl.ds(r0, count), :].astype(F32)
        inv = lax.rsqrt(jnp.mean(xf * xf, axis=-1, keepdims=True) + EPS)
        h_v[pl.ds(r0, count), :] = (xf * inv * gain_ref[...].astype(F32).reshape(1, width)).astype(BF)

    def norm_step(i, carry):
        norm_rows(pl.multiple_of(i * NORM_ROWS, NORM_ROWS), NORM_ROWS)
        return carry

    def rope(vals, rs=slice(None)):
        return (vals * cos_v[rs, :] + pltpu.roll(vals, HEAD // 2, 1) * sin_v[rs, :]).astype(BF)

    def own_to(rel, cc, head, peer):
        return remote(kv_v.at[0, 0, head], kv_v.at[rel, cc, head],
                      kv_send.at[rel, head], kv_recv.at[rel, cc, head], peer)

    def piece_sem(rel, head, late):
        return late_recv.at[rel] if late else kv_recv.at[rel, 0, head]

    def own_chunk(rel, head, peer, i, count=1, late=False):
        ks = slice(i * chunk, (i + count) * chunk)
        return remote(kv_v.at[0, 0, head, :, ks, :], kv_v.at[rel, 0, head, :, ks, :],
                      kv_send.at[rel, head], piece_sem(rel, head, late), peer)

    def left_v(head, ks=slice(None), late=False):
        return remote(kv_v.at[0, 0, head, 1, ks, :], kv_v.at[2, 0, head, 1, ks, :],
                      kv_send.at[2, head], piece_sem(2, head, late), x_left)

    half_chunks = LOAD_CHUNKS // 2
    key_halves = (slice(0, half_chunks * chunk), slice(half_chunks * chunk, rows))

    def far_k(head, ks=slice(None)):
        return remote(kv_v.at[1, 0, head, 0, ks, :], kv_v.at[3, 0, head, 0, ks, :], far_send.at[head, 0], far_recv.at[head, 0], x_right)

    def far_v(head, ks=slice(None)):
        return remote(kv_v.at[2, 0, head, 1, ks, :], kv_v.at[3, 0, head, 1, ks, :], far_send.at[head, 1], far_recv.at[head, 1], x_left)

    def fwd_sib(rel, head):
        return remote(kv_v.at[rel, 0, head], kv_v.at[rel, 1, head],
                      kv_fwd_send.at[rel, head], kv_recv.at[rel, 1, head], sibling)

    right_sends = chip < ring - 1

    x_loads[0].wait()
    with jax.named_scope('norm'):
        lax.fori_loop(0, chunk // NORM_ROWS, norm_step, 0)
    loads[2].start()
    for copy in loads[:2]:
        copy.wait()
    steps = ((0, 1), (1, 1), (2, LOAD_CHUNKS - 2))
    for n, (i, count) in enumerate(steps):
        ahead = steps[n + 1] if n + 1 < len(steps) else (0, 0)
        for k in range(ahead[0], sum(ahead)):
            x_loads[k].wait()
        ks = slice(i * chunk, (i + count) * chunk)
        with jax.named_scope('kv_proj'):
            k_proj, v_proj = (jnp.dot(h_v[ks, :], wkv_v[w], preferred_element_type=F32) for w in range(2))
            for r in range(ahead[0] * chunk, sum(ahead) * chunk, 16):
                norm_rows(r, 16)
            for h in range(kv_heads):
                hc = slice(h * HEAD, (h + 1) * HEAD)
                k_head = rope(k_proj[:, hc], ks)
                kv_v[0, 0, h, 0, ks, :] = k_head
                kc_v[ks, hc] = k_head
                v_head = v_proj[:, hc].astype(BF)
                vc_v[ks, hc] = v_head
                for k in range(count):
                    kv_v[0, 0, h, 1, (i + k) * chunk:(i + k + 1) * chunk, :] = v_head[k * chunk:(k + 1) * chunk, :].T

        @pl.when(right_sends)
        def _(i=i, count=count):
            own_chunk(1, 0, x_right, i, count).start()

        @pl.when(chip == 0)
        def _(i=i, count=count):
            own_chunk(2, 0, x_left, i, count).start()

        @pl.when(chip == 1)
        def _(ks=ks):
            left_v(0, ks).start()

    loads[3].start()

    @pl.when(core == 0)
    def _():
        own_to(0, 1, 0, sibling).start()
        own_to(0, 1, 1, sibling).start()

    def head_one(i):
        @pl.when(right_sends)
        def _():
            own_chunk(1, 1, x_right, i * half_chunks, half_chunks, i == 1).start()

        @pl.when(chip == 0)
        def _():
            own_chunk(2, 1, x_left, i * half_chunks, half_chunks, i == 1).start()

        @pl.when(chip == 1)
        def _():
            left_v(1, key_halves[i], i == 1).start()

    head_one(0)
    loads[2].wait()

    with jax.named_scope('q_proj'):
        q_pair = None
        for j in range(kv_heads * group_size // 2 + 1):
            last = q_pair
            if j < kv_heads * group_size // 2:
                q_pair = jnp.dot(h_v[...], wq_v[:, j * 2 * HEAD:(j + 1) * 2 * HEAD], preferred_element_type=F32)
            if j > 0:
                q_v[2 * j - 2] = rope(last[:, :HEAD]).T
                q_v[2 * j - 1] = rope(last[:, HEAD:]).T

    def attend(tiles, first):
        def start(tile):
            rel, ccs, head, qi, rs, r0 = tile
            keys = r0 + Q_TILE if first else rows
            q_t = q_v[qi, :, rs]
            s = jnp.concatenate([jnp.dot(kv_v[rel, cc, head, 0, :keys, :], q_t, preferred_element_type=F32) for cc in ccs], axis=0)
            if first:
                key_id = lax.broadcasted_iota(jnp.int32, s.shape, 0)
                row_id = lax.broadcasted_iota(jnp.int32, s.shape, 1) + r0
                s = jnp.where(key_id <= row_id, s, -jnp.inf)
            return s

        def soften(tile, s):
            rel, ccs, head, qi, rs, r0 = tile
            m_new = jnp.max(s, axis=0, keepdims=True)
            alpha = None
            if not first:
                m_old = m_v[qi, :, rs]
                m_new = jnp.maximum(m_old, m_new)
                alpha = jnp.exp2((m_old - m_new) * SCORE_EXP2)
            p = jnp.exp2((s - m_new) * SCORE_EXP2)
            l_new = jnp.sum(p, axis=0, keepdims=True)
            l_v[qi, :, rs] = l_new if first else l_v[qi, :, rs] * alpha + l_new
            m_v[qi, :, rs] = m_new
            return p.astype(BF), alpha

        def gather(tile, p, alpha):
            rel, ccs, head, qi, rs, r0 = tile
            keys = r0 + Q_TILE if first else rows
            v_t = jnp.concatenate([kv_v[rel, cc, head, 1, j * HEAD:(j + 1) * HEAD, :] for cc in ccs for j in range(keys // HEAD)], axis=1)
            o_new = jnp.dot(v_t, p, preferred_element_type=F32)
            acc_v[qi, :, rs] = o_new if first else acc_v[qi, :, rs] * alpha + o_new

        s = start(tiles[0])
        held = None
        for i in range(len(tiles) + 1):
            s_next = start(tiles[i + 1]) if i + 1 < len(tiles) else None
            if held is not None:
                gather(tiles[i - 1], *held)
            if i < len(tiles):
                held = soften(tiles[i], s)
            s = s_next

    def head_tiles(rel, ccs, head):
        return [(rel, ccs, head, head * group_size + g, slice(rt * Q_TILE, (rt + 1) * Q_TILE), rt * Q_TILE)
                for g in range(group_size) for rt in range(rows // Q_TILE)]

    def own_unit(head, carry):
        attend(head_tiles(0, (0,), head), True)
        return carry

    with jax.named_scope('own'):
        lax.fori_loop(0, kv_heads, own_unit, 0)

    def far_unit(rel, ccs, head):
        with jax.named_scope('far'):
            attend(head_tiles(rel, ccs, head), False)

    has_left = chip >= 1
    has_right = chip >= 3
    has_far = chip >= 2
    fwd_right = jnp.logical_and(chip >= 1, chip <= 2)

    def take_head_zero():
        @pl.when(has_left)
        def _():
            own_to(1, 0, 0, x_right).wait_recv()

            @pl.when(fwd_right)
            def _():
                far_k(0).start()

            fwd_sib(1, 0).start()

        @pl.when(has_right)
        def _():
            own_to(2, 0, 0, x_left).wait_recv()
            far_v(0).start()
            fwd_sib(2, 0).start()

        @pl.when(chip == 0)
        def _():
            left_v(0).wait_recv()
            far_v(0).start()

    def take_head_one(i):
        @pl.when(has_left)
        def _():
            own_chunk(1, 1, x_right, i * half_chunks, half_chunks, i == 1).wait_recv()

            @pl.when(fwd_right)
            def _():
                far_k(1, key_halves[i]).start()

            if i == 1:
                fwd_sib(1, 1).start()

        @pl.when(has_right)
        def _():
            own_chunk(2, 1, x_left, i * half_chunks, half_chunks, i == 1).wait_recv()
            far_v(1, key_halves[i]).start()
            if i == 1:
                fwd_sib(2, 1).start()

        @pl.when(chip == 0)
        def _():
            left_v(1, key_halves[i], i == 1).wait_recv()
            far_v(1, key_halves[i]).start()

    @pl.when(core == 1)
    def _():
        own_to(0, 1, 0, sibling).wait_recv()
        own_to(0, 1, 1, sibling).wait_recv()

    take_head_zero()
    head_one(1)

    ends = jnp.logical_or(chip == 0, chip == 3)

    def wx_late(c):
        @pl.when(fwd_right)
        def _():
            wx_own(0, c, chip).start()

        @pl.when(ends)
        def _():
            wx_own(1, c, chip).start()

    for c in range(2):
        wo_part(c, 1).wait_recv()

        @pl.when(ends)
        def _(c=c):
            wx_own(0, c, chip).start()

        @pl.when(fwd_right)
        def _(c=c):
            wx_own(1, c, chip).start()

    def sibling_unit(head, carry):
        far_unit(0, (1,), head)
        return carry

    @pl.when(core == 1)
    def _():
        lax.fori_loop(0, kv_heads, sibling_unit, 0)

    def seg(index):
        return pl.ds(pl.multiple_of(index * seg_rows, seg_rows), seg_rows)

    own_seg, far_seg = tp, (tp + 2) % ring
    mate_seg = ((tp + ring + turn) % ring, (tp + ring - turn) % ring)

    head_cols = group_size * HEAD

    def o_part(c, which, head):
        hc = slice(head * head_cols, (head + 1) * head_cols)
        return remote(o_v.at[seg(mate_seg[c] if which else far_seg), hc], ox_v.at[c, which, :, hc],
                      o_send, o_recv.at[which], y_mate[c])

    def finish_rows(head, rs):
        for qi in range(head * group_size, (head + 1) * group_size):
            o_v[rs, qi * HEAD:(qi + 1) * HEAD] = (acc_v[qi, :, rs] * (1.0 / l_v[qi, :, rs])).astype(BF).T

    loads[3].wait()

    def sib_wait(rel, head):
        remote(kv_v.at[rel, 0, head], kv_v.at[rel, 1, head], kv_fwd_send.at[rel, head], kv_recv.at[rel, 1, head], sibling).wait_recv()

    shift = (chip // (ring - 1)) * (1 - core)

    def side_unit(u, carry):
        head = u // 3
        rel = 1 + u % 3
        need = ((rel == 1) & has_left) | ((rel == 2) & has_right) | ((rel == 3) & has_far)

        @pl.when((u == 0) & has_left)
        def _():
            sib_wait(1, 0)

        at = u - shift

        @pl.when((at == 1) & has_far)
        def _():
            with jax.named_scope('far_h0'):
                far_k(0).wait_recv()
                far_v(0).wait_recv()
                fwd_sib(3, 0).start()

        @pl.when((u == 1) & has_right)
        def _():
            sib_wait(2, 0)

        @pl.when(u == 1)
        def _():
            take_head_one(0)

        @pl.when(at == 2)
        def _():
            with jax.named_scope('take_h1'):
                take_head_one(1)
                for c in range(2):
                    wx_late(c)

        @pl.when((u == 2) & has_far)
        def _():
            sib_wait(3, 0)

        @pl.when(u == 3)
        def _():
            finish_rows(0, slice(0, rows))
            for c in range(2):
                o_part(c, 0, 0).start()
            for c in range(2):
                o_part(c, 1, 0).start()

        @pl.when((u == 3) & (chip < 2))
        def _():
            with jax.named_scope('wx_wait'):
                for c in range(2):
                    for d in range(2):
                        wx_own(d, c, chip_right if d else chip_left).wait_recv()
                        wx_pass(d, c, chip_right if d else chip_left).start()

        @pl.when((u == 3) & has_left)
        def _():
            sib_wait(1, 1)

        @pl.when(need)
        def _():
            far_unit(rel, (0, 1), head)

        return carry

    lax.fori_loop(0, 4, side_unit, 0)

    @pl.when(has_far)
    def _():
        with jax.named_scope('far_h1'):
            far_k(1).wait_recv()
            far_v(1).wait_recv()
            fwd_sib(3, 1).start()

    @pl.when(has_right)
    def _():
        sib_wait(2, 1)

    def col(c, g):
        return pl.ds(pl.multiple_of(c * half + g * cols, cols), cols)

    def two_mates(c, g, own_rows, which):
        g0 = pl.multiple_of(g * cols, cols)
        return (jnp.dot(o_v[seg(own_rows), :], wo_v[:, col(c, g)], preferred_element_type=F32)
                + jnp.dot(ox_v[c, which], wox_v[c, :, pl.ds(g0, cols)], preferred_element_type=F32))

    def cross(c, g):
        return remote(part_v.at[c, g], recv_v.at[c, g], part_send, part_recv.at[c, g], y_mate[1 - c])

    def f1(c, g, d, owner):
        block = out_v.at[seg(owner), col(c, g)]
        return remote(block, block, f1_send, f1_recv.at[c, g] if c == d else f1_late, y_left if d else y_right)

    def f2(g, d, owner):
        block = out_v.at[seg(owner), col(d, g)]
        return remote(block, block, f2_send, f2_recv, y_left if d else y_right)

    def project_cross(g, carry):
        for c in range(2):
            part_v[c, g] = two_mates(c, g, mate_seg[1 - c], 0).astype(BF)
            cross(c, g).start()
        return carry

    def seg_step(j, carry):
        index = (tp + ring + 2 * ((3 - j) // 3) + turn * ((j % 3) % 2) - turn * (j // 2 - j // 3)) % ring
        rs = seg(index)

        @pl.when(j == 3)
        def _():
            with jax.named_scope('mates'):
                all_bytes(wox_v.at[:, :k_half, :], wo_fwd_send, wo_fwd_recv).wait_recv()
                all_bytes(ox_v.at[:, 0], o_send, o_recv.at[0]).wait_recv()

            with jax.named_scope('cross'):
                lax.fori_loop(0, CHUNKS, project_cross, 0)

        def seg_tiles(*rels):
            return [(rel, (0, 1), 1, group_size + g, rs, 0) for rel in rels for g in range(group_size)]

        @pl.when(has_right)
        def _():
            with jax.named_scope('right_seg'):
                attend(seg_tiles(2), False)

        @pl.when((j == 0) & has_far)
        def _():
            sib_wait(3, 1)

        @pl.when(has_far)
        def _():
            with jax.named_scope('far_seg'):
                attend(seg_tiles(3), False)

        finish_rows(1, rs)

        @pl.when(j == 0)
        def _():
            for c in range(2):
                o_part(c, 0, 1).start()
            with jax.named_scope('wo_wait'):
                for c in range(2):
                    wo_part(c, 0).wait_recv()
                    wo_share(c, 0, core).start()

        @pl.when(j == 1)
        def _():
            o_part(0, 1, 1).start()
            with jax.named_scope('sub_wait'):
                @pl.when(has_far)
                def _():
                    for d in range(2):
                        for c in range(2):
                            wx_own(d, c, chip_right if d else chip_left).wait_recv()

                for d, gets in ((0, fwd_right), (1, ends)):
                    @pl.when(gets)
                    def _(d=d):
                        for c in range(2):
                            wx_pass(d, c, chip_far).wait_recv()

                for c in range(2):
                    wo_share(c, 1, core).start()

        @pl.when(j == 2)
        def _():
            o_part(1, 1, 1).start()

        return carry

    with jax.named_scope('segs'):
        lax.fori_loop(0, ring, seg_step, 0)

    with jax.named_scope('caches'):
        k_out[...] = kc_v[...].reshape(k_out.shape)
        v_out[...] = vc_v[...].reshape(v_out.shape)

    all_bytes(ox_v.at[:, 1], o_send, o_recv.at[1]).wait_recv()

    def project_own(g, carry):
        for c in range(2):
            attn = two_mates(c, g, own_seg, 1)
            cross(c, g).wait_recv()
            attn = attn + recv_v[c, g].astype(F32)
            out_v[seg(own_seg), col(c, g)] = (x_v[seg(own_seg), col(c, g)].astype(F32) + attn).astype(BF)
            for d in range(2):
                f1(c, g, d, own_seg).start()
        return carry

    with jax.named_scope('own_out'):
        lax.fori_loop(0, CHUNKS, project_own, 0)

    side_seg = ((tp + ring - 1) % ring, (tp + 1) % ring)

    def pass_on(g, carry):
        for d in range(2):
            f1(d, g, d, side_seg[d]).wait_recv()
            f2(g, d, side_seg[d]).start()
        return carry

    with jax.named_scope('pass_on'):
        lax.fori_loop(0, CHUNKS, pass_on, 0)

    with jax.named_scope('drain'):
        own_rows = out_v.at[:seg_rows, :]
        all_bytes(own_rows, f2_send, f1_late).wait_recv()
        all_bytes(own_rows, f2_send, f2_recv).wait_recv()
        all_bytes(own_rows, f2_send, f2_recv).wait_send()
        all_bytes(out_v.at[:2 * seg_rows, :], f1_send, f2_recv).wait_send()
        all_bytes(part_v, part_send, f2_recv).wait_send()
        all_bytes(ox_v, o_send, f2_recv).wait_send()
        all_bytes(wox_v.at[:, :k_half, :], wo_fwd_send, f2_recv).wait_send()
    passed = wox_v.at[0, :SHARED_ROWS, :]
    all_bytes(passed, wx_send, f2_recv).wait_send()
    all_bytes(wox_v.at[0, :2 * (direct_rows + SHARED_ROWS // ring), :], wo_send, f2_recv).wait_send()

    @pl.when(chip < 2)
    def _():
        all_bytes(passed, wf_send, f2_recv).wait_send()

    @pl.when(core == 0)
    def _():
        own_to(0, 1, 0, sibling).wait_send()
        own_to(0, 1, 1, sibling).wait_send()

    for head in range(kv_heads):
        @pl.when(right_sends)
        def _(head=head):
            own_to(1, 0, head, x_right).wait_send()

        @pl.when(chip == 0)
        def _(head=head):
            own_to(2, 0, head, x_left).wait_send()

        @pl.when(chip == 1)
        def _(head=head):
            left_v(head).wait_send()

        @pl.when(fwd_right)
        def _(head=head):
            far_k(head).wait_send()

        @pl.when(jnp.logical_or(chip == 0, has_right))
        def _(head=head):
            far_v(head).wait_send()

        for rel, sent in ((1, has_left), (2, has_right), (3, has_far)):
            @pl.when(sent)
            def _(rel=rel, head=head):
                fwd_sib(rel, head).wait_send()


def copy_out(*refs):
    count = len(refs) // 2
    sems = refs[-1]
    copies = [pltpu.make_async_copy(refs[i], refs[count + i], sems.at[i]) for i in range(count)]
    for copy in copies:
        copy.start()
    for copy in copies:
        copy.wait()


def solution(mesh):
    ring = mesh.shape['tp']
    if mesh.shape['cp'] != 2 * ring or ring != 4:
        raise ValueError('mesh')
    row_spec = P(('dp', 'cp'), None)
    cache_spec = P(('dp', 'cp'), 'tp', None)
    head_cols = P(None, 'tp')

    def local_block(hidden, positions, norm_gain, w_query, w_key, w_value, w_out):
        rows, width = hidden.shape
        kv_heads = w_key.shape[1] // HEAD
        q_heads = w_query.shape[1] // HEAD
        seg_rows, half = rows // ring, width // 2
        cols = half // CHUNKS
        dma = pltpu.SemaphoreType.DMA
        out, k_new, v_new = pl.pallas_call(
            lambda *refs: block_kernel(ring, kv_heads, q_heads // kv_heads, *refs),
            out_shape=(
                pltpu.VMEM((rows, width), BF),
                pltpu.VMEM((rows, kv_heads, HEAD), BF),
                pltpu.VMEM((rows, kv_heads, HEAD), BF),
            ),
            in_specs=[pl.BlockSpec(memory_space=pl.ANY)] * 8,
            out_specs=[pl.BlockSpec(memory_space=pltpu.VMEM)] * 3,
            scratch_shapes=[
                pltpu.VMEM((rows,), jnp.int32),
                pltpu.VMEM((width,), BF),
                pltpu.VMEM((1, HEAD), F32),
                pltpu.VMEM((rows, width), BF),
                pltpu.VMEM((rows, width), BF),
                pltpu.VMEM(w_query.shape, BF),
                pltpu.VMEM((2, width, kv_heads * HEAD), BF),
                pltpu.VMEM(w_out.shape, BF),
                pltpu.VMEM((rows, HEAD), F32),
                pltpu.VMEM((rows, HEAD), F32),
                pltpu.VMEM((rows, kv_heads * HEAD), BF),
                pltpu.VMEM((rows, kv_heads * HEAD), BF),
                pltpu.VMEM((q_heads, HEAD, rows), BF),
                pltpu.VMEM((4, 2, kv_heads, 2, rows, HEAD), BF),
                pltpu.VMEM((q_heads, 1, rows), F32),
                pltpu.VMEM((q_heads, 1, rows), F32),
                pltpu.VMEM((q_heads, HEAD, rows), F32),
                pltpu.VMEM((rows, q_heads * HEAD), BF),
                pltpu.VMEM((2, q_heads * HEAD, half), BF),
                pltpu.VMEM((2, 2, seg_rows, q_heads * HEAD), BF),
                pltpu.VMEM((2, CHUNKS, seg_rows, cols), BF),
                pltpu.VMEM((2, CHUNKS, seg_rows, cols), BF),
                dma((7 + LOAD_CHUNKS,)),
                dma((3, kv_heads)),
                dma((4, 2, kv_heads)),
                dma((4, kv_heads)),
                dma((kv_heads, 2)), dma((kv_heads, 2)), dma((3,)),
                dma(()), dma((2, 2)), dma(()), dma((2, 2)), dma(()), dma((2, 2)), dma(()), dma(()),
                dma(()), dma((2,)),
                dma(()), dma((2, CHUNKS)),
                dma(()), dma((2, CHUNKS)), dma(()),
                dma(()), dma(()),
            ],
            compiler_params=pltpu.CompilerParams(collective_id=0, has_side_effects=True, vmem_limit_bytes=60 * 1024 * 1024),
            name='attn_block',
        )(hidden, positions, norm_gain, jnp.asarray(inverse_freq()), w_query, w_key, w_value, w_out)
        results = [pltpu.with_memory_space_constraint(r, pltpu.VMEM) for r in (out, k_new, v_new)]
        return pl.pallas_call(
            copy_out,
            out_shape=tuple(jax.ShapeDtypeStruct(r.shape, r.dtype) for r in results),
            in_specs=[pl.BlockSpec(memory_space=pltpu.VMEM)] * 3,
            out_specs=[pl.BlockSpec(memory_space=pl.ANY)] * 3,
            scratch_shapes=[dma((3,))],
            compiler_params=pltpu.CompilerParams(vmem_limit_bytes=8 * 1024 * 1024),
            name='copy_out',
        )(*results)

    return jax.shard_map(local_block, mesh=mesh,
                         in_specs=(row_spec, P(('dp', 'cp')), P(None), head_cols, head_cols, head_cols, P('tp', None)),
                         out_specs=(row_spec, cache_spec, cache_spec), check_vma=False)
```
